256 devices in a mesh: district: 4 (over y_lo, core), sub: 64 (over x, y_hi, z).
Axes of the slice: x: 4, y: 4 (y_hi: 2, y_lo: 2; y = y_hi * 2 + y_lo), z: 8, core: 2. Of those that a mesh axis runs over, the one named last changes fastest.
Arguments:
- cost_terms: bfloat16 [8, 4096, 768], P('district', 'sub'), may hold values from -6 to 6
- neighbours: int32 [8, 4096, 4], P('district', 'sub'), may hold values from 0 to 4095, as said below
- relayout: int32 [8, 4096], P('district'), may hold values from 0 to 4095, as said below
- ownership: int32 [8, 4096], P('district', 'sub'), may hold values from 0 to 31
- capacity: float32 [16, 48], replicated, may hold values from -192 to 192
- coupling: bfloat16 [8, 768, 192], P('district'), may hold values from -0.21875 to 0.21875
- solve_factor: bfloat16 [8, 768, 768], P('district')
Outputs:
- control_plan: float32 [8, 4096, 768], P('district', 'sub')
- flow_prices: float32 [8, 4096, 192], P('district', 'sub')
- reservoir_duals: float32 [16, 48], replicated
The draws below stay inside these ranges and needn't reach their ends.
Inputs may be any that keep to these rules, and one draw needn't show every extreme that they name: `neighbours`: each entry lies within 16 of its own balanced position and differs from it. `relayout`: each row is a permutation; of the subsystems at geographic positions s * 64 to (s + 1) * 64 - 1, exactly 1 go to balanced positions j * 64 to (j + 1) * 64 - 1, for every s and j. `ownership`: values of 16 or more mean that the subsystem draws from no reservoir.
All inputs are finite; a program needn't handle non-finite values.
Results may differ from the reference program's by a relative error of at most 0.018.
Values may be sent and summed in bfloat16 or wider, within the bound.
A program may use at most 64 MiB of HBM per device.

```python
import math
import jax
import jax.numpy as jnp
from jax import lax

HORIZON = 48
UNKNOWNS = 768
INTERFACE = 192
SUB_DEV = 64
DISTRICTS = 8
SUB_DIST = 4096
PEER_SHARE = 1
REACH_SPAN = 16
LINK_COUNT = 4
RESERVOIRS = 16
RESERVOIR_LOAD = 1024
OUTER_ITERS = 2
INNER_ITERS = 4


def draw_neighbours(key, part):
    picks = jax.random.randint(key, (DISTRICTS, SUB_DIST, LINK_COUNT), 0, 2 * REACH_SPAN)
    offsets = picks - REACH_SPAN + (picks >= REACH_SPAN).astype(jnp.int32)
    places = jnp.arange(SUB_DIST, dtype=jnp.int32)[None, :, None]
    target = places + offsets
    target = jnp.where((target < 0) | (target >= SUB_DIST), places - offsets, target)
    return target.astype(jnp.int32)


def draw_relayout(key, part):
    first_key = jax.random.fold_in(key, 11)
    second_key = jax.random.fold_in(key, 23)
    groups = SUB_DIST // SUB_DEV
    base = jnp.tile(jnp.arange(SUB_DEV, dtype=jnp.int32)[None, :], (DISTRICTS * groups, 1))
    source_perm = jax.random.permutation(first_key, base, axis=1, independent=True).reshape(DISTRICTS, groups, SUB_DEV)
    target_perm = jax.random.permutation(second_key, base, axis=1, independent=True).reshape(DISTRICTS, groups, SUB_DEV)
    dest_block = source_perm // PEER_SHARE
    within = source_perm % PEER_SHARE
    sources = jnp.arange(groups, dtype=jnp.int32)[None, :, None]
    slot_index = sources * PEER_SHARE + within
    district_rows = jnp.arange(DISTRICTS, dtype=jnp.int32)[:, None, None]
    target = dest_block * SUB_DEV + target_perm[district_rows, dest_block, slot_index]
    return target.reshape(DISTRICTS, SUB_DIST).astype(jnp.int32)


def draw_solve_factor(key, part):
    first_key = jax.random.fold_in(key, 5)
    second_key = jax.random.fold_in(key, 7)
    diagonal = jnp.exp(jax.random.uniform(first_key, (DISTRICTS, UNKNOWNS), jnp.float32, jnp.log(0.5), jnp.log(2.0)))
    spread = jax.random.normal(second_key, (DISTRICTS, UNKNOWNS, UNKNOWNS), jnp.float32) * (0.5 / UNKNOWNS ** 0.5)
    matrix = spread + diagonal[:, :, None] * jnp.eye(UNKNOWNS, dtype=jnp.float32)[None, :, :]
    return matrix.astype(jnp.bfloat16)


def set_ends(entries, own_key, low, high):
    dims = entries.shape
    index_at = [jax.random.randint(jax.random.fold_in(own_key, axis), (), 0, dims[axis]) for axis in range(len(dims))]
    entries = entries.at[tuple(index_at)].set(low)
    longest = dims.index(max(dims))
    index_at[longest] = (index_at[longest] + 1) % dims[longest]
    return entries.at[tuple(index_at)].set(high)


def shard_levels(key, shape, pieces, least, high):
    factor_of, own = 1.0, jax.random.fold_in(key, 6)
    for position, parts in pieces:
        heights = jnp.exp(jax.random.uniform(jax.random.fold_in(own, position), (parts,), jnp.float32, least / len(pieces), high / len(pieces)))
        factor_of = factor_of * jnp.repeat(heights, shape[position] // parts).reshape([-1 if axis == position else 1 for axis in range(len(shape))])
    return factor_of


def normal_values(stream_key, shape, scale, limit, split=(), held_as=jnp.bfloat16):
    values = scale * jax.random.normal(stream_key, shape, jnp.float32)
    if split:
        values = values * shard_levels(stream_key, shape, split, -0.22, 0.18)
    return jnp.clip(values, -limit, limit).astype(held_as)


def setup_inputs(seed: int = 0) -> dict:
    seeds = jax.random.split(jax.random.key(seed), 8)
    return {
        "cost_terms": normal_values(seeds[0], (DISTRICTS, SUB_DIST, UNKNOWNS), 1.0, 6.0, ((0, 4), (1, 64))),
        "neighbours": draw_neighbours(jax.random.fold_in(seeds[7], 71), 0),
        "relayout": draw_relayout(jax.random.fold_in(seeds[7], 71), 0),
        "ownership": set_ends(jax.random.randint(seeds[3], (DISTRICTS, SUB_DIST), 0, 2 * RESERVOIRS), jax.random.fold_in(seeds[3], 1), 0, (2 * RESERVOIRS) - 1).astype(jnp.int32),
        "capacity": normal_values(seeds[4], (RESERVOIRS, HORIZON), (RESERVOIR_LOAD ** 0.5), 192.0, (), jnp.float32),
        "coupling": normal_values(seeds[5], (DISTRICTS, UNKNOWNS, INTERFACE), UNKNOWNS ** -0.5, 0.21875, ((0, 4),)),
        "solve_factor": draw_solve_factor(jax.random.fold_in(seeds[7], 71), 0),
    }


price_step = 0.3
reserve_step = 1.0

def neighbour_mean(values, links):
    district_rows = jnp.arange(values.shape[0], dtype=jnp.int32)[:, None]
    running = jnp.zeros(links.shape[:2] + values.shape[2:], jnp.float32)
    for which in range(LINK_COUNT):
        running = running + values[district_rows, links[:, :, which]].astype(jnp.float32)
    return running / LINK_COUNT

def reference(cost_terms, neighbours, relayout, ownership, capacity, coupling, solve_factor):
    district_rows = jnp.arange(DISTRICTS, dtype=jnp.int32)[:, None]
    inverse = jnp.argsort(relayout, axis=1, stable=True).astype(jnp.int32)
    balanced_costs = cost_terms[district_rows, inverse]
    owner_slot = jnp.where(ownership < RESERVOIRS, ownership, RESERVOIRS).astype(jnp.int32)
    flow_prices = jnp.zeros((DISTRICTS, SUB_DIST, INTERFACE), jnp.float32)
    reserve_duals = jnp.zeros((RESERVOIRS, HORIZON), jnp.float32)
    dual_scale = reserve_step / math.sqrt(RESERVOIR_LOAD)
    highest = lax.Precision.HIGHEST
    coupling_wide = coupling.astype(jnp.float32)
    factor_wide = solve_factor.astype(jnp.float32)
    plan_now = None
    flow_now = None
    for outer_step in range(OUTER_ITERS):
        for inner_step in range(INNER_ITERS):
            padded_duals = jnp.concatenate([reserve_duals, jnp.zeros((1, HORIZON), jnp.float32)], axis=0)
            boundary = padded_duals[owner_slot]
            boundary = jnp.concatenate([boundary, jnp.zeros((DISTRICTS, SUB_DIST, INTERFACE - HORIZON), jnp.float32)], axis=2)
            price_term = (flow_prices - neighbour_mean(flow_prices, neighbours) + boundary).astype(jnp.bfloat16)
            gradient = (balanced_costs.astype(jnp.float32) + jnp.einsum('dsf,dzf->dsz', price_term.astype(jnp.float32), coupling_wide, precision=highest)).astype(jnp.bfloat16)
            plan_now = -jnp.einsum('dsz,dzw->dsw', gradient.astype(jnp.float32), factor_wide, precision=highest)
            plan_rounded = plan_now.astype(jnp.bfloat16)
            flow_now = jnp.einsum('dsz,dzf->dsf', plan_rounded.astype(jnp.float32), coupling_wide, precision=highest).astype(jnp.bfloat16)
            flow_prices = flow_prices + price_step * (flow_now.astype(jnp.float32) - neighbour_mean(flow_now, neighbours))
        draws = jax.ops.segment_sum(flow_now[:, :, :HORIZON].astype(jnp.float32).reshape(-1, HORIZON), owner_slot.reshape(-1), num_segments=RESERVOIRS + 1)[:RESERVOIRS]
        reserve_duals = reserve_duals + (draws - capacity) * dual_scale
    control_plan = plan_now[district_rows, relayout]
    return (control_plan, flow_prices, reserve_duals)
```

```python
import math

import jax
import jax.numpy as jnp
from jax import lax
from jax.experimental import pallas as pl
from jax.experimental.pallas import tpu as pltpu
from jax.sharding import PartitionSpec as P

MESH = pl.DeviceIdType.MESH
F32, BF16 = jnp.float32, jnp.bfloat16
HORIZON, UNKNOWNS, INTERFACE, BLOCK = 48, 768, 192, 64
RES, SUBS, DISTS = 16, 64, 4
REACH = 4
SLAB = 2 * REACH + 1
ROWS = 640
OWN = 32 + REACH * BLOCK
LANES = 256
STEP = 0.3
PEERS = SUBS - 1
OTHERS = 24


def dot(a, b):
    return jnp.dot(a, b, preferred_element_type=F32)


def dot_ta(a, b):
    return lax.dot_general(a, b, (((0,), (0,)), ((), ())), preferred_element_type=F32)


def dot_tb(a, b):
    return lax.dot_general(a, b, (((1,), (1,)), ((), ())), preferred_element_type=F32)


def iota(shape, dim):
    return lax.broadcasted_iota(jnp.int32, shape, dim)


def kernel(
    cost, coup, solve, own_ref, rt_ref, meta_ref, cap_ref,
    plan_o, price_o, dual_o,
    X, S, C, cs, cts, send1, recv1, send2, recv2, mbuf, offs, L2, lown, p4t, p5, mp, vfull,
    zf, zb, sacc, usum, ara, arb,
    load_sem, s1, r1, s2, r2, sm, rm, sa, ra, sb, rb,
):
    sub = lax.axis_index("sub")
    dist = lax.axis_index("district")
    sxy, sz = sub // 8, lax.rem(sub, 8)

    loads = []
    for d in range(2):
        loads.append(pltpu.make_async_copy(cost.at[d], X.at[d], load_sem.at[3 * d]))
        loads.append(pltpu.make_async_copy(solve.at[d], S.at[d], load_sem.at[3 * d + 1]))
        loads.append(pltpu.make_async_copy(coup.at[d], C.at[d], load_sem.at[3 * d + 2]))
    for copy in loads:
        copy.start()

    barrier = pltpu.get_barrier_semaphore()

    def hello(k, _):
        pl.semaphore_signal(
            barrier, inc=1, device_id={"sub": lax.rem(sub + k, SUBS)}, device_id_type=MESH
        )
        return 0

    lax.fori_loop(1, SUBS, hello, 0)

    def hello_other(k, _):
        there = lax.rem(dist + 1 + k // 8, DISTS)
        pl.semaphore_signal(
            barrier,
            inc=1,
            device_id={"district": there, "sub": lax.rem(k, 8) * 8 + sz},
            device_id_type=MESH,
        )
        return 0

    lax.fori_loop(0, OTHERS, hello_other, 0)

    first = []
    for d in range(2):
        for copy in loads[3 * d : 3 * d + 3]:
            copy.wait()
        cs_d = dot(X[d], S[d])
        cs[d * BLOCK : (d + 1) * BLOCK] = cs_d
        first.append(dot((-cs_d).astype(BF16), C[d]).astype(BF16))
    first = jnp.concatenate(first, axis=0)
    first = jnp.concatenate([first, jnp.zeros((2 * BLOCK, LANES - INTERFACE), BF16)], axis=1)
    lane = iota((2 * BLOCK, 2 * BLOCK), 1)
    row = iota((2 * BLOCK, 2 * BLOCK), 0)
    own_block = own_ref[...]
    to_dest = jnp.where(2 * own_block + lane // BLOCK == row, 1.0, 0.0).astype(BF16)
    eye = jnp.where(lane == row, 1.0, 0.0).astype(BF16)
    send1[0:REACH] = jnp.zeros((REACH, 2, LANES), BF16)
    send1[REACH + SUBS : SUBS + 2 * REACH] = jnp.zeros((REACH, 2, LANES), BF16)
    send1[REACH : REACH + SUBS] = dot(to_dest, first).astype(BF16).reshape(SUBS, 2, LANES)

    pl.semaphore_wait(barrier, PEERS + OTHERS)

    def meta_copy(k):
        return pltpu.make_async_remote_copy(
            src_ref=meta_ref,
            dst_ref=mbuf.at[2 * REACH - k],
            send_sem=sm,
            recv_sem=rm,
            device_id={"sub": lax.rem(sub + k - REACH + SUBS, SUBS)},
            device_id_type=MESH,
        )

    for k in range(SLAB):
        if k != REACH:
            meta_copy(k).start()

    def slab_copy(k):
        peer = lax.rem(sub + k, SUBS)
        return pltpu.make_async_remote_copy(
            src_ref=send1.at[pl.ds(peer, SLAB)],
            dst_ref=recv1.at[sub],
            send_sem=s1,
            recv_sem=r1,
            device_id={"sub": peer},
            device_id_type=MESH,
        )

    def send_slab(k, _):
        slab_copy(k).start()
        return 0

    lax.fori_loop(1, SUBS, send_slab, 0)
    recv1[sub] = send1[pl.ds(sub, SLAB)]
    mbuf[REACH] = meta_ref[...]

    p5[...] = dot_ta(to_dest, eye).astype(BF16)
    for d in range(2):
        cts_d = dot_ta(C[d], S[d]).astype(BF16)
        cts[d] = cts_d
        m_d = dot(cts_d, C[d])
        mp[d] = jnp.zeros((LANES, LANES), BF16)
        mp[d, 0:INTERFACE, 0:INTERFACE] = (-STEP * m_d).astype(BF16)
        ri = iota((LANES - INTERFACE, LANES - 128), 0)
        li = iota((LANES - INTERFACE, LANES - 128), 1)
        shift = jnp.where(li - (INTERFACE - 128) == ri + RES, 1.0, 0.0)
        mp[d, INTERFACE:LANES, 128:LANES] = shift.astype(BF16)

    rt = rt_ref[...]
    block_of, place_in = rt // BLOCK, lax.rem(rt, BLOCK)
    lane1 = iota((1, 2 * BLOCK), 1)

    def places(m):
        hit = block_of == sub + (m - REACH)
        place = jnp.sum(jnp.where(hit, place_in + 1, 0), axis=0, keepdims=True) - 1
        return jnp.where(place >= 0, place + BLOCK * lax.rem(lane1, 2), -1)

    def place_map(m):
        return jnp.where(places(m) == row, 1.0, 0.0).astype(BF16)

    p4t[...] = dot_ta(place_map(REACH), eye).astype(BF16)

    meta_all = pltpu.make_async_remote_copy(
        src_ref=mbuf.at[pl.ds(0, SLAB - 1)],
        dst_ref=mbuf.at[pl.ds(0, SLAB - 1)],
        send_sem=sm,
        recv_sem=rm,
        device_id={"sub": sub},
        device_id_type=MESH,
    )
    meta_all.wait_recv()
    eye64 = jnp.where(
        iota((BLOCK, 128), 0) == iota((BLOCK, 128), 1), 1.0, 0.0
    ).astype(BF16)
    zero32 = jnp.zeros((32, 16), F32)
    offs[0:32] = zero32
    offs[ROWS - 32 : ROWS] = zero32
    for m in range(SLAB):
        offs[32 + m * BLOCK : 32 + (m + 1) * BLOCK] = dot_tb(eye64, mbuf[m])
    diff = (iota((LANES, LANES), 1) - iota((LANES, LANES), 0)).astype(F32)
    for d in range(2):
        for i in range(3):
            cols = offs[192 * i : 192 * i + 256]
            near = jnp.where(diff == 0.0, 1.0, 0.0)
            for k in range(4):
                at = 4 * d + k
                near = near - jnp.where(diff == cols[:, at : at + 1], 0.25, 0.0)
            near = near.astype(BF16)
            L2[d, i] = dot(near, near)[32:224].astype(BF16)
        cols = offs[OWN : OWN + BLOCK]
        diff_own = (
            iota((BLOCK, 128), 1) - 32 - iota((BLOCK, 128), 0)
        ).astype(F32)
        near = jnp.where(diff_own == 0.0, 1.0, 0.0)
        for k in range(4):
            at = 4 * d + k
            near = near - jnp.where(diff_own == cols[:, at : at + 1], 0.25, 0.0)
        lown[d] = near.astype(BF16)

    for d in range(2):
        for top in (0, ROWS - 32):
            zf[d, top : top + 32] = jnp.zeros((32, LANES), F32)
            zb[d, top : top + 32] = jnp.zeros((32, LANES), BF16)
    slabs_all = pltpu.make_async_remote_copy(
        src_ref=recv1.at[pl.ds(0, PEERS)],
        dst_ref=recv1.at[pl.ds(0, PEERS)],
        send_sem=s1,
        recv_sem=r1,
        device_id={"sub": sub},
        device_id_type=MESH,
    )
    slabs_all.wait_recv()
    lane_e = iota((BLOCK, 128), 1) - (INTERFACE - 128)
    for m in range(SLAB):
        arrived = recv1[:, m].reshape(2 * BLOCK, LANES)
        rows_m = dot(place_map(m), arrived)
        top = 32 + m * BLOCK
        for d in range(2):
            part = rows_m[d * BLOCK : (d + 1) * BLOCK]
            owner = offs[top : top + BLOCK, 8 + d : 9 + d].astype(jnp.int32)
            mark = jnp.where((lane_e == owner) & (lane_e >= 0) & (lane_e < RES), 1.0, 0.0)
            low, high = part[:, 0:128], part[:, 128:LANES] + mark
            zf[d, top : top + BLOCK, 0:128] = low
            zf[d, top : top + BLOCK, 128:LANES] = high
            zb[d, top : top + BLOCK, 0:128] = low.astype(BF16)
            zb[d, top : top + BLOCK, 128:LANES] = high.astype(BF16)
    for d in range(2):
        sacc[d] = zf[d, OWN - 32 : OWN + 96]
        usum[d] = jnp.zeros((BLOCK, LANES), F32)

    def half(d, i):
        u = dot(L2[d, i], zb[d, 192 * i : 192 * i + 256])
        if i == 1:
            usum[d] += u[BLOCK : 2 * BLOCK]
        return u.astype(BF16)

    def advance(d, i, u):
        at = 32 + 192 * i
        z = zf[d, at : at + 192] + dot(u, mp[d])
        zf[d, at : at + 192] = z
        zb[d, at : at + 192] = z.astype(BF16)
        if i == 1:
            sacc[d] += z[32:160]

    def step(chunks):
        us = [(d, i, half(d, i)) for d in range(2) for i in chunks]
        for d, i, u in us:
            advance(d, i, u)

    def full_step(_, carry):
        step((0, 1, 2))
        return carry

    def marks(d):
        return zb[d, OWN : OWN + BLOCK, INTERFACE:LANES]

    def draw_part(flows):
        total = 0.0
        for d in range(2):
            first_marks = zb[d, OWN : OWN + BLOCK, INTERFACE : INTERFACE + RES]
            total = total + dot_ta(first_marks, flows[d])
        return total[:, 0:128]

    def folded(part):
        low, high = part[0:8, 0:64], part[8:16, 0:64]
        return jnp.concatenate([low, high], axis=1)

    def start_a(t):
        def go(k, _):
            z = lax.rem(sz + k, 8)
            pltpu.make_async_remote_copy(
                src_ref=ara.at[t, sz],
                dst_ref=ara.at[t, sz],
                send_sem=sa.at[t],
                recv_sem=ra.at[t],
                device_id={"sub": sxy * 8 + z},
                device_id_type=MESH,
            ).start()
            return 0

        lax.fori_loop(1, 8, go, 0)

    def start_b(t):
        here = dist * 8 + sxy

        def go(k, _):
            there = lax.rem(here + k, 32)
            pltpu.make_async_remote_copy(
                src_ref=arb.at[t, here],
                dst_ref=arb.at[t, here],
                send_sem=sb.at[t],
                recv_sem=rb.at[t],
                device_id={"district": there // 8, "sub": lax.rem(there, 8) * 8 + sz},
                device_id_type=MESH,
            ).start()
            return 0

        lax.fori_loop(1, 32, go, 0)

    def all_of(buf, t, count, send_sem, recv_sem):
        return pltpu.make_async_remote_copy(
            src_ref=buf.at[t, pl.ds(0, count)],
            dst_ref=buf.at[t, pl.ds(0, count)],
            send_sem=send_sem.at[t],
            recv_sem=recv_sem.at[t],
            device_id={"sub": sub},
            device_id_type=MESH,
        )

    def reduce_a(t, part):
        ara[t, sz] = folded(part)
        start_a(t)

    def reduce_b(t):
        all_of(ara, t, 7, sa, ra).wait_recv()
        arb[t, dist * 8 + sxy] = jnp.sum(ara[t], axis=0)
        start_b(t)

    def reduce_end(t):
        all_of(arb, t, 31, sb, rb).wait_recv()
        total = jnp.sum(arb[t], axis=0)
        return jnp.concatenate([total[:, 0:64], total[:, 64:128]], axis=0)

    def own_flows(d, top=OWN):
        return zb[d, top : top + BLOCK, 0:INTERFACE]

    lax.fori_loop(0, 3, full_step, 0)
    reduce_a(0, draw_part([own_flows(d) for d in range(2)]))
    lax.fori_loop(0, 2, full_step, 0)
    step((1,))

    us = [half(d, 1) for d in range(2)]
    back = []
    for d in range(2):
        prices = (STEP * usum[d]).astype(BF16)
        back.append(
            jnp.concatenate([prices[:, 0:INTERFACE], marks(d)], axis=1)
        )
    back = dot(p4t[...], jnp.concatenate(back, axis=0)).astype(BF16)
    send2[...] = back.reshape(SUBS, 2, LANES)

    def row_copy(k):
        peer = lax.rem(sub + k, SUBS)
        return pltpu.make_async_remote_copy(
            src_ref=send2.at[peer],
            dst_ref=recv2.at[sub],
            send_sem=s2,
            recv_sem=r2,
            device_id={"sub": peer},
            device_id_type=MESH,
        )

    def send_row(k, _):
        row_copy(k).start()
        return 0

    lax.fori_loop(1, SUBS, send_row, 0)
    recv2[sub] = send2[sub]

    stacks = [marks(d) for d in range(2)]
    near_marks = [
        dot(lown[d], zb[d, OWN - 32 : OWN + 96])[:, 128:LANES] for d in range(2)
    ]
    for d in range(2):
        advance(d, 1, us[d])
    price0 = []
    for d in range(2):
        sums = sacc[d][:, 0:INTERFACE]
        price0.append(dot(lown[d], sums.astype(BF16)))

    reduce_b(0)
    capacity = cap_ref[...]
    scale = 1.0 / math.sqrt(DISTS * 2 * SUBS * BLOCK / (2 * RES))
    duals = (reduce_end(0)[:, 0:HORIZON] - capacity) * scale
    wide = jnp.concatenate([duals, jnp.zeros((RES, INTERFACE - HORIZON), F32)], axis=1)

    binom = (1.0, 6.0, 15.0, 20.0)
    in_price = (1.0, -0.9, 0.27, -0.027)
    in_flow = (-1.0, 0.9, -0.27, 0.027)
    in_sum = (-4.0, 1.8, -0.36, 0.027)
    flows = []
    for d in range(2):
        powers = [wide]
        m_d = mp[d, 0:INTERFACE, 0:INTERFACE]
        for _ in range(4):
            powers.append(dot(powers[-1].astype(BF16), m_d) * (-1.0 / STEP))
        stack_price = [powers[j] * (in_price[j] / binom[j]) for j in range(4)]
        stack_flow = [powers[j + 1] * (in_flow[j] / binom[j]) for j in range(4)]
        stack_sum = [powers[j + 1] * (in_sum[j] / binom[j]) for j in range(4)]
        stack_price, stack_flow, stack_sum = [
            jnp.concatenate(t, axis=0).astype(BF16) for t in (stack_price, stack_flow, stack_sum)
        ]
        q8 = zf[d, OWN : OWN + BLOCK, 0:INTERFACE] + dot(stacks[d], stack_flow)
        flows.append(q8.astype(BF16))
        near_d = near_marks[d][:, INTERFACE - 128 : 128].astype(BF16)
        price_o[d] = STEP * (price0[d] + dot(near_d, stack_sum))
        vfull[d, 0:INTERFACE] = cts[d]
        vfull[d, INTERFACE:LANES] = dot(stack_price, cts[d]).astype(BF16)
    reduce_a(1, draw_part(flows))

    rows_all = pltpu.make_async_remote_copy(
        src_ref=recv2.at[pl.ds(0, PEERS)],
        dst_ref=recv2.at[pl.ds(0, PEERS)],
        send_sem=s2,
        recv_sem=r2,
        device_id={"sub": sub},
        device_id_type=MESH,
    )
    rows_all.wait_recv()
    mine = dot(p5[...], recv2[...].reshape(2 * BLOCK, LANES)).astype(BF16)
    for d in range(2):
        at = d * BLOCK
        plan_o[d] = -(cs[at : at + BLOCK] + dot(mine[at : at + BLOCK], vfull[d]))

    reduce_b(1)
    dual_o[...] = duals + (reduce_end(1)[:, 0:HORIZON] - capacity) * scale

    meta_all.wait_send()
    slabs_all.wait_send()
    rows_all.wait_send()
    for t in range(2):
        all_of(ara, t, 7, sa, ra).wait_send()
        all_of(arb, t, 31, sb, rb).wait_send()


def on_device(cost_terms, neighbours, relayout, ownership, capacity, coupling, solve_factor):
    sub = lax.axis_index("sub")
    mine = lax.dynamic_slice_in_dim(relayout, sub * BLOCK, BLOCK, axis=1)
    own = (mine // BLOCK).reshape(1, 2 * BLOCK)
    rt = relayout.reshape(2, SUBS, BLOCK).transpose(2, 1, 0).reshape(BLOCK, 2 * SUBS)
    places = sub * BLOCK + jnp.arange(BLOCK, dtype=jnp.int32)
    offsets = (neighbours - places[None, :, None]).transpose(0, 2, 1).reshape(8, BLOCK)
    meta = jnp.concatenate([offsets, ownership, jnp.zeros((6, BLOCK), jnp.int32)], axis=0)
    meta = jnp.pad(meta, ((0, 0), (0, 128 - BLOCK))).astype(BF16)
    vmem = pl.BlockSpec(memory_space=pltpu.VMEM)
    hbm = pl.BlockSpec(memory_space=pl.ANY)
    dma = pltpu.SemaphoreType.DMA
    return pl.pallas_call(
        kernel,
        out_shape=(
            jax.ShapeDtypeStruct((2, BLOCK, UNKNOWNS), F32),
            jax.ShapeDtypeStruct((2, BLOCK, INTERFACE), F32),
            jax.ShapeDtypeStruct((RES, HORIZON), F32),
        ),
        in_specs=[hbm, hbm, hbm, vmem, vmem, vmem, vmem],
        out_specs=(vmem, vmem, vmem),
        scratch_shapes=[
            pltpu.VMEM((2, BLOCK, UNKNOWNS), BF16),
            pltpu.VMEM((2, UNKNOWNS, UNKNOWNS), BF16),
            pltpu.VMEM((2, UNKNOWNS, INTERFACE), BF16),
            pltpu.VMEM((2 * BLOCK, UNKNOWNS), F32),
            pltpu.VMEM((2, INTERFACE, UNKNOWNS), BF16),
            pltpu.VMEM((SUBS + 2 * REACH, 2, LANES), BF16),
            pltpu.VMEM((SUBS, SLAB, 2, LANES), BF16),
            pltpu.VMEM((SUBS, 2, LANES), BF16),
            pltpu.VMEM((SUBS, 2, LANES), BF16),
            pltpu.VMEM((SLAB, 16, 128), BF16),
            pltpu.VMEM((ROWS, 16), F32),
            pltpu.VMEM((2, 3, 192, 256), BF16),
            pltpu.VMEM((2, BLOCK, 128), BF16),
            pltpu.VMEM((128, 128), BF16),
            pltpu.VMEM((128, 128), BF16),
            pltpu.VMEM((2, LANES, LANES), BF16),
            pltpu.VMEM((2, LANES, UNKNOWNS), BF16),
            pltpu.VMEM((2, ROWS, LANES), F32),
            pltpu.VMEM((2, ROWS, LANES), BF16),
            pltpu.VMEM((2, 128, LANES), F32),
            pltpu.VMEM((2, BLOCK, LANES), F32),
            pltpu.VMEM((2, 8, 8, 128), F32),
            pltpu.VMEM((2, 32, 8, 128), F32),
            dma((6,)),
            dma, dma, dma, dma, dma, dma,
            dma((2,)), dma((2,)), dma((2,)), dma((2,)),
        ],
        compiler_params=pltpu.CompilerParams(
            collective_id=0, has_side_effects=True, vmem_limit_bytes=48 * 1024 * 1024
        ),
    )(cost_terms, coupling, solve_factor, own, rt, meta, capacity)


def solution(mesh):
    placed = (
        P("district", "sub", None),
        P("district", "sub", None),
        P("district", None),
        P("district", "sub"),
        P(),
        P("district", None, None),
        P("district", None, None),
    )
    return jax.shard_map(
        on_device,
        mesh=mesh,
        in_specs=placed,
        out_specs=(P("district", "sub", None), P("district", "sub", None), P()),
        check_vma=False,
    )
```

```python
import math

import jax
import jax.numpy as jnp
from jax import lax
from jax.experimental import pallas as pl
from jax.experimental.pallas import tpu as pltpu
from jax.sharding import PartitionSpec as P

MESH = pl.DeviceIdType.MESH
F32, BF16 = jnp.float32, jnp.bfloat16
HORIZON, UNKNOWNS, INTERFACE, BLOCK = 48, 768, 192, 64
RES, SUBS, DISTS = 16, 64, 4
REACH = 4
SLAB = 2 * REACH + 1
ROWS = 640
OWN = 32 + REACH * BLOCK
LANES = 256
STEP = 0.3
PEERS = SUBS - 1
OTHERS = 24
VMEM_LIMIT = 67043328 - 700 * 1024


def dot(a, b):
    return jnp.dot(a, b, preferred_element_type=F32)


def dot_ta(a, b):
    return lax.dot_general(a, b, (((0,), (0,)), ((), ())), preferred_element_type=F32)


def dot_tb(a, b):
    return lax.dot_general(a, b, (((1,), (1,)), ((), ())), preferred_element_type=F32)


def iota(shape, dim):
    return lax.broadcasted_iota(jnp.int32, shape, dim)


def kernel(
    cost, coup, solve, rel_h, near_h, owner_h, cap_h,
    plan_o, price_o, dual_o,
    X, S, C, cs, vfull, rel, near_in, owner_in, cap, meta, cts, send1, recv1, send2, recv2, mbuf, offs, L2, lown, p4t, p5, mp,
    zf, zb, sacc, usum, ara, arb,
    load_sem, s1, r1, s2, r2, sm, rm, sa, ra, sb, rb,
):
    sub = lax.axis_index("sub")
    dist = lax.axis_index("district")
    sxy, sz = sub // 8, lax.rem(sub, 8)

    small = [
        pltpu.make_async_copy(src, dst, load_sem.at[6 + i])
        for i, (src, dst) in enumerate(
            ((rel_h, rel), (near_h, near_in), (owner_h, owner_in), (cap_h, cap))
        )
    ]
    loads = []
    for d in range(2):
        loads.append(pltpu.make_async_copy(cost.at[d], X.at[d], load_sem.at[3 * d]))
        loads.append(pltpu.make_async_copy(solve.at[d], S.at[d], load_sem.at[3 * d + 1]))
        loads.append(pltpu.make_async_copy(coup.at[d], C.at[d], load_sem.at[3 * d + 2]))
    for copy in small + loads:
        copy.start()

    barrier = pltpu.get_barrier_semaphore()

    def hello(k, _):
        pl.semaphore_signal(
            barrier, inc=1, device_id={"sub": lax.rem(sub + k, SUBS)}, device_id_type=MESH
        )
        return 0

    lax.fori_loop(1, SUBS, hello, 0)

    def hello_other(k, _):
        there = lax.rem(dist + 1 + k // 8, DISTS)
        pl.semaphore_signal(
            barrier,
            inc=1,
            device_id={"district": there, "sub": lax.rem(k, 8) * 8 + sz},
            device_id_type=MESH,
        )
        return 0

    lax.fori_loop(0, OTHERS, hello_other, 0)

    for copy in small:
        copy.wait()
    place = iota((4, BLOCK), 1) + sub * BLOCK
    told = [near_in[d] - place for d in range(2)] + [owner_in[...], jnp.zeros((6, BLOCK), jnp.int32)]
    told = jnp.concatenate(told, axis=0).astype(F32)
    meta[...] = jnp.concatenate([told, jnp.zeros((16, BLOCK), F32)], axis=1).astype(BF16)
    mbuf[REACH] = meta[...]
    here = rel[sub // 2]
    here = jnp.where(lax.rem(sub, 2) == 0, here[:, 0:BLOCK], here[:, BLOCK:128]) // BLOCK
    own_block = jnp.concatenate([here[0:1], here[1:2]], axis=1)

    first = []
    for d in range(2):
        for copy in loads[3 * d : 3 * d + 3]:
            copy.wait()
        cs_d = dot(X[d], S[d])
        cs[d * BLOCK : (d + 1) * BLOCK] = cs_d
        first.append(dot_tb((-cs_d).astype(BF16), C[d]).astype(BF16))
    first = jnp.concatenate(first, axis=0)
    first = jnp.concatenate([first, jnp.zeros((2 * BLOCK, LANES - INTERFACE), BF16)], axis=1)
    lane = iota((2 * BLOCK, 2 * BLOCK), 1)
    row = iota((2 * BLOCK, 2 * BLOCK), 0)
    to_dest = jnp.where(2 * own_block + lane // BLOCK == row, 1.0, 0.0).astype(BF16)
    eye = jnp.where(lane == row, 1.0, 0.0).astype(BF16)
    send1[0:REACH] = jnp.zeros((REACH, 2, LANES), BF16)
    send1[REACH + SUBS : SUBS + 2 * REACH] = jnp.zeros((REACH, 2, LANES), BF16)
    send1[REACH : REACH + SUBS] = dot(to_dest, first).astype(BF16).reshape(SUBS, 2, LANES)

    pl.semaphore_wait(barrier, PEERS + OTHERS)

    def meta_copy(k):
        return pltpu.make_async_remote_copy(
            src_ref=meta,
            dst_ref=mbuf.at[2 * REACH - k],
            send_sem=sm,
            recv_sem=rm,
            device_id={"sub": lax.rem(sub + k - REACH + SUBS, SUBS)},
            device_id_type=MESH,
        )

    for k in range(SLAB):
        if k != REACH:
            meta_copy(k).start()

    def slot_of(device):
        return lax.rem(device, 2) * (SUBS // 2) + device // 2

    def slab_copy(k):
        peer = lax.rem(sub + k, SUBS)
        return pltpu.make_async_remote_copy(
            src_ref=send1.at[pl.ds(peer, SLAB)],
            dst_ref=recv1.at[slot_of(sub)],
            send_sem=s1,
            recv_sem=r1,
            device_id={"sub": peer},
            device_id_type=MESH,
        )

    def send_slab(k, _):
        slab_copy(k).start()
        return 0

    lax.fori_loop(1, SUBS, send_slab, 0)
    recv1[slot_of(sub)] = send1[pl.ds(sub, SLAB)]

    p5[...] = dot_ta(to_dest, eye).astype(BF16)
    for d in range(2):
        cts_d = dot(C[d], S[d]).astype(BF16)
        cts[d] = cts_d
        m_d = dot_tb(cts_d, C[d])
        mp[d] = jnp.zeros((LANES, LANES), BF16)
        mp[d, 0:INTERFACE, 0:INTERFACE] = (-STEP * m_d).astype(BF16)
        ri = iota((LANES - INTERFACE, LANES - 128), 0)
        li = iota((LANES - INTERFACE, LANES - 128), 1)
        shift = jnp.where(li - (INTERFACE - 128) == ri + RES, 1.0, 0.0)
        mp[d, INTERFACE:LANES, 128:LANES] = shift.astype(BF16)

    by_pair = rel[...].reshape(SUBS, 128)
    eye_s = eye[0:SUBS, 0:SUBS]

    def turned(values):
        flat = dot_ta(values.astype(F32).astype(BF16), eye_s)
        return jnp.concatenate([flat[0:BLOCK], flat[BLOCK:128]], axis=1).astype(jnp.int32)

    block_of, place_in = turned(by_pair // BLOCK), turned(lax.rem(by_pair, BLOCK))
    lane1 = iota((1, 2 * BLOCK), 1)

    def places(m):
        hit = block_of == sub + (m - REACH)
        place = jnp.sum(jnp.where(hit, place_in + 1, 0), axis=0, keepdims=True) - 1
        return jnp.where(place >= 0, place + BLOCK * lax.rem(lane1, 2), -1)

    def place_map(m):
        return jnp.where(places(m) == row, 1.0, 0.0).astype(BF16)

    p4t[...] = dot_ta(place_map(REACH), eye).astype(BF16)

    meta_all = pltpu.make_async_remote_copy(
        src_ref=mbuf.at[pl.ds(0, SLAB - 1)],
        dst_ref=mbuf.at[pl.ds(0, SLAB - 1)],
        send_sem=sm,
        recv_sem=rm,
        device_id={"sub": sub},
        device_id_type=MESH,
    )
    meta_all.wait_recv()
    eye64 = jnp.where(
        iota((BLOCK, 128), 0) == iota((BLOCK, 128), 1), 1.0, 0.0
    ).astype(BF16)
    zero32 = jnp.zeros((32, 16), F32)
    offs[0:32] = zero32
    offs[ROWS - 32 : ROWS] = zero32
    for m in range(SLAB):
        offs[32 + m * BLOCK : 32 + (m + 1) * BLOCK] = dot_tb(eye64, mbuf[m])
    diff = (iota((LANES, LANES), 1) - iota((LANES, LANES), 0)).astype(F32)
    for d in range(2):
        for i in range(3):
            cols = offs[192 * i : 192 * i + 256]
            near = jnp.where(diff == 0.0, 1.0, 0.0)
            for k in range(4):
                at = 4 * d + k
                near = near - jnp.where(diff == cols[:, at : at + 1], 0.25, 0.0)
            near = near.astype(BF16)
            L2[d, i] = dot(near, near)[32:224].astype(BF16)
        cols = offs[OWN : OWN + BLOCK]
        diff_own = (
            iota((BLOCK, 128), 1) - 32 - iota((BLOCK, 128), 0)
        ).astype(F32)
        near = jnp.where(diff_own == 0.0, 1.0, 0.0)
        for k in range(4):
            at = 4 * d + k
            near = near - jnp.where(diff_own == cols[:, at : at + 1], 0.25, 0.0)
        lown[d] = near.astype(BF16)

    for d in range(2):
        for top in (0, ROWS - 32):
            zf[d, top : top + 32] = jnp.zeros((32, LANES), F32)
            zb[d, top : top + 32] = jnp.zeros((32, LANES), BF16)
    slabs_all = pltpu.make_async_remote_copy(
        src_ref=recv1.at[pl.ds(0, PEERS)],
        dst_ref=recv1.at[pl.ds(0, PEERS)],
        send_sem=s1,
        recv_sem=r1,
        device_id={"sub": sub},
        device_id_type=MESH,
    )
    slabs_all.wait_recv()
    lane_e = iota((BLOCK, 128), 1) - (INTERFACE - 128)
    for m in range(SLAB):
        arrived = recv1[:, m].reshape(2 * BLOCK, LANES)
        rows_m = dot(place_map(m), arrived)
        top = 32 + m * BLOCK
        for d in range(2):
            part = rows_m[d * BLOCK : (d + 1) * BLOCK]
            owner = offs[top : top + BLOCK, 8 + d : 9 + d].astype(jnp.int32)
            mark = jnp.where((lane_e == owner) & (lane_e >= 0) & (lane_e < RES), 1.0, 0.0)
            low, high = part[:, 0:128], part[:, 128:LANES] + mark
            zf[d, top : top + BLOCK, 0:128] = low
            zf[d, top : top + BLOCK, 128:LANES] = high
            zb[d, top : top + BLOCK, 0:128] = low.astype(BF16)
            zb[d, top : top + BLOCK, 128:LANES] = high.astype(BF16)
    for d in range(2):
        sacc[d] = zf[d, OWN - 32 : OWN + 96]
        usum[d] = jnp.zeros((BLOCK, LANES), F32)

    def half(d, i):
        u = dot(L2[d, i], zb[d, 192 * i : 192 * i + 256])
        if i == 1:
            usum[d] += u[BLOCK : 2 * BLOCK]
        return u.astype(BF16)

    def advance(d, i, u):
        at = 32 + 192 * i
        z = zf[d, at : at + 192] + dot(u, mp[d])
        zf[d, at : at + 192] = z
        zb[d, at : at + 192] = z.astype(BF16)
        if i == 1:
            sacc[d] += z[32:160]

    def step(chunks):
        us = [(d, i, half(d, i)) for d in range(2) for i in chunks]
        for d, i, u in us:
            advance(d, i, u)

    def full_step(_, carry):
        step((0, 1, 2))
        return carry

    def marks(d):
        return zb[d, OWN : OWN + BLOCK, INTERFACE:LANES]

    def draw_part(flows):
        total = 0.0
        for d in range(2):
            first_marks = zb[d, OWN : OWN + BLOCK, INTERFACE : INTERFACE + RES]
            total = total + dot_ta(first_marks, flows[d])
        return total[:, 0:128]

    def folded(part):
        low, high = part[0:8, 0:64], part[8:16, 0:64]
        return jnp.concatenate([low, high], axis=1)

    def start_a(t):
        def go(k, _):
            z = lax.rem(sz + k, 8)
            pltpu.make_async_remote_copy(
                src_ref=ara.at[t, sz],
                dst_ref=ara.at[t, sz],
                send_sem=sa.at[t],
                recv_sem=ra.at[t],
                device_id={"sub": sxy * 8 + z},
                device_id_type=MESH,
            ).start()
            return 0

        lax.fori_loop(1, 8, go, 0)

    def start_b(t):
        here = dist * 8 + sxy

        def go(k, _):
            there = lax.rem(here + k, 32)
            pltpu.make_async_remote_copy(
                src_ref=arb.at[t, here],
                dst_ref=arb.at[t, here],
                send_sem=sb.at[t],
                recv_sem=rb.at[t],
                device_id={"district": there // 8, "sub": lax.rem(there, 8) * 8 + sz},
                device_id_type=MESH,
            ).start()
            return 0

        lax.fori_loop(1, 32, go, 0)

    def all_of(buf, t, count, send_sem, recv_sem):
        return pltpu.make_async_remote_copy(
            src_ref=buf.at[t, pl.ds(0, count)],
            dst_ref=buf.at[t, pl.ds(0, count)],
            send_sem=send_sem.at[t],
            recv_sem=recv_sem.at[t],
            device_id={"sub": sub},
            device_id_type=MESH,
        )

    def reduce_a(t, part):
        ara[t, sz] = folded(part)
        start_a(t)

    def reduce_b(t):
        all_of(ara, t, 7, sa, ra).wait_recv()
        arb[t, dist * 8 + sxy] = jnp.sum(ara[t], axis=0)
        start_b(t)

    def reduce_end(t):
        all_of(arb, t, 31, sb, rb).wait_recv()
        total = jnp.sum(arb[t], axis=0)
        return jnp.concatenate([total[:, 0:64], total[:, 64:128]], axis=0)

    def own_flows(d, top=OWN):
        return zb[d, top : top + BLOCK, 0:INTERFACE]

    lax.fori_loop(0, 3, full_step, 0)
    reduce_a(0, draw_part([own_flows(d) for d in range(2)]))
    lax.fori_loop(0, 2, full_step, 0)
    step((1,))

    us = [half(d, 1) for d in range(2)]
    back = []
    for d in range(2):
        prices = (STEP * usum[d]).astype(BF16)
        back.append(
            jnp.concatenate([prices[:, 0:INTERFACE], marks(d)], axis=1)
        )
    back = dot(p4t[...], jnp.concatenate(back, axis=0)).astype(BF16)
    send2[...] = back.reshape(SUBS, 2, LANES)

    def row_copy(k):
        peer = lax.rem(sub + k, SUBS)
        return pltpu.make_async_remote_copy(
            src_ref=send2.at[slot_of(peer)],
            dst_ref=recv2.at[sub],
            send_sem=s2,
            recv_sem=r2,
            device_id={"sub": peer},
            device_id_type=MESH,
        )

    def send_row(k, _):
        row_copy(k).start()
        return 0

    lax.fori_loop(1, SUBS, send_row, 0)
    recv2[sub] = send2[slot_of(sub)]

    stacks = [marks(d) for d in range(2)]
    near_marks = [
        dot(lown[d], zb[d, OWN - 32 : OWN + 96])[:, 128:LANES] for d in range(2)
    ]
    for d in range(2):
        advance(d, 1, us[d])
    price0 = []
    for d in range(2):
        sums = sacc[d][:, 0:INTERFACE]
        price0.append(dot(lown[d], sums.astype(BF16)))

    reduce_b(0)
    capacity = cap[...]
    scale = 1.0 / math.sqrt(DISTS * 2 * SUBS * BLOCK / (2 * RES))
    duals = (reduce_end(0)[:, 0:HORIZON] - capacity) * scale
    wide = jnp.concatenate([duals, jnp.zeros((RES, INTERFACE - HORIZON), F32)], axis=1)

    binom = (1.0, 6.0, 15.0, 20.0)
    in_price = (1.0, -0.9, 0.27, -0.027)
    in_flow = (-1.0, 0.9, -0.27, 0.027)
    in_sum = (-4.0, 1.8, -0.36, 0.027)
    flows = []
    for d in range(2):
        powers = [wide]
        m_d = mp[d, 0:INTERFACE, 0:INTERFACE]
        for _ in range(4):
            powers.append(dot(powers[-1].astype(BF16), m_d) * (-1.0 / STEP))
        stack_price = [powers[j] * (in_price[j] / binom[j]) for j in range(4)]
        stack_flow = [powers[j + 1] * (in_flow[j] / binom[j]) for j in range(4)]
        stack_sum = [powers[j + 1] * (in_sum[j] / binom[j]) for j in range(4)]
        stack_price, stack_flow, stack_sum = [
            jnp.concatenate(t, axis=0).astype(BF16) for t in (stack_price, stack_flow, stack_sum)
        ]
        q8 = zf[d, OWN : OWN + BLOCK, 0:INTERFACE] + dot(stacks[d], stack_flow)
        flows.append(q8.astype(BF16))
        near_d = near_marks[d][:, INTERFACE - 128 : 128].astype(BF16)
        price_o[d] = STEP * (price0[d] + dot(near_d, stack_sum))
        vfull[d, 0:INTERFACE] = cts[d]
        vfull[d, INTERFACE:LANES] = dot(stack_price, cts[d]).astype(BF16)
    reduce_a(1, draw_part(flows))

    rows_all = pltpu.make_async_remote_copy(
        src_ref=recv2.at[pl.ds(0, PEERS)],
        dst_ref=recv2.at[pl.ds(0, PEERS)],
        send_sem=s2,
        recv_sem=r2,
        device_id={"sub": sub},
        device_id_type=MESH,
    )
    rows_all.wait_recv()
    mine = dot(p5[...], recv2[...].reshape(2 * BLOCK, LANES)).astype(BF16)
    for d in range(2):
        at = d * BLOCK
        plan_o[d] = -(cs[at : at + BLOCK] + dot(mine[at : at + BLOCK], vfull[d]))

    reduce_b(1)
    dual_o[...] = duals + (reduce_end(1)[:, 0:HORIZON] - capacity) * scale

    meta_all.wait_send()
    slabs_all.wait_send()
    rows_all.wait_send()
    for t in range(2):
        all_of(ara, t, 7, sa, ra).wait_send()
        all_of(arb, t, 31, sb, rb).wait_send()


def write_out(plan, price, dual, plan_o, price_o, dual_o, sems):
    copies = [
        pltpu.make_async_copy(src, dst, sems.at[i])
        for i, (src, dst) in enumerate(((plan, plan_o), (price, price_o), (dual, dual_o)))
    ]
    for copy in copies:
        copy.start()
    for copy in copies:
        copy.wait()


def on_device(cost_terms, neighbours, relayout, ownership, capacity, coupling, solve_factor):
    pairs = relayout.reshape(2, SUBS // 2, 2 * BLOCK).transpose(1, 0, 2)
    vmem = pl.BlockSpec(memory_space=pltpu.VMEM)
    hbm = pl.BlockSpec(memory_space=pltpu.HBM)
    dma = pltpu.SemaphoreType.DMA
    parts = pl.pallas_call(
        kernel,
        out_shape=(
            pltpu.VMEM((2, BLOCK, UNKNOWNS), F32),
            pltpu.VMEM((2, BLOCK, INTERFACE), F32),
            pltpu.VMEM((RES, HORIZON), F32),
        ),
        in_specs=[hbm] * 7,
        out_specs=(vmem,) * 3,
        scratch_shapes=[
            pltpu.VMEM((2, BLOCK, UNKNOWNS), BF16),
            pltpu.VMEM((2, UNKNOWNS, UNKNOWNS), BF16),
            pltpu.VMEM((2, INTERFACE, UNKNOWNS), BF16),
            pltpu.VMEM((2 * BLOCK, UNKNOWNS), F32),
            pltpu.VMEM((2, LANES, UNKNOWNS), BF16),
            pltpu.VMEM((SUBS // 2, 2, 2 * BLOCK), jnp.int32),
            pltpu.VMEM((2, 4, BLOCK), jnp.int32),
            pltpu.VMEM((2, BLOCK), jnp.int32),
            pltpu.VMEM((RES, HORIZON), F32),
            pltpu.VMEM((16, 128), BF16),
            pltpu.VMEM((2, INTERFACE, UNKNOWNS), BF16),
            pltpu.VMEM((SUBS + 2 * REACH, 2, LANES), BF16),
            pltpu.VMEM((SUBS, SLAB, 2, LANES), BF16),
            pltpu.VMEM((SUBS, 2, LANES), BF16),
            pltpu.VMEM((SUBS, 2, LANES), BF16),
            pltpu.VMEM((SLAB, 16, 128), BF16),
            pltpu.VMEM((ROWS, 16), F32),
            pltpu.VMEM((2, 3, 192, 256), BF16),
            pltpu.VMEM((2, BLOCK, 128), BF16),
            pltpu.VMEM((128, 128), BF16),
            pltpu.VMEM((128, 128), BF16),
            pltpu.VMEM((2, LANES, LANES), BF16),
            pltpu.VMEM((2, ROWS, LANES), F32),
            pltpu.VMEM((2, ROWS, LANES), BF16),
            pltpu.VMEM((2, 128, LANES), F32),
            pltpu.VMEM((2, BLOCK, LANES), F32),
            pltpu.VMEM((2, 8, 8, 128), F32),
            pltpu.VMEM((2, 32, 8, 128), F32),
            dma((10,)),
            dma, dma, dma, dma, dma, dma,
            dma((2,)), dma((2,)), dma((2,)), dma((2,)),
        ],
        compiler_params=pltpu.CompilerParams(
            collective_id=0, has_side_effects=True, vmem_limit_bytes=VMEM_LIMIT
        ),
    )(
        cost_terms, coupling.transpose(0, 2, 1), solve_factor, pairs,
        neighbours.transpose(0, 2, 1), ownership, capacity,
    )
    return pl.pallas_call(
        write_out,
        out_shape=(
            jax.ShapeDtypeStruct((2, BLOCK, UNKNOWNS), F32),
            jax.ShapeDtypeStruct((2, BLOCK, INTERFACE), F32),
            jax.ShapeDtypeStruct((RES, HORIZON), F32),
        ),
        in_specs=[vmem] * 3,
        out_specs=(hbm,) * 3,
        scratch_shapes=[dma((3,))],
        compiler_params=pltpu.CompilerParams(vmem_limit_bytes=1024 * 1024),
    )(*parts)


def solution(mesh):
    placed = (
        P("district", "sub", None),
        P("district", "sub", None),
        P("district", None),
        P("district", "sub"),
        P(),
        P("district", None, None),
        P("district", None, None),
    )
    return jax.shard_map(
        on_device,
        mesh=mesh,
        in_specs=placed,
        out_specs=(P("district", "sub", None), P("district", "sub", None), P()),
        check_vma=False,
    )
```

```python
import math

import jax
import jax.numpy as jnp
from jax import lax
from jax.experimental import pallas as pl
from jax.experimental.pallas import tpu as pltpu
from jax.sharding import PartitionSpec as P

MESH = pl.DeviceIdType.MESH
F32, BF16 = jnp.float32, jnp.bfloat16
HORIZON, UNKNOWNS, INTERFACE, BLOCK = 48, 768, 192, 64
RES, SUBS, DISTS = 16, 64, 4
PAIRS = SUBS // 2
REACH = 2
SLAB = 2 * REACH + 1
PAIR = 2 * BLOCK
ROWS = SLAB * PAIR
OWN = REACH * PAIR
LANES = 256
STEP = 0.3
PEERS = SUBS - 1
OTHERS = 27
VMEM_LIMIT = 67043328 - 700 * 1024


def dot(a, b):
    return jnp.dot(a, b, preferred_element_type=F32)


def dot_ta(a, b):
    return lax.dot_general(a, b, (((0,), (0,)), ((), ())), preferred_element_type=F32)


def dot_tb(a, b):
    return lax.dot_general(a, b, (((1,), (1,)), ((), ())), preferred_element_type=F32)


def iota(shape, dim):
    return lax.broadcasted_iota(jnp.int32, shape, dim)


def folded(part):
    return jnp.concatenate([part[0:8, 0:64], part[8:16, 0:64]], axis=1)


def unfolded(part):
    return jnp.concatenate([part[:, 0:64], part[:, 64:128]], axis=0)


def kernel(
    cost, coup, solve, rel_h, near_h, owner_h, cap_h,
    plan_o, price_o, dual_o,
    X, S, C, cs, vfull, rel, near_in, owner_in, cap, meta, cts, send1, recv1, send2, recv2,
    mbuf, offs, L2, lown, p4t, p5, mp, zf, zb, sacc, usum, ara, arb, aka, akb, arc, price_s, price_r,
    load_sem, s1, r1, s2, r2, sm, rm, sp, rp, sa, ra, sb, rb, ska, rka, skb, rkb, sc, rc,
):
    sub = lax.axis_index("sub")
    dist = lax.axis_index("district")
    sxy, sz = sub // 8, lax.rem(sub, 8)
    pair, side = sub // 2, lax.rem(sub, 2)

    small = [
        pltpu.make_async_copy(src, dst, load_sem.at[6 + i])
        for i, (src, dst) in enumerate(
            ((rel_h, rel), (near_h, near_in), (owner_h, owner_in), (cap_h, cap))
        )
    ]
    loads = []
    for d in range(2):
        loads.append(pltpu.make_async_copy(cost.at[d], X.at[d], load_sem.at[3 * d]))
        loads.append(pltpu.make_async_copy(solve.at[d], S.at[d], load_sem.at[3 * d + 1]))
        loads.append(pltpu.make_async_copy(coup.at[d], C.at[d], load_sem.at[3 * d + 2]))
    for copy in small + loads:
        copy.start()

    barrier = pltpu.get_barrier_semaphore()

    def hello(k, _):
        pl.semaphore_signal(
            barrier, inc=1, device_id={"sub": lax.rem(sub + k, SUBS)}, device_id_type=MESH
        )
        return 0

    lax.fori_loop(1, SUBS, hello, 0)

    def hello_other(k, _):
        there = lax.rem(dist + 1 + k // 8, DISTS)
        pl.semaphore_signal(
            barrier,
            inc=1,
            device_id={"district": there, "sub": lax.rem(k, 8) * 8 + sz},
            device_id_type=MESH,
        )
        return 0

    lax.fori_loop(0, 24, hello_other, 0)
    for k in range(1, 4):
        pl.semaphore_signal(
            barrier,
            inc=1,
            device_id={"district": lax.rem(dist + k, DISTS), "sub": 2 * pair + 1 - side},
            device_id_type=MESH,
        )

    def whole(buf, send_sem, recv_sem):
        return pltpu.make_async_remote_copy(
            src_ref=buf,
            dst_ref=buf,
            send_sem=send_sem,
            recv_sem=recv_sem,
            device_id={"sub": sub},
            device_id_type=MESH,
        )

    for copy in small:
        copy.wait()
    place = iota((4, BLOCK), 1) + sub * BLOCK
    told = [near_in[d] - place for d in range(2)] + [owner_in[...], jnp.zeros((6, BLOCK), jnp.int32)]
    told = jnp.concatenate(told, axis=0).astype(F32)
    meta[...] = jnp.concatenate([told, jnp.zeros((16, BLOCK), F32)], axis=1).astype(BF16)
    mbuf[2 * REACH + side] = meta[...]
    here = rel[pair]
    here = jnp.where(side == 0, here[:, 0:BLOCK], here[:, BLOCK:PAIR]) // BLOCK
    own_block = jnp.concatenate([here[0:1], here[1:2]], axis=1)

    first = []
    for d in range(2):
        for copy in loads[3 * d : 3 * d + 3]:
            copy.wait()
        cs_d = dot(X[d], S[d])
        cs[d * BLOCK : (d + 1) * BLOCK] = cs_d
        first.append(dot_tb((-cs_d).astype(BF16), C[d]).astype(BF16))
    first = jnp.concatenate(first, axis=0)
    first = jnp.concatenate([first, jnp.zeros((2 * BLOCK, LANES - INTERFACE), BF16)], axis=1)
    lane = iota((2 * BLOCK, 2 * BLOCK), 1)
    row = iota((2 * BLOCK, 2 * BLOCK), 0)
    to_dest = jnp.where(own_block + BLOCK * (lane // BLOCK) == row, 1.0, 0.0).astype(BF16)
    eye = jnp.where(lane == row, 1.0, 0.0).astype(BF16)
    sorted_rows = dot(to_dest, first).astype(BF16)
    for d in range(2):
        send1[d, 0:REACH] = jnp.zeros((REACH, 2, LANES), BF16)
        send1[d, REACH + PAIRS : PAIRS + 2 * REACH] = jnp.zeros((REACH, 2, LANES), BF16)
        send1[d, REACH : REACH + PAIRS] = sorted_rows[d * BLOCK : (d + 1) * BLOCK].reshape(
            PAIRS, 2, LANES
        )

    pl.semaphore_wait(barrier, PEERS + OTHERS)

    for k in range(2 * SLAB):
        a, e = k // 2, k % 2

        def meta_copy():
            pltpu.make_async_remote_copy(
                src_ref=meta,
                dst_ref=mbuf.at[4 * REACH - 2 * a + side],
                send_sem=sm,
                recv_sem=rm,
                device_id={"sub": 2 * lax.rem(pair + a - REACH + PAIRS, PAIRS) + e},
                device_id_type=MESH,
            ).start()

        if a == REACH:
            pl.when(side != e)(meta_copy)
        else:
            meta_copy()

    def slot_of(device):
        return lax.rem(device, 2) * PAIRS + device // 2

    def send_slab(k, _):
        peer = lax.rem(sub + k, SUBS)
        pltpu.make_async_remote_copy(
            src_ref=send1.at[lax.rem(peer, 2), pl.ds(peer // 2, SLAB)],
            dst_ref=recv1.at[slot_of(sub)],
            send_sem=s1,
            recv_sem=r1,
            device_id={"sub": peer},
            device_id_type=MESH,
        ).start()
        return 0

    lax.fori_loop(1, SUBS, send_slab, 0)
    recv1[slot_of(sub)] = send1[side, pl.ds(pair, SLAB)]

    back_at = 4 * (own_block // 2) + 2 * (lane // BLOCK) + lax.rem(own_block, 2)
    p5[...] = dot_ta(jnp.where(back_at == row, 1.0, 0.0).astype(BF16), eye).astype(BF16)
    for d in range(2):
        cts_d = dot(C[d], S[d]).astype(BF16)
        cts[d] = cts_d
        m_d = dot_tb(cts_d, C[d])
        mp[d] = jnp.zeros((LANES, LANES), BF16)
        mp[d, 0:INTERFACE, 0:INTERFACE] = (-STEP * m_d).astype(BF16)
        ri = iota((LANES - INTERFACE, LANES - 128), 0)
        li = iota((LANES - INTERFACE, LANES - 128), 1)
        shift = jnp.where(li - (INTERFACE - 128) == ri + RES, 1.0, 0.0)
        mp[d, INTERFACE:LANES, 128:LANES] = shift.astype(BF16)
        vfull[d, 0:INTERFACE] = cts_d

    by_pair = rel[...].reshape(SUBS, PAIR)
    si, sj = iota((SUBS, SUBS), 0), iota((SUBS, SUBS), 1)
    pick = jnp.where((si // 2 == sj // 2) & (lax.rem(si, 2) == side), 1.0, 0.0).astype(BF16)

    def turned(values):
        flat = dot_ta(values.astype(F32).astype(BF16), pick)
        return jnp.concatenate([flat[0:BLOCK], flat[BLOCK:PAIR]], axis=1).astype(jnp.int32)

    block_of, place_in = turned(by_pair // BLOCK), turned(lax.rem(by_pair, BLOCK))
    odd = lax.rem(iota((1, PAIR), 1), 2)

    def place_map(a):
        hit = block_of == 2 * (pair + a - REACH) + odd
        at = jnp.sum(jnp.where(hit, place_in + 1, 0), axis=0, keepdims=True) - 1
        at = jnp.where(at >= 0, at + BLOCK * odd, -1)
        return jnp.where(at == row, 1.0, 0.0).astype(BF16)

    p4t[...] = dot_ta(place_map(REACH), eye).astype(BF16)

    whole(mbuf.at[pl.ds(0, 2 * SLAB - 1)], sm, rm).wait_recv()
    eye64 = jnp.where(
        iota((BLOCK, 128), 0) == iota((BLOCK, 128), 1), 1.0, 0.0
    ).astype(BF16)
    for m in range(2 * SLAB):
        cols = dot_tb(eye64, mbuf[m])
        top = m * BLOCK
        offs[top : top + BLOCK, 0:4] = jnp.where(side == 0, cols[:, 0:4], cols[:, 4:8])
        offs[top : top + BLOCK, 4:5] = jnp.where(side == 0, cols[:, 8:9], cols[:, 9:10])
    diff = (iota((LANES, LANES), 1) - iota((LANES, LANES), 0)).astype(F32)
    for i in range(3):
        cols = offs[192 * i : 192 * i + 256]
        near = jnp.where(diff == 0.0, 1.0, 0.0)
        for k in range(4):
            near = near - jnp.where(diff == cols[:, k : k + 1], 0.25, 0.0)
        near = near.astype(BF16)
        L2[i] = dot(near, near)[32:224].astype(BF16)
        if i == 1:
            lown[...] = near[64:192]

    sacc[...] = jnp.zeros((256, LANES), F32)
    whole(recv1.at[pl.ds(0, PEERS)], s1, r1).wait_recv()
    lane_e = iota((PAIR, 128), 1) - (INTERFACE - 128)
    for a in range(SLAB):
        arrived = recv1[:, a].reshape(2 * SUBS, LANES)
        part = dot(place_map(a), arrived)
        top = a * PAIR
        owner = offs[top : top + PAIR, 4:5].astype(jnp.int32)
        mark = jnp.where((lane_e == owner) & (lane_e >= 0) & (lane_e < RES), 1.0, 0.0)
        low, high = part[:, 0:128], part[:, 128:LANES] + mark
        zf[top : top + PAIR, 0:128] = low
        zf[top : top + PAIR, 128:LANES] = high
        zb[top : top + PAIR, 0:128] = low.astype(BF16)
        zb[top : top + PAIR, 128:LANES] = high.astype(BF16)
    sacc[32:224] = zf[224:416]
    usum[...] = jnp.zeros((PAIR, LANES), F32)
    flow_map = mp.at[side]

    def half(i):
        u = dot(L2[i], zb[192 * i : 192 * i + 256])
        if i == 1:
            usum[...] += u[32:160]
        return u.astype(BF16)

    def advance(i, u):
        at = 32 + 192 * i
        z = zf[at : at + 192] + dot(u, flow_map[...])
        zf[at : at + 192] = z
        zb[at : at + 192] = z.astype(BF16)
        if i == 1:
            sacc[32:224] += z

    def step():
        us = [half(i) for i in range(3)]
        for i, u in enumerate(us):
            advance(i, u)

    def full_step(_, carry):
        step()
        return carry

    def own_part(with_lanes):
        marked = zb[OWN : OWN + PAIR, INTERFACE : INTERFACE + RES]
        return dot_ta(marked, with_lanes)

    def to_z(buf, t, send_sem, recv_sem, first_k, stride):
        def go(k, _):
            z = lax.rem(sz + first_k + stride * k, 8)
            pltpu.make_async_remote_copy(
                src_ref=buf.at[t, sz],
                dst_ref=buf.at[t, sz],
                send_sem=send_sem.at[t],
                recv_sem=recv_sem.at[t],
                device_id={"sub": sxy * 8 + z},
                device_id_type=MESH,
            ).start()
            return 0

        lax.fori_loop(0, 8 // stride - 1, go, 0)

    def start_b(t):
        here_b = dist * 8 + sxy

        def go(k, _):
            there = lax.rem(here_b + k, 32)
            pltpu.make_async_remote_copy(
                src_ref=arb.at[t, here_b],
                dst_ref=arb.at[t, here_b],
                send_sem=sb.at[t],
                recv_sem=rb.at[t],
                device_id={"district": there // 8, "sub": lax.rem(there, 8) * 8 + sz},
                device_id_type=MESH,
            ).start()
            return 0

        lax.fori_loop(1, 32, go, 0)

    def all_of(buf, t, count, send_sem, recv_sem):
        return whole(buf.at[t, pl.ds(0, count)], send_sem.at[t], recv_sem.at[t])

    def reduce_a(t, part):
        ara[t, sz] = folded(part)
        to_z(ara, t, sa, ra, 1, 1)

    def reduce_b(t):
        all_of(ara, t, 7, sa, ra).wait_recv()
        arb[t, dist * 8 + sxy] = jnp.sum(ara[t], axis=0)
        start_b(t)

    def reduce_end(t):
        all_of(arb, t, 31, sb, rb).wait_recv()
        return unfolded(jnp.sum(arb[t], axis=0))

    lax.fori_loop(0, 3, full_step, 0)
    reduce_a(0, own_part(zb[OWN : OWN + PAIR, 0:128]))
    marks = zb[OWN : OWN + PAIR, INTERFACE:LANES]
    aka[0, sz // 2] = folded(own_part(marks))

    def go_k(k, _):
        z = lax.rem(sz + 2 + 2 * k, 8)
        pltpu.make_async_remote_copy(
            src_ref=aka.at[0, sz // 2],
            dst_ref=aka.at[0, sz // 2],
            send_sem=ska,
            recv_sem=rka,
            device_id={"sub": sxy * 8 + z},
            device_id_type=MESH,
        ).start()
        return 0

    lax.fori_loop(0, 3, go_k, 0)
    near_marks = dot(lown[...], zb[192:448])[:, INTERFACE:LANES].astype(BF16)
    step()
    step()
    step()

    u = half(1)
    prices = (STEP * usum[...]).astype(BF16)
    back = jnp.concatenate([prices[:, 0:INTERFACE], marks], axis=1)
    send2[...] = dot(p4t[...], back).astype(BF16).reshape(SUBS, 2, LANES)

    def send_row(k, _):
        peer = lax.rem(sub + k, SUBS)
        pltpu.make_async_remote_copy(
            src_ref=send2.at[slot_of(peer)],
            dst_ref=recv2.at[sub],
            send_sem=s2,
            recv_sem=r2,
            device_id={"sub": peer},
            device_id_type=MESH,
        ).start()
        return 0

    lax.fori_loop(1, SUBS, send_row, 0)
    recv2[sub] = send2[slot_of(sub)]

    advance(1, u)
    reduce_a(1, own_part(zb[OWN : OWN + PAIR, 0:128]))
    price0 = dot(lown[...], sacc[...].astype(BF16))[:, 0:INTERFACE]

    reduce_b(0)
    whole(aka.at[0, pl.ds(0, 3)], ska, rka).wait_recv()
    akb[0, sxy] = jnp.sum(aka[0], axis=0)

    def go_kb(k, _):
        xy = lax.rem(sxy + k, 8)
        pltpu.make_async_remote_copy(
            src_ref=akb.at[0, sxy],
            dst_ref=akb.at[0, sxy],
            send_sem=skb,
            recv_sem=rkb,
            device_id={"sub": xy * 8 + sz},
            device_id_type=MESH,
        ).start()
        return 0

    lax.fori_loop(1, 8, go_kb, 0)
    reduce_b(1)
    capacity = cap[...]
    scale = 1.0 / math.sqrt(DISTS * 2 * SUBS * BLOCK / (2 * RES))
    duals = (reduce_end(0)[:, 0:HORIZON] - capacity) * scale
    wide = jnp.concatenate([duals, jnp.zeros((RES, INTERFACE - HORIZON), F32)], axis=1)

    binom = (1.0, 3.0, 3.0, 1.0)
    in_price = (1.0, -0.9, 0.27, -0.027)
    in_flow = (-1.0, 0.9, -0.27, 0.027)
    in_sum = (-4.0, 1.8, -0.36, 0.027)

    def powers_of(m_ref, count):
        powers = [wide]
        for _ in range(count):
            powers.append(
                dot(powers[-1].astype(BF16), m_ref[0:INTERFACE, 0:INTERFACE]) * (-1.0 / STEP)
            )
        return powers

    def stack(powers, weights):
        return jnp.concatenate(
            [p * (w / b) for p, w, b in zip(powers, weights, binom)], axis=0
        ).astype(BF16)

    powers = powers_of(flow_map, 4)
    whole(akb.at[0, pl.ds(0, 7)], skb, rkb).wait_recv()
    unit = unfolded(jnp.sum(akb[0], axis=0)).astype(BF16)
    here_c = dist * 2 + side
    arc[here_c] = folded(dot(unit, stack(powers[1:], in_flow))[:, 0:128])

    def go_c(k, _):
        there = lax.rem(here_c + k, 8)
        pltpu.make_async_remote_copy(
            src_ref=arc.at[here_c],
            dst_ref=arc.at[here_c],
            send_sem=sc,
            recv_sem=rc,
            device_id={"district": there // 2, "sub": 2 * pair + lax.rem(there, 2)},
            device_id_type=MESH,
        ).start()
        return 0

    lax.fori_loop(1, 8, go_c, 0)
    final_price = STEP * (price0 + dot(near_marks, stack(powers[1:], in_sum)))
    halves = [final_price[0:BLOCK], final_price[BLOCK:PAIR]]
    price_s[...] = jnp.where(side == 0, halves[1], halves[0])
    price_copy = pltpu.make_async_remote_copy(
        src_ref=price_s,
        dst_ref=price_r,
        send_sem=sp,
        recv_sem=rp,
        device_id={"sub": 2 * pair + 1 - side},
        device_id_type=MESH,
    )
    price_copy.start()
    price_o[side] = jnp.where(side == 0, halves[0], halves[1])
    for d in range(2):
        powers_d = powers_of(mp.at[d], 3)
        vfull[d, INTERFACE:LANES] = dot(stack(powers_d, in_price), cts[d]).astype(BF16)

    whole(recv2.at[pl.ds(0, PEERS)], s2, r2).wait_recv()
    mine = dot(p5[...], recv2[...].reshape(2 * SUBS, LANES)).astype(BF16)
    for d in range(2):
        at = d * BLOCK
        plan_o[d] = -(cs[at : at + BLOCK] + dot(mine[at : at + BLOCK], vfull[d]))

    price_copy.wait_recv()
    price_o[1 - side] = price_r[...]
    draws0 = reduce_end(1)[:, 0:HORIZON]
    whole(arc.at[pl.ds(0, 7)], sc, rc).wait_recv()
    draws1 = unfolded(jnp.sum(arc[...], axis=0))[:, 0:HORIZON]
    dual_o[...] = duals + (draws0 + draws1 - capacity) * scale

    whole(mbuf.at[pl.ds(0, 2 * SLAB - 1)], sm, rm).wait_send()
    whole(recv1.at[pl.ds(0, PEERS)], s1, r1).wait_send()
    whole(recv2.at[pl.ds(0, PEERS)], s2, r2).wait_send()
    for t in range(2):
        all_of(ara, t, 7, sa, ra).wait_send()
        all_of(arb, t, 31, sb, rb).wait_send()
    whole(aka.at[0, pl.ds(0, 3)], ska, rka).wait_send()
    whole(akb.at[0, pl.ds(0, 7)], skb, rkb).wait_send()
    whole(arc.at[pl.ds(0, 7)], sc, rc).wait_send()
    price_copy.wait_send()


def write_out(plan, price, dual, plan_o, price_o, dual_o, sems):
    copies = [
        pltpu.make_async_copy(src, dst, sems.at[i])
        for i, (src, dst) in enumerate(((plan, plan_o), (price, price_o), (dual, dual_o)))
    ]
    for copy in copies:
        copy.start()
    for copy in copies:
        copy.wait()


def on_device(cost_terms, neighbours, relayout, ownership, capacity, coupling, solve_factor):
    pairs = relayout.reshape(2, SUBS // 2, 2 * BLOCK).transpose(1, 0, 2)
    vmem = pl.BlockSpec(memory_space=pltpu.VMEM)
    hbm = pl.BlockSpec(memory_space=pltpu.HBM)
    dma = pltpu.SemaphoreType.DMA
    parts = pl.pallas_call(
        kernel,
        out_shape=(
            pltpu.VMEM((2, BLOCK, UNKNOWNS), F32),
            pltpu.VMEM((2, BLOCK, INTERFACE), F32),
            pltpu.VMEM((RES, HORIZON), F32),
        ),
        in_specs=[hbm] * 7,
        out_specs=(vmem,) * 3,
        scratch_shapes=[
            pltpu.VMEM((2, BLOCK, UNKNOWNS), BF16),
            pltpu.VMEM((2, UNKNOWNS, UNKNOWNS), BF16),
            pltpu.VMEM((2, INTERFACE, UNKNOWNS), BF16),
            pltpu.VMEM((2 * BLOCK, UNKNOWNS), F32),
            pltpu.VMEM((2, LANES, UNKNOWNS), BF16),
            pltpu.VMEM((SUBS // 2, 2, 2 * BLOCK), jnp.int32),
            pltpu.VMEM((2, 4, BLOCK), jnp.int32),
            pltpu.VMEM((2, BLOCK), jnp.int32),
            pltpu.VMEM((RES, HORIZON), F32),
            pltpu.VMEM((16, 128), BF16),
            pltpu.VMEM((2, INTERFACE, UNKNOWNS), BF16),
            pltpu.VMEM((2, PAIRS + 2 * REACH, 2, LANES), BF16),
            pltpu.VMEM((SUBS, SLAB, 2, LANES), BF16),
            pltpu.VMEM((SUBS, 2, LANES), BF16),
            pltpu.VMEM((SUBS, 2, LANES), BF16),
            pltpu.VMEM((2 * SLAB, 16, 128), BF16),
            pltpu.VMEM((ROWS, 8), F32),
            pltpu.VMEM((3, 192, 256), BF16),
            pltpu.VMEM((PAIR, 256), BF16),
            pltpu.VMEM((128, 128), BF16),
            pltpu.VMEM((128, 128), BF16),
            pltpu.VMEM((2, LANES, LANES), BF16),
            pltpu.VMEM((ROWS, LANES), F32),
            pltpu.VMEM((ROWS, LANES), BF16),
            pltpu.VMEM((256, LANES), F32),
            pltpu.VMEM((PAIR, LANES), F32),
            pltpu.VMEM((2, 8, 8, 128), F32),
            pltpu.VMEM((2, 32, 8, 128), F32),
            pltpu.VMEM((1, 4, 8, 128), F32),
            pltpu.VMEM((1, 8, 8, 128), F32),
            pltpu.VMEM((8, 8, 128), F32),
            pltpu.VMEM((BLOCK, INTERFACE), F32),
            pltpu.VMEM((BLOCK, INTERFACE), F32),
            dma((10,)),
            dma, dma, dma, dma, dma, dma, dma, dma,
            dma((2,)), dma((2,)), dma((2,)), dma((2,)),
            dma, dma, dma, dma, dma, dma,
        ],
        compiler_params=pltpu.CompilerParams(
            collective_id=0, has_side_effects=True, vmem_limit_bytes=VMEM_LIMIT
        ),
    )(
        cost_terms, coupling.transpose(0, 2, 1), solve_factor, pairs,
        neighbours.transpose(0, 2, 1), ownership, capacity,
    )
    return pl.pallas_call(
        write_out,
        out_shape=(
            jax.ShapeDtypeStruct((2, BLOCK, UNKNOWNS), F32),
            jax.ShapeDtypeStruct((2, BLOCK, INTERFACE), F32),
            jax.ShapeDtypeStruct((RES, HORIZON), F32),
        ),
        in_specs=[vmem] * 3,
        out_specs=(hbm,) * 3,
        scratch_shapes=[dma((3,))],
        compiler_params=pltpu.CompilerParams(vmem_limit_bytes=1024 * 1024),
    )(*parts)


def solution(mesh):
    placed = (
        P("district", "sub", None),
        P("district", "sub", None),
        P("district", None),
        P("district", "sub"),
        P(),
        P("district", None, None),
        P("district", None, None),
    )
    return jax.shard_map(
        on_device,
        mesh=mesh,
        in_specs=placed,
        out_specs=(P("district", "sub", None), P("district", "sub", None), P()),
        check_vma=False,
    )
```

```python
import math

import jax
import jax.numpy as jnp
from jax import lax
from jax.experimental import pallas as pl
from jax.experimental.pallas import tpu as pltpu
from jax.sharding import PartitionSpec as P

MESH = pl.DeviceIdType.MESH
F32, BF16 = jnp.float32, jnp.bfloat16
HORIZON, UNKNOWNS, INTERFACE, BLOCK = 48, 768, 192, 64
RES, SUBS, DISTS = 16, 64, 4
PAIRS = SUBS // 2
REACH = 2
SLAB = 2 * REACH + 1
PAIR = 2 * BLOCK
ROWS = SLAB * PAIR
OWN = REACH * PAIR
LANES = 256
STEP = 0.3
PEERS = SUBS - 1
OTHERS = 27
VMEM_LIMIT = 67043328 - 700 * 1024


def dot(a, b):
    return jnp.dot(a, b, preferred_element_type=F32)


def dot_ta(a, b):
    return lax.dot_general(a, b, (((0,), (0,)), ((), ())), preferred_element_type=F32)


def dot_tb(a, b):
    return lax.dot_general(a, b, (((1,), (1,)), ((), ())), preferred_element_type=F32)


def iota(shape, dim):
    return lax.broadcasted_iota(jnp.int32, shape, dim)


def offsets_by_hops():
    def hops(at):
        x, y, z = at
        return min(x, 4 - x) + 2 * y + min(z, 8 - z)

    every = [(x, y, z) for z in range(8) for x in range(4) for y in range(2)]
    return sorted(every, key=lambda at: (-hops(at), at))


def folded(part):
    return jnp.concatenate([part[0:8, 0:64], part[8:16, 0:64]], axis=1)


def unfolded(part):
    return jnp.concatenate([part[:, 0:64], part[:, 64:128]], axis=0)


def kernel(
    cost, coup, solve, rel_h, near_h, owner_h, cap_h,
    plan_o, price_o, dual_o,
    X, S, C, cs, vfull, rel, near_in, owner_in, cap, meta, cts, send1, recv1, send2, recv2,
    mbuf, offs, L2, lown, p4t, p5, mp, zf, zb, sacc, usum, ara, arb, aka, akb, arc, price_s, price_r,
    load_sem, s1, r1, s2, r2, sm, rm, sp, rp, sa, ra, sb, rb, ska, rka, skb, rkb, sc, rc,
):
    sub = lax.axis_index("sub")
    dist = lax.axis_index("district")
    sxy, sz = sub // 8, lax.rem(sub, 8)
    pair, side = sub // 2, lax.rem(sub, 2)

    small = [
        pltpu.make_async_copy(src, dst, load_sem.at[6 + i])
        for i, (src, dst) in enumerate(
            ((rel_h, rel), (near_h, near_in), (owner_h, owner_in), (cap_h, cap))
        )
    ]
    loads = []
    for d in range(2):
        loads.append(pltpu.make_async_copy(cost.at[d], X.at[d], load_sem.at[3 * d]))
        loads.append(pltpu.make_async_copy(solve.at[d], S.at[d], load_sem.at[3 * d + 1]))
        loads.append(pltpu.make_async_copy(coup.at[d], C.at[d], load_sem.at[3 * d + 2]))
    for copy in small + loads:
        copy.start()

    barrier = pltpu.get_barrier_semaphore()
    sx, sy = sub // 16, lax.rem(sxy, 2)
    x_at = [16 * lax.rem(sx + k, 4) for k in range(4)]
    y_at = [8 * lax.rem(sy + k, 2) for k in range(2)]
    z_at = [lax.rem(sz + k, 8) for k in range(8)]
    xy_at = {(x, y): x_at[x] + y_at[y] for x in range(4) for y in range(2)}
    dist_at = [lax.rem(dist + k, DISTS) for k in range(DISTS)]
    order = offsets_by_hops()
    peers = [xy_at[x, y] + z_at[z] for x, y, z in order[:-1]]
    level = [xy_at[x, y] for x, y, z in order if z == 0]
    ring = [z_at[k] for k in (4, 3, 5, 2, 6, 1, 7)]

    def hello(device):
        pl.semaphore_signal(barrier, inc=1, device_id=device, device_id_type=MESH)

    for peer in peers:
        hello({"sub": peer})
    for at in level:
        for k in range(1, DISTS):
            hello({"district": dist_at[k], "sub": at + sz})
    for k in range(1, DISTS):
        hello({"district": dist_at[k], "sub": 2 * pair + 1 - side})

    def whole(buf, send_sem, recv_sem):
        return pltpu.make_async_remote_copy(
            src_ref=buf,
            dst_ref=buf,
            send_sem=send_sem,
            recv_sem=recv_sem,
            device_id={"sub": sub},
            device_id_type=MESH,
        )

    for copy in small:
        copy.wait()
    place = iota((4, BLOCK), 1) + sub * BLOCK
    told = [near_in[d] - place for d in range(2)] + [owner_in[...], jnp.zeros((6, BLOCK), jnp.int32)]
    told = jnp.concatenate(told, axis=0).astype(F32)
    meta[...] = jnp.concatenate([told, jnp.zeros((16, BLOCK), F32)], axis=1).astype(BF16)
    mbuf[2 * REACH + side] = meta[...]
    here = rel[pair]
    here = jnp.where(side == 0, here[:, 0:BLOCK], here[:, BLOCK:PAIR]) // BLOCK
    own_block = jnp.concatenate([here[0:1], here[1:2]], axis=1)

    first = []
    for d in range(2):
        for copy in loads[3 * d : 3 * d + 3]:
            copy.wait()
        cs_d = dot(X[d], S[d])
        cs[d * BLOCK : (d + 1) * BLOCK] = cs_d
        first.append(dot_tb((-cs_d).astype(BF16), C[d]).astype(BF16))
    first = jnp.concatenate(first, axis=0)
    first = jnp.concatenate([first, jnp.zeros((2 * BLOCK, LANES - INTERFACE), BF16)], axis=1)
    lane = iota((2 * BLOCK, 2 * BLOCK), 1)
    row = iota((2 * BLOCK, 2 * BLOCK), 0)
    to_dest = jnp.where(own_block + BLOCK * (lane // BLOCK) == row, 1.0, 0.0).astype(BF16)
    eye = jnp.where(lane == row, 1.0, 0.0).astype(BF16)
    sorted_rows = dot(to_dest, first).astype(BF16)
    for d in range(2):
        send1[d, 0:REACH] = jnp.zeros((REACH, 2, LANES), BF16)
        send1[d, REACH + PAIRS : PAIRS + 2 * REACH] = jnp.zeros((REACH, 2, LANES), BF16)
        send1[d, REACH : REACH + PAIRS] = sorted_rows[d * BLOCK : (d + 1) * BLOCK].reshape(
            PAIRS, 2, LANES
        )

    pl.semaphore_wait(barrier, PEERS + OTHERS)

    for k in range(2 * SLAB):
        a, e = k // 2, k % 2

        def meta_copy():
            pltpu.make_async_remote_copy(
                src_ref=meta,
                dst_ref=mbuf.at[4 * REACH - 2 * a + side],
                send_sem=sm,
                recv_sem=rm,
                device_id={"sub": 2 * lax.rem(pair + a - REACH + PAIRS, PAIRS) + e},
                device_id_type=MESH,
            ).start()

        if a == REACH:
            pl.when(side != e)(meta_copy)
        else:
            meta_copy()

    def slot_of(device):
        return lax.rem(device, 2) * PAIRS + device // 2

    slot = slot_of(sub)
    for peer in peers:
        pltpu.make_async_remote_copy(
            src_ref=send1.at[lax.rem(peer, 2), pl.ds(peer // 2, SLAB)],
            dst_ref=recv1.at[slot],
            send_sem=s1,
            recv_sem=r1,
            device_id={"sub": peer},
            device_id_type=MESH,
        ).start()
    recv1[slot_of(sub)] = send1[side, pl.ds(pair, SLAB)]

    back_at = 4 * (own_block // 2) + 2 * (lane // BLOCK) + lax.rem(own_block, 2)
    p5[...] = dot_ta(jnp.where(back_at == row, 1.0, 0.0).astype(BF16), eye).astype(BF16)
    for d in range(2):
        cts_d = dot(C[d], S[d]).astype(BF16)
        cts[d] = cts_d
        m_d = dot_tb(cts_d, C[d])
        mp[d] = jnp.zeros((LANES, LANES), BF16)
        mp[d, 0:INTERFACE, 0:INTERFACE] = (-STEP * m_d).astype(BF16)
        ri = iota((LANES - INTERFACE, LANES - 128), 0)
        li = iota((LANES - INTERFACE, LANES - 128), 1)
        shift = jnp.where(li - (INTERFACE - 128) == ri + RES, 1.0, 0.0)
        mp[d, INTERFACE:LANES, 128:LANES] = shift.astype(BF16)
        vfull[d, 0:INTERFACE] = cts_d

    by_pair = rel[...].reshape(SUBS, PAIR)
    si, sj = iota((SUBS, SUBS), 0), iota((SUBS, SUBS), 1)
    pick = jnp.where((si // 2 == sj // 2) & (lax.rem(si, 2) == side), 1.0, 0.0).astype(BF16)

    def turned(values):
        flat = dot_ta(values.astype(F32).astype(BF16), pick)
        return jnp.concatenate([flat[0:BLOCK], flat[BLOCK:PAIR]], axis=1).astype(jnp.int32)

    block_of, place_in = turned(by_pair // BLOCK), turned(lax.rem(by_pair, BLOCK))
    odd = lax.rem(iota((1, PAIR), 1), 2)

    def place_map(a):
        hit = block_of == 2 * (pair + a - REACH) + odd
        at = jnp.sum(jnp.where(hit, place_in + 1, 0), axis=0, keepdims=True) - 1
        at = jnp.where(at >= 0, at + BLOCK * odd, -1)
        return jnp.where(at == row, 1.0, 0.0).astype(BF16)

    p4t[...] = dot_ta(place_map(REACH), eye).astype(BF16)

    whole(mbuf.at[pl.ds(0, 2 * SLAB - 1)], sm, rm).wait_recv()
    eye64 = jnp.where(
        iota((BLOCK, 128), 0) == iota((BLOCK, 128), 1), 1.0, 0.0
    ).astype(BF16)
    for m in range(2 * SLAB):
        cols = dot_tb(eye64, mbuf[m])
        top = m * BLOCK
        offs[top : top + BLOCK, 0:4] = jnp.where(side == 0, cols[:, 0:4], cols[:, 4:8])
        offs[top : top + BLOCK, 4:5] = jnp.where(side == 0, cols[:, 8:9], cols[:, 9:10])
    diff = (iota((LANES, LANES), 1) - iota((LANES, LANES), 0)).astype(F32)
    for i in range(3):
        cols = offs[192 * i : 192 * i + 256]
        near = jnp.where(diff == 0.0, 1.0, 0.0)
        for k in range(4):
            near = near - jnp.where(diff == cols[:, k : k + 1], 0.25, 0.0)
        near = near.astype(BF16)
        L2[i] = dot(near, near)[32:224].astype(BF16)
        if i == 1:
            lown[...] = near[64:192]

    sacc[...] = jnp.zeros((256, LANES), F32)
    whole(recv1.at[pl.ds(0, PEERS)], s1, r1).wait_recv()
    lane_e = iota((PAIR, 128), 1) - (INTERFACE - 128)
    for a in range(SLAB):
        arrived = recv1[:, a].reshape(2 * SUBS, LANES)
        part = dot(place_map(a), arrived)
        top = a * PAIR
        owner = offs[top : top + PAIR, 4:5].astype(jnp.int32)
        mark = jnp.where((lane_e == owner) & (lane_e >= 0) & (lane_e < RES), 1.0, 0.0)
        low, high = part[:, 0:128], part[:, 128:LANES] + mark
        zf[top : top + PAIR, 0:128] = low
        zf[top : top + PAIR, 128:LANES] = high
        zb[top : top + PAIR, 0:128] = low.astype(BF16)
        zb[top : top + PAIR, 128:LANES] = high.astype(BF16)
    sacc[32:224] = zf[224:416]
    usum[...] = jnp.zeros((PAIR, LANES), F32)
    flow_map = mp.at[side]

    def half(i):
        u = dot(L2[i], zb[192 * i : 192 * i + 256])
        if i == 1:
            usum[...] += u[32:160]
        return u.astype(BF16)

    def advance(i, u):
        at = 32 + 192 * i
        z = zf[at : at + 192] + dot(u, flow_map[...])
        zf[at : at + 192] = z
        zb[at : at + 192] = z.astype(BF16)
        if i == 1:
            sacc[32:224] += z

    def step():
        us = [half(i) for i in range(3)]
        for i, u in enumerate(us):
            advance(i, u)

    def full_step(_, carry):
        step()
        return carry

    def own_part(with_lanes):
        marked = zb[OWN : OWN + PAIR, INTERFACE : INTERFACE + RES]
        return dot_ta(marked, with_lanes)

    def to_z(buf, t, send_sem, recv_sem):
        for z in ring:
            pltpu.make_async_remote_copy(
                src_ref=buf.at[t, sz],
                dst_ref=buf.at[t, sz],
                send_sem=send_sem.at[t],
                recv_sem=recv_sem.at[t],
                device_id={"sub": sxy * 8 + z},
                device_id_type=MESH,
            ).start()

    def start_b(t):
        here_b = dist * 8 + sxy
        for at in level:
            for k in (2, 1, 3, 0):
                if k == 0 and at is level[-1]:
                    continue
                pltpu.make_async_remote_copy(
                    src_ref=arb.at[t, here_b],
                    dst_ref=arb.at[t, here_b],
                    send_sem=sb.at[t],
                    recv_sem=rb.at[t],
                    device_id={"district": dist_at[k], "sub": at + sz},
                    device_id_type=MESH,
                ).start()

    def all_of(buf, t, count, send_sem, recv_sem):
        return whole(buf.at[t, pl.ds(0, count)], send_sem.at[t], recv_sem.at[t])

    def reduce_a(t, part):
        ara[t, sz] = folded(part)
        to_z(ara, t, sa, ra)

    def reduce_b(t):
        all_of(ara, t, 7, sa, ra).wait_recv()
        arb[t, dist * 8 + sxy] = jnp.sum(ara[t], axis=0)
        start_b(t)

    def reduce_end(t):
        all_of(arb, t, 31, sb, rb).wait_recv()
        return unfolded(jnp.sum(arb[t], axis=0))

    lax.fori_loop(0, 3, full_step, 0)
    reduce_a(0, own_part(zb[OWN : OWN + PAIR, 0:128]))
    marks = zb[OWN : OWN + PAIR, INTERFACE:LANES]
    aka[0, sz // 2] = folded(own_part(marks))

    def go_k(k, _):
        z = lax.rem(sz + 2 + 2 * k, 8)
        pltpu.make_async_remote_copy(
            src_ref=aka.at[0, sz // 2],
            dst_ref=aka.at[0, sz // 2],
            send_sem=ska,
            recv_sem=rka,
            device_id={"sub": sxy * 8 + z},
            device_id_type=MESH,
        ).start()
        return 0

    lax.fori_loop(0, 3, go_k, 0)
    near_marks = dot(lown[...], zb[192:448])[:, INTERFACE:LANES].astype(BF16)
    step()
    step()
    step()

    u = half(1)
    prices = (STEP * usum[...]).astype(BF16)
    back = jnp.concatenate([prices[:, 0:INTERFACE], marks], axis=1)
    send2[...] = dot(p4t[...], back).astype(BF16).reshape(SUBS, 2, LANES)

    for peer in peers:
        pltpu.make_async_remote_copy(
            src_ref=send2.at[slot_of(peer)],
            dst_ref=recv2.at[sub],
            send_sem=s2,
            recv_sem=r2,
            device_id={"sub": peer},
            device_id_type=MESH,
        ).start()
    recv2[sub] = send2[slot_of(sub)]

    advance(1, u)
    reduce_a(1, own_part(zb[OWN : OWN + PAIR, 0:128]))
    price0 = dot(lown[...], sacc[...].astype(BF16))[:, 0:INTERFACE]

    reduce_b(0)
    whole(aka.at[0, pl.ds(0, 3)], ska, rka).wait_recv()
    akb[0, sxy] = jnp.sum(aka[0], axis=0)

    def go_kb(k, _):
        xy = lax.rem(sxy + k, 8)
        pltpu.make_async_remote_copy(
            src_ref=akb.at[0, sxy],
            dst_ref=akb.at[0, sxy],
            send_sem=skb,
            recv_sem=rkb,
            device_id={"sub": xy * 8 + sz},
            device_id_type=MESH,
        ).start()
        return 0

    lax.fori_loop(1, 8, go_kb, 0)
    reduce_b(1)
    capacity = cap[...]
    scale = 1.0 / math.sqrt(DISTS * 2 * SUBS * BLOCK / (2 * RES))
    duals = (reduce_end(0)[:, 0:HORIZON] - capacity) * scale
    wide = jnp.concatenate([duals, jnp.zeros((RES, INTERFACE - HORIZON), F32)], axis=1)

    binom = (1.0, 3.0, 3.0, 1.0)
    in_price = (1.0, -0.9, 0.27, -0.027)
    in_flow = (-1.0, 0.9, -0.27, 0.027)
    in_sum = (-4.0, 1.8, -0.36, 0.027)

    def powers_of(m_ref, count):
        powers = [wide]
        for _ in range(count):
            powers.append(
                dot(powers[-1].astype(BF16), m_ref[0:INTERFACE, 0:INTERFACE]) * (-1.0 / STEP)
            )
        return powers

    def stack(powers, weights):
        return jnp.concatenate(
            [p * (w / b) for p, w, b in zip(powers, weights, binom)], axis=0
        ).astype(BF16)

    powers = powers_of(flow_map, 4)
    whole(akb.at[0, pl.ds(0, 7)], skb, rkb).wait_recv()
    unit = unfolded(jnp.sum(akb[0], axis=0)).astype(BF16)
    here_c = dist * 2 + side
    arc[here_c] = folded(dot(unit, stack(powers[1:], in_flow))[:, 0:128])

    def go_c(k, _):
        there = lax.rem(here_c + k, 8)
        pltpu.make_async_remote_copy(
            src_ref=arc.at[here_c],
            dst_ref=arc.at[here_c],
            send_sem=sc,
            recv_sem=rc,
            device_id={"district": there // 2, "sub": 2 * pair + lax.rem(there, 2)},
            device_id_type=MESH,
        ).start()
        return 0

    lax.fori_loop(1, 8, go_c, 0)
    final_price = STEP * (price0 + dot(near_marks, stack(powers[1:], in_sum)))
    halves = [final_price[0:BLOCK], final_price[BLOCK:PAIR]]
    price_s[...] = jnp.where(side == 0, halves[1], halves[0])
    price_copy = pltpu.make_async_remote_copy(
        src_ref=price_s,
        dst_ref=price_r,
        send_sem=sp,
        recv_sem=rp,
        device_id={"sub": 2 * pair + 1 - side},
        device_id_type=MESH,
    )
    price_copy.start()
    price_o[side] = jnp.where(side == 0, halves[0], halves[1])
    for d in range(2):
        powers_d = powers_of(mp.at[d], 3)
        vfull[d, INTERFACE:LANES] = dot(stack(powers_d, in_price), cts[d]).astype(BF16)

    whole(recv2.at[pl.ds(0, PEERS)], s2, r2).wait_recv()
    mine = dot(p5[...], recv2[...].reshape(2 * SUBS, LANES)).astype(BF16)
    for d in range(2):
        at = d * BLOCK
        plan_o[d] = -(cs[at : at + BLOCK] + dot(mine[at : at + BLOCK], vfull[d]))

    price_copy.wait_recv()
    price_o[1 - side] = price_r[...]
    draws0 = reduce_end(1)[:, 0:HORIZON]
    whole(arc.at[pl.ds(0, 7)], sc, rc).wait_recv()
    draws1 = unfolded(jnp.sum(arc[...], axis=0))[:, 0:HORIZON]
    dual_o[...] = duals + (draws0 + draws1 - capacity) * scale

    whole(mbuf.at[pl.ds(0, 2 * SLAB - 1)], sm, rm).wait_send()
    whole(recv1.at[pl.ds(0, PEERS)], s1, r1).wait_send()
    whole(recv2.at[pl.ds(0, PEERS)], s2, r2).wait_send()
    for t in range(2):
        all_of(ara, t, 7, sa, ra).wait_send()
        all_of(arb, t, 31, sb, rb).wait_send()
    whole(aka.at[0, pl.ds(0, 3)], ska, rka).wait_send()
    whole(akb.at[0, pl.ds(0, 7)], skb, rkb).wait_send()
    whole(arc.at[pl.ds(0, 7)], sc, rc).wait_send()
    price_copy.wait_send()


def write_out(plan, price, dual, plan_o, price_o, dual_o, sems):
    copies = [
        pltpu.make_async_copy(src, dst, sems.at[i])
        for i, (src, dst) in enumerate(((plan, plan_o), (price, price_o), (dual, dual_o)))
    ]
    for copy in copies:
        copy.start()
    for copy in copies:
        copy.wait()


def on_device(cost_terms, neighbours, relayout, ownership, capacity, coupling, solve_factor):
    pairs = relayout.reshape(2, SUBS // 2, 2 * BLOCK).transpose(1, 0, 2)
    vmem = pl.BlockSpec(memory_space=pltpu.VMEM)
    hbm = pl.BlockSpec(memory_space=pltpu.HBM)
    dma = pltpu.SemaphoreType.DMA
    parts = pl.pallas_call(
        kernel,
        out_shape=(
            pltpu.VMEM((2, BLOCK, UNKNOWNS), F32),
            pltpu.VMEM((2, BLOCK, INTERFACE), F32),
            pltpu.VMEM((RES, HORIZON), F32),
        ),
        in_specs=[hbm] * 7,
        out_specs=(vmem,) * 3,
        scratch_shapes=[
            pltpu.VMEM((2, BLOCK, UNKNOWNS), BF16),
            pltpu.VMEM((2, UNKNOWNS, UNKNOWNS), BF16),
            pltpu.VMEM((2, INTERFACE, UNKNOWNS), BF16),
            pltpu.VMEM((2 * BLOCK, UNKNOWNS), F32),
            pltpu.VMEM((2, LANES, UNKNOWNS), BF16),
            pltpu.VMEM((SUBS // 2, 2, 2 * BLOCK), jnp.int32),
            pltpu.VMEM((2, 4, BLOCK), jnp.int32),
            pltpu.VMEM((2, BLOCK), jnp.int32),
            pltpu.VMEM((RES, HORIZON), F32),
            pltpu.VMEM((16, 128), BF16),
            pltpu.VMEM((2, INTERFACE, UNKNOWNS), BF16),
            pltpu.VMEM((2, PAIRS + 2 * REACH, 2, LANES), BF16),
            pltpu.VMEM((SUBS, SLAB, 2, LANES), BF16),
            pltpu.VMEM((SUBS, 2, LANES), BF16),
            pltpu.VMEM((SUBS, 2, LANES), BF16),
            pltpu.VMEM((2 * SLAB, 16, 128), BF16),
            pltpu.VMEM((ROWS, 8), F32),
            pltpu.VMEM((3, 192, 256), BF16),
            pltpu.VMEM((PAIR, 256), BF16),
            pltpu.VMEM((128, 128), BF16),
            pltpu.VMEM((128, 128), BF16),
            pltpu.VMEM((2, LANES, LANES), BF16),
            pltpu.VMEM((ROWS, LANES), F32),
            pltpu.VMEM((ROWS, LANES), BF16),
            pltpu.VMEM((256, LANES), F32),
            pltpu.VMEM((PAIR, LANES), F32),
            pltpu.VMEM((2, 8, 8, 128), F32),
            pltpu.VMEM((2, 32, 8, 128), F32),
            pltpu.VMEM((1, 4, 8, 128), F32),
            pltpu.VMEM((1, 8, 8, 128), F32),
            pltpu.VMEM((8, 8, 128), F32),
            pltpu.VMEM((BLOCK, INTERFACE), F32),
            pltpu.VMEM((BLOCK, INTERFACE), F32),
            dma((10,)),
            dma, dma, dma, dma, dma, dma, dma, dma,
            dma((2,)), dma((2,)), dma((2,)), dma((2,)),
            dma, dma, dma, dma, dma, dma,
        ],
        compiler_params=pltpu.CompilerParams(
            collective_id=0, has_side_effects=True, vmem_limit_bytes=VMEM_LIMIT
        ),
    )(
        cost_terms, coupling.transpose(0, 2, 1), solve_factor, pairs,
        neighbours.transpose(0, 2, 1), ownership, capacity,
    )
    return pl.pallas_call(
        write_out,
        out_shape=(
            jax.ShapeDtypeStruct((2, BLOCK, UNKNOWNS), F32),
            jax.ShapeDtypeStruct((2, BLOCK, INTERFACE), F32),
            jax.ShapeDtypeStruct((RES, HORIZON), F32),
        ),
        in_specs=[vmem] * 3,
        out_specs=(hbm,) * 3,
        scratch_shapes=[dma((3,))],
        compiler_params=pltpu.CompilerParams(vmem_limit_bytes=1024 * 1024),
    )(*parts)


def solution(mesh):
    placed = (
        P("district", "sub", None),
        P("district", "sub", None),
        P("district", None),
        P("district", "sub"),
        P(),
        P("district", None, None),
        P("district", None, None),
    )
    return jax.shard_map(
        on_device,
        mesh=mesh,
        in_specs=placed,
        out_specs=(P("district", "sub", None), P("district", "sub", None), P()),
        check_vma=False,
    )
```

```python
import math

import jax
import jax.numpy as jnp
from jax import lax
from jax.experimental import pallas as pl
from jax.experimental.pallas import tpu as pltpu
from jax.sharding import PartitionSpec as P

MESH = pl.DeviceIdType.MESH
F32, BF16 = jnp.float32, jnp.bfloat16
HORIZON, UNKNOWNS, INTERFACE, BLOCK = 48, 768, 192, 64
RES, SUBS, DISTS = 16, 64, 4
PAIRS = SUBS // 2
REACH = 2
SLAB = 2 * REACH + 1
PAIR = 2 * BLOCK
ROWS = SLAB * PAIR
OWN = REACH * PAIR
LANES = 256
STEP = 0.3
PEERS = SUBS - 1
OTHERS = 27
VMEM_LIMIT = 67043328 - 700 * 1024


def dot(a, b):
    return jnp.dot(a, b, preferred_element_type=F32)


def dot_ta(a, b):
    return lax.dot_general(a, b, (((0,), (0,)), ((), ())), preferred_element_type=F32)


def dot_tb(a, b):
    return lax.dot_general(a, b, (((1,), (1,)), ((), ())), preferred_element_type=F32)


def two_parts(x):
    high = x.astype(BF16)
    return jnp.concatenate([high, (x - high.astype(F32)).astype(BF16)], axis=0)


def dot2(x, b):
    out = dot(two_parts(x), b)
    return out[: x.shape[0]] + out[x.shape[0] :]


def iota(shape, dim):
    return lax.broadcasted_iota(jnp.int32, shape, dim)


def offsets_by_hops():
    def hops(at):
        x, y, z = at
        return min(x, 4 - x) + 2 * y + min(z, 8 - z)

    every = [(x, y, z) for z in range(8) for x in range(4) for y in range(2)]
    return sorted(every, key=lambda at: (-hops(at), at))


def folded(part):
    return jnp.concatenate([part[0:8, 0:64], part[8:16, 0:64]], axis=1)


def unfolded(part):
    return jnp.concatenate([part[:, 0:64], part[:, 64:128]], axis=0)


def kernel(
    cost, coup, solve, rel_h, near_h, owner_h, cap_h,
    plan_o, price_o, dual_o,
    X, S, C, cs, vfull, rel, near_in, owner_in, cap, meta, cts, send1, recv1, send2, recv2,
    mbuf, offs, L2, lown, p4t, p5, mp, zf, zb, sacc, usum, ara, arb, aka, akb, arc, price_s, price_r,

    load_sem, s1, r1, s2, r2, sm, rm, sp, rp, sa, ra, sb, rb, ska, rka, skb, rkb, sc, rc, se, re,
):
    sub = lax.axis_index("sub")
    dist = lax.axis_index("district")
    sxy, sz = sub // 8, lax.rem(sub, 8)
    pair, side = sub // 2, lax.rem(sub, 2)

    small = [
        pltpu.make_async_copy(src, dst, load_sem.at[6 + i])
        for i, (src, dst) in enumerate(
            ((rel_h, rel), (near_h, near_in), (owner_h, owner_in), (cap_h, cap))
        )
    ]
    loads = []
    for d in range(2):
        loads.append(pltpu.make_async_copy(cost.at[d], X.at[d], load_sem.at[3 * d]))
        loads.append(pltpu.make_async_copy(solve.at[d], S.at[d], load_sem.at[3 * d + 1]))
        loads.append(pltpu.make_async_copy(coup.at[d], C.at[d], load_sem.at[3 * d + 2]))
    for copy in small + loads:
        copy.start()

    barrier = pltpu.get_barrier_semaphore()
    sx, sy = sub // 16, lax.rem(sxy, 2)
    x_at = [16 * lax.rem(sx + k, 4) for k in range(4)]
    y_at = [8 * lax.rem(sy + k, 2) for k in range(2)]
    z_at = [lax.rem(sz + k, 8) for k in range(8)]
    xy_at = {(x, y): x_at[x] + y_at[y] for x in range(4) for y in range(2)}
    dist_at = [lax.rem(dist + k, DISTS) for k in range(DISTS)]
    order = offsets_by_hops()
    peers = [xy_at[x, y] + z_at[z] for x, y, z in order[:-1]]
    level = [xy_at[x, y] for x, y, z in order if z == 0]
    ring = [z_at[k] for k in (4, 3, 5, 2, 6, 1, 7)]

    def hello(device):
        pl.semaphore_signal(barrier, inc=1, device_id=device, device_id_type=MESH)

    for peer in peers:
        hello({"sub": peer})
    for at in level:
        for k in range(1, DISTS):
            hello({"district": dist_at[k], "sub": at + sz})
    for k in range(1, DISTS):
        hello({"district": dist_at[k], "sub": 2 * pair + 1 - side})

    def whole(buf, send_sem, recv_sem):
        return pltpu.make_async_remote_copy(
            src_ref=buf,
            dst_ref=buf,
            send_sem=send_sem,
            recv_sem=recv_sem,
            device_id={"sub": sub},
            device_id_type=MESH,
        )

    for copy in small:
        copy.wait()
    place = iota((4, BLOCK), 1) + sub * BLOCK
    for d in range(2):
        told = [near_in[d] - place, owner_in[d : d + 1], jnp.zeros((11, BLOCK), jnp.int32)]
        told = jnp.concatenate(told, axis=0).astype(F32)
        meta[d] = jnp.concatenate([told, jnp.zeros((16, BLOCK), F32)], axis=1).astype(BF16)
    mbuf[2 * REACH + side] = meta[side]
    here = rel[pair]
    here = jnp.where(side == 0, here[:, 0:BLOCK], here[:, BLOCK:PAIR]) // BLOCK
    own_block = jnp.concatenate([here[0:1], here[1:2]], axis=1)

    first = []
    for d in range(2):
        for copy in loads[3 * d : 3 * d + 3]:
            copy.wait()
        cs_d = dot(X[d], S[d])
        cs[d * BLOCK : (d + 1) * BLOCK] = cs_d
        first.append(dot_tb((-cs_d).astype(BF16), C[d]).astype(BF16))
    first = jnp.concatenate(first, axis=0)
    first = jnp.concatenate([first, jnp.zeros((2 * BLOCK, LANES - INTERFACE), BF16)], axis=1)
    lane = iota((2 * BLOCK, 2 * BLOCK), 1)
    row = iota((2 * BLOCK, 2 * BLOCK), 0)
    to_dest = jnp.where(own_block + BLOCK * (lane // BLOCK) == row, 1.0, 0.0).astype(BF16)
    eye = jnp.where(lane == row, 1.0, 0.0).astype(BF16)
    sorted_rows = dot(to_dest, first).astype(BF16)
    for d in range(2):
        send1[d, 0:REACH] = jnp.zeros((REACH, 2, LANES), BF16)
        send1[d, REACH + PAIRS : PAIRS + 2 * REACH] = jnp.zeros((REACH, 2, LANES), BF16)
        send1[d, REACH : REACH + PAIRS] = sorted_rows[d * BLOCK : (d + 1) * BLOCK].reshape(
            PAIRS, 2, LANES
        )

    pl.semaphore_wait(barrier, PEERS + OTHERS)

    for k in range(2 * SLAB):
        a, e = k // 2, k % 2

        def meta_copy():
            pltpu.make_async_remote_copy(
                src_ref=meta.at[e],
                dst_ref=mbuf.at[4 * REACH - 2 * a + side],
                send_sem=sm,
                recv_sem=rm,
                device_id={"sub": 2 * lax.rem(pair + a - REACH + PAIRS, PAIRS) + e},
                device_id_type=MESH,
            ).start()

        if a == REACH:
            pl.when(side != e)(meta_copy)
        else:
            meta_copy()

    def slot_of(device):
        return lax.rem(device, 2) * PAIRS + device // 2

    slot = slot_of(sub)
    for peer in peers:
        pltpu.make_async_remote_copy(
            src_ref=send1.at[lax.rem(peer, 2), REACH + peer // 2],
            dst_ref=recv1.at[slot, REACH],
            send_sem=se,
            recv_sem=re,
            device_id={"sub": peer},
            device_id_type=MESH,
        ).start()
    for peer in peers:
        for first in (0, REACH + 1):
            pltpu.make_async_remote_copy(
                src_ref=send1.at[lax.rem(peer, 2), pl.ds(peer // 2 + first, REACH)],
                dst_ref=recv1.at[slot, pl.ds(first, REACH)],
                send_sem=s1,
                recv_sem=r1,
                device_id={"sub": peer},
                device_id_type=MESH,
            ).start()
    recv1[slot] = send1[side, pl.ds(pair, SLAB)]

    back_at = 4 * (own_block // 2) + 2 * (lane // BLOCK) + lax.rem(own_block, 2)
    p5[...] = dot_ta(jnp.where(back_at == row, 1.0, 0.0).astype(BF16), eye).astype(BF16)
    for d in range(2):
        cts_d = dot(C[d], S[d]).astype(BF16)
        cts[d] = cts_d
        m_d = dot_tb(cts_d, C[d])
        mp[d] = jnp.zeros((LANES, LANES), BF16)
        mp[d, 0:INTERFACE, 0:INTERFACE] = (-STEP * m_d).astype(BF16)
        ri = iota((LANES - INTERFACE, LANES - 128), 0)
        li = iota((LANES - INTERFACE, LANES - 128), 1)
        shift = jnp.where(li - (INTERFACE - 128) == ri + RES, 1.0, 0.0)
        mp[d, INTERFACE:LANES, 128:LANES] = shift.astype(BF16)
        vfull[d, 0:INTERFACE] = cts_d

    by_pair = rel[...].reshape(SUBS, PAIR)
    si, sj = iota((SUBS, SUBS), 0), iota((SUBS, SUBS), 1)
    pick = jnp.where((si // 2 == sj // 2) & (lax.rem(si, 2) == side), 1.0, 0.0).astype(BF16)

    def turned(values):
        flat = dot_ta(values.astype(F32).astype(BF16), pick)
        return jnp.concatenate([flat[0:BLOCK], flat[BLOCK:PAIR]], axis=1).astype(jnp.int32)

    block_of, place_in = turned(by_pair // BLOCK), turned(lax.rem(by_pair, BLOCK))
    odd = lax.rem(iota((1, PAIR), 1), 2)

    def place_map(a):
        hit = block_of == 2 * (pair + a - REACH) + odd
        at = jnp.sum(jnp.where(hit, place_in + 1, 0), axis=0, keepdims=True) - 1
        at = jnp.where(at >= 0, at + BLOCK * odd, -1)
        return jnp.where(at == row, 1.0, 0.0).astype(BF16)

    own_map = place_map(REACH)
    p4t[...] = dot_ta(own_map, eye).astype(BF16)

    whole(mbuf.at[pl.ds(0, 2 * SLAB - 1)], sm, rm).wait_recv()
    eye64 = jnp.where(
        iota((BLOCK, 128), 0) == iota((BLOCK, 128), 1), 1.0, 0.0
    ).astype(BF16)
    for m in range(2 * SLAB):
        offs[m * BLOCK : (m + 1) * BLOCK] = dot_tb(eye64, mbuf[m])
    diff = (iota((LANES, LANES), 1) - iota((LANES, LANES), 0)).astype(F32)
    for i in range(3):
        cols = offs[192 * i : 192 * i + 256]
        near = jnp.where(diff == 0.0, 1.0, 0.0)
        for k in range(4):
            near = near - jnp.where(diff == cols[:, k : k + 1], 0.25, 0.0)
        near = near.astype(BF16)
        L2[i, 32:224] = dot(near, near)[32:224].astype(BF16)
        L2[i, 0:32] = jnp.zeros((32, 256), BF16)
        L2[i, 224:256] = jnp.zeros((32, 256), BF16)
        if i == 1:
            lown[...] = near[64:192]

    def to_z(buf, t, send_sem, recv_sem):
        for z in ring:
            pltpu.make_async_remote_copy(
                src_ref=buf.at[t, sz],
                dst_ref=buf.at[t, sz],
                send_sem=send_sem.at[t],
                recv_sem=recv_sem.at[t],
                device_id={"sub": sxy * 8 + z},
                device_id_type=MESH,
            ).start()

    def start_b(t):
        here_b = dist * 8 + sxy
        for at in level:
            for k in (2, 1, 3, 0):
                if k == 0 and at is level[-1]:
                    continue
                pltpu.make_async_remote_copy(
                    src_ref=arb.at[t, here_b],
                    dst_ref=arb.at[t, here_b],
                    send_sem=sb.at[t],
                    recv_sem=rb.at[t],
                    device_id={"district": dist_at[k], "sub": at + sz},
                    device_id_type=MESH,
                ).start()

    def all_of(buf, t, count, send_sem, recv_sem):
        return whole(buf.at[t, pl.ds(0, count)], send_sem.at[t], recv_sem.at[t])

    def reduce_a(t, part):
        ara[t, sz] = folded(part)
        to_z(ara, t, sa, ra)

    def reduce_b(t):
        all_of(ara, t, 7, sa, ra).wait_recv()
        arb[t, dist * 8 + sxy] = jnp.sum(ara[t], axis=0)
        start_b(t)

    def reduce_end(t):
        all_of(arb, t, 31, sb, rb).wait_recv()
        return unfolded(jnp.sum(arb[t], axis=0))

    flow_map = mp.at[side]
    owners = []
    for a in range(SLAB):
        owner = [mbuf[2 * a + e][4:5, 0:BLOCK].astype(F32) for e in range(2)]
        owner = jnp.concatenate(owner, axis=1)
        owners.append(jnp.where(iota((RES, PAIR), 0).astype(F32) == owner, 1.0, 0.0))
    own_owners = owners[REACH]
    half_tile = jnp.zeros((2 * RES, BLOCK), F32)

    def back_step(tiles):
        rows2 = jnp.concatenate([two_parts(t) for t in tiles], axis=1)
        out0 = dot(rows2[:, 0:256], L2[0])
        out1 = dot(rows2[:, 192:448], L2[1])
        out2 = dot(rows2[:, 384:640], L2[2])
        out1 = jnp.concatenate([half_tile, out1, half_tile], axis=1)
        sums = [
            out0[:, 0:128],
            out0[:, 128:256] + out1[:, 0:128],
            out1[:, 128:256],
            out1[:, 256:384] + out2[:, 0:128],
            out2[:, 128:256],
        ]
        return [t[0:RES] + t[RES : 2 * RES] for t in sums]

    def seen_flows(weights):
        turned_weights = dot(two_parts(weights), own_map).astype(BF16)
        sums = dot(turned_weights, recv1[:, REACH].reshape(2 * SUBS, LANES))[:, 0:INTERFACE]
        sums = sums[0:BLOCK] + sums[BLOCK : 2 * BLOCK]
        return [sums[RES * j : RES * (j + 1)] for j in range(4)]

    def draws_of(seen, count):
        total = seen[count]
        for j in reversed(range(count)):
            total = dot2(total, flow_map[0:INTERFACE, 0:INTERFACE])
            total = total + seen[j] * float(math.comb(count, j))
        return total[:, 0:128]

    weights, tiles = [own_owners], owners
    for _ in range(3):
        tiles = back_step(tiles)
        weights.append(tiles[REACH])
    weights = jnp.concatenate(weights, axis=0)
    unit = dot_tb(two_parts(weights), own_owners.astype(BF16))
    unit = unit[0:BLOCK] + unit[BLOCK : 2 * BLOCK]
    unit = [unit[RES * j : RES * (j + 1), 0:RES] for j in range(4)]
    aka[0, sz // 2] = folded(jnp.concatenate(unit, axis=1))
    whole(recv1.at[pl.ds(0, PEERS), REACH], se, re).wait_recv()
    seen = seen_flows(weights)
    reduce_a(0, draws_of(seen, 3))

    def go_k(k, _):
        z = lax.rem(sz + 2 + 2 * k, 8)
        pltpu.make_async_remote_copy(
            src_ref=aka.at[0, sz // 2],
            dst_ref=aka.at[0, sz // 2],
            send_sem=ska,
            recv_sem=rka,
            device_id={"sub": sxy * 8 + z},
            device_id_type=MESH,
        ).start()
        return 0

    lax.fori_loop(0, 3, go_k, 0)
    weights = []
    for _ in range(4):
        tiles = back_step(tiles)
        weights.append(tiles[REACH])
    weights = jnp.concatenate(weights, axis=0)
    seen = seen + seen_flows(weights)
    reduce_a(1, draws_of(seen, 7))

    sacc[...] = jnp.zeros((256, LANES), F32)
    whole(recv1.at[pl.ds(0, PEERS), pl.ds(0, 2 * REACH)], s1, r1).wait_recv()
    lane_e = iota((PAIR, 128), 1) - (INTERFACE - 128)
    for a in range(SLAB):
        arrived = recv1[:, a].reshape(2 * SUBS, LANES)
        part = dot(place_map(a), arrived)
        top = a * PAIR
        owner = offs[top : top + PAIR, 4:5].astype(jnp.int32)
        mark = jnp.where((lane_e == owner) & (lane_e >= 0) & (lane_e < RES), 1.0, 0.0)
        low, high = part[:, 0:128], part[:, 128:LANES] + mark
        zf[top : top + PAIR, 0:128] = low
        zf[top : top + PAIR, 128:LANES] = high
        zb[top : top + PAIR, 0:128] = low.astype(BF16)
        zb[top : top + PAIR, 128:LANES] = high.astype(BF16)
    sacc[32:224] = zf[224:416]
    usum[...] = jnp.zeros((PAIR, LANES), F32)

    def half(i):
        u = dot(L2[i, 32:224], zb[192 * i : 192 * i + 256])
        if i == 1:
            usum[...] += u[32:160]
        return u.astype(BF16)

    def advance(i, u):
        at = 32 + 192 * i
        z = zf[at : at + 192] + dot(u, flow_map[...])
        zf[at : at + 192] = z
        zb[at : at + 192] = z.astype(BF16)
        if i == 1:
            sacc[32:224] += z

    def step():
        us = [half(i) for i in range(3)]
        for i, u in enumerate(us):
            advance(i, u)

    def full_step(_, carry):
        step()
        return carry

    lax.fori_loop(0, 3, full_step, 0)
    marks = zb[OWN : OWN + PAIR, INTERFACE:LANES]
    near_marks = dot(lown[...], zb[192:448])[:, INTERFACE:LANES].astype(BF16)
    step()
    step()
    step()
    reduce_b(0)

    u = half(1)
    prices = (STEP * usum[...]).astype(BF16)
    back = jnp.concatenate([prices[:, 0:INTERFACE], marks], axis=1)
    send2[...] = dot(p4t[...], back).astype(BF16).reshape(SUBS, 2, LANES)

    for peer in peers:
        pltpu.make_async_remote_copy(
            src_ref=send2.at[slot_of(peer)],
            dst_ref=recv2.at[sub],
            send_sem=s2,
            recv_sem=r2,
            device_id={"sub": peer},
            device_id_type=MESH,
        ).start()
    recv2[sub] = send2[slot_of(sub)]

    advance(1, u)
    price0 = dot(lown[...], sacc[...].astype(BF16))[:, 0:INTERFACE]

    whole(aka.at[0, pl.ds(0, 3)], ska, rka).wait_recv()
    akb[0, sxy] = jnp.sum(aka[0], axis=0)

    def go_kb(k, _):
        xy = lax.rem(sxy + k, 8)
        pltpu.make_async_remote_copy(
            src_ref=akb.at[0, sxy],
            dst_ref=akb.at[0, sxy],
            send_sem=skb,
            recv_sem=rkb,
            device_id={"sub": xy * 8 + sz},
            device_id_type=MESH,
        ).start()
        return 0

    lax.fori_loop(1, 8, go_kb, 0)
    reduce_b(1)
    capacity = cap[...]
    scale = 1.0 / math.sqrt(DISTS * 2 * SUBS * BLOCK / (2 * RES))
    duals = (reduce_end(0)[:, 0:HORIZON] - capacity) * scale
    wide = jnp.concatenate([duals, jnp.zeros((RES, INTERFACE - HORIZON), F32)], axis=1)

    binom = (1.0, 3.0, 3.0, 1.0)
    in_price = (1.0, -0.9, 0.27, -0.027)
    in_flow = (-1.0, 0.9, -0.27, 0.027)
    in_sum = (-4.0, 1.8, -0.36, 0.027)

    def powers_of(m_ref, count):
        powers = [wide]
        for _ in range(count):
            powers.append(dot2(powers[-1], m_ref[0:INTERFACE, 0:INTERFACE]) * (-1.0 / STEP))
        return powers

    def stack(powers, weights, counts=binom):
        return jnp.concatenate([p * (w / b) for p, w, b in zip(powers, weights, counts)], axis=0)

    powers = powers_of(flow_map, 4)
    whole(akb.at[0, pl.ds(0, 7)], skb, rkb).wait_recv()
    unit = unfolded(jnp.sum(akb[0], axis=0))
    here_c = dist * 2 + side
    caused = two_parts(stack(powers[1:], in_flow, (1.0,) * 4))
    caused = dot2(unit, caused[0:BLOCK]) + dot(unit.astype(BF16), caused[BLOCK:PAIR])
    arc[here_c] = folded(caused[:, 0:128])

    def go_c(k, _):
        there = lax.rem(here_c + k, 8)
        pltpu.make_async_remote_copy(
            src_ref=arc.at[here_c],
            dst_ref=arc.at[here_c],
            send_sem=sc,
            recv_sem=rc,
            device_id={"district": there // 2, "sub": 2 * pair + lax.rem(there, 2)},
            device_id_type=MESH,
        ).start()
        return 0

    lax.fori_loop(1, 8, go_c, 0)
    final_price = STEP * (price0 + dot(near_marks, stack(powers[1:], in_sum).astype(BF16)))
    halves = [final_price[0:BLOCK], final_price[BLOCK:PAIR]]
    price_s[...] = jnp.where(side == 0, halves[1], halves[0])
    price_copy = pltpu.make_async_remote_copy(
        src_ref=price_s,
        dst_ref=price_r,
        send_sem=sp,
        recv_sem=rp,
        device_id={"sub": 2 * pair + 1 - side},
        device_id_type=MESH,
    )
    price_copy.start()
    price_o[side] = jnp.where(side == 0, halves[0], halves[1])
    for d in range(2):
        powers_d = powers_of(mp.at[d], 3)
        vfull[d, INTERFACE:LANES] = dot(stack(powers_d, in_price).astype(BF16), cts[d]).astype(BF16)

    whole(recv2.at[pl.ds(0, PEERS)], s2, r2).wait_recv()
    mine = dot(p5[...], recv2[...].reshape(2 * SUBS, LANES)).astype(BF16)
    for d in range(2):
        at = d * BLOCK
        plan_o[d] = -(cs[at : at + BLOCK] + dot(mine[at : at + BLOCK], vfull[d]))

    price_copy.wait_recv()
    price_o[1 - side] = price_r[...]
    draws0 = reduce_end(1)[:, 0:HORIZON]
    whole(arc.at[pl.ds(0, 7)], sc, rc).wait_recv()
    draws1 = unfolded(jnp.sum(arc[...], axis=0))[:, 0:HORIZON]
    dual_o[...] = duals + (draws0 + draws1 - capacity) * scale

    whole(mbuf.at[pl.ds(0, 2 * SLAB - 1)], sm, rm).wait_send()
    whole(recv1.at[pl.ds(0, PEERS), pl.ds(0, 2 * REACH)], s1, r1).wait_send()
    whole(recv2.at[pl.ds(0, PEERS)], s2, r2).wait_send()
    for t in range(2):
        all_of(ara, t, 7, sa, ra).wait_send()
        all_of(arb, t, 31, sb, rb).wait_send()
    whole(aka.at[0, pl.ds(0, 3)], ska, rka).wait_send()
    whole(akb.at[0, pl.ds(0, 7)], skb, rkb).wait_send()
    whole(arc.at[pl.ds(0, 7)], sc, rc).wait_send()
    whole(recv1.at[pl.ds(0, PEERS), REACH], se, re).wait_send()
    price_copy.wait_send()


def write_out(plan, price, dual, plan_o, price_o, dual_o, sems):
    copies = [
        pltpu.make_async_copy(src, dst, sems.at[i])
        for i, (src, dst) in enumerate(((plan, plan_o), (price, price_o), (dual, dual_o)))
    ]
    for copy in copies:
        copy.start()
    for copy in copies:
        copy.wait()


def on_device(cost_terms, neighbours, relayout, ownership, capacity, coupling, solve_factor):
    pairs = relayout.reshape(2, SUBS // 2, 2 * BLOCK).transpose(1, 0, 2)
    vmem = pl.BlockSpec(memory_space=pltpu.VMEM)
    hbm = pl.BlockSpec(memory_space=pltpu.HBM)
    dma = pltpu.SemaphoreType.DMA
    parts = pl.pallas_call(
        kernel,
        out_shape=(
            pltpu.VMEM((2, BLOCK, UNKNOWNS), F32),
            pltpu.VMEM((2, BLOCK, INTERFACE), F32),
            pltpu.VMEM((RES, HORIZON), F32),
        ),
        in_specs=[hbm] * 7,
        out_specs=(vmem,) * 3,
        scratch_shapes=[
            pltpu.VMEM((2, BLOCK, UNKNOWNS), BF16),
            pltpu.VMEM((2, UNKNOWNS, UNKNOWNS), BF16),
            pltpu.VMEM((2, INTERFACE, UNKNOWNS), BF16),
            pltpu.VMEM((2 * BLOCK, UNKNOWNS), F32),
            pltpu.VMEM((2, LANES, UNKNOWNS), BF16),
            pltpu.VMEM((SUBS // 2, 2, 2 * BLOCK), jnp.int32),
            pltpu.VMEM((2, 4, BLOCK), jnp.int32),
            pltpu.VMEM((2, BLOCK), jnp.int32),
            pltpu.VMEM((RES, HORIZON), F32),
            pltpu.VMEM((2, 16, 128), BF16),
            pltpu.VMEM((2, INTERFACE, UNKNOWNS), BF16),
            pltpu.VMEM((2, PAIRS + 2 * REACH, 2, LANES), BF16),
            pltpu.VMEM((SUBS, SLAB, 2, LANES), BF16),
            pltpu.VMEM((SUBS, 2, LANES), BF16),
            pltpu.VMEM((SUBS, 2, LANES), BF16),
            pltpu.VMEM((2 * SLAB, 16, 128), BF16),
            pltpu.VMEM((ROWS, 16), F32),
            pltpu.VMEM((3, 256, 256), BF16),
            pltpu.VMEM((PAIR, 256), BF16),
            pltpu.VMEM((128, 128), BF16),
            pltpu.VMEM((128, 128), BF16),
            pltpu.VMEM((2, LANES, LANES), BF16),
            pltpu.VMEM((ROWS, LANES), F32),
            pltpu.VMEM((ROWS, LANES), BF16),
            pltpu.VMEM((256, LANES), F32),
            pltpu.VMEM((PAIR, LANES), F32),
            pltpu.VMEM((2, 8, 8, 128), F32),
            pltpu.VMEM((2, 32, 8, 128), F32),
            pltpu.VMEM((1, 4, 8, 128), F32),
            pltpu.VMEM((1, 8, 8, 128), F32),
            pltpu.VMEM((8, 8, 128), F32),
            pltpu.VMEM((BLOCK, INTERFACE), F32),
            pltpu.VMEM((BLOCK, INTERFACE), F32),
            dma((10,)),
            dma, dma, dma, dma, dma, dma, dma, dma,
            dma((2,)), dma((2,)), dma((2,)), dma((2,)),
            dma, dma, dma, dma, dma, dma, dma, dma,
        ],
        compiler_params=pltpu.CompilerParams(
            collective_id=0, has_side_effects=True, vmem_limit_bytes=VMEM_LIMIT
        ),
    )(
        cost_terms, coupling.transpose(0, 2, 1), solve_factor, pairs,
        neighbours.transpose(0, 2, 1), ownership, capacity,
    )
    return pl.pallas_call(
        write_out,
        out_shape=(
            jax.ShapeDtypeStruct((2, BLOCK, UNKNOWNS), F32),
            jax.ShapeDtypeStruct((2, BLOCK, INTERFACE), F32),
            jax.ShapeDtypeStruct((RES, HORIZON), F32),
        ),
        in_specs=[vmem] * 3,
        out_specs=(hbm,) * 3,
        scratch_shapes=[dma((3,))],
        compiler_params=pltpu.CompilerParams(vmem_limit_bytes=1024 * 1024),
    )(*parts)


def solution(mesh):
    placed = (
        P("district", "sub", None),
        P("district", "sub", None),
        P("district", None),
        P("district", "sub"),
        P(),
        P("district", None, None),
        P("district", None, None),
    )
    return jax.shard_map(
        on_device,
        mesh=mesh,
        in_specs=placed,
        out_specs=(P("district", "sub", None), P("district", "sub", None), P()),
        check_vma=False,
    )
```

```python
import math

import jax
import jax.numpy as jnp
from jax import lax
from jax.experimental import pallas as pl
from jax.experimental.pallas import tpu as pltpu
from jax.sharding import PartitionSpec as P

MESH = pl.DeviceIdType.MESH
F32, BF16 = jnp.float32, jnp.bfloat16
HORIZON, UNKNOWNS, INTERFACE, BLOCK = 48, 768, 192, 64
RES, SUBS, DISTS = 16, 64, 4
PAIRS = SUBS // 2
REACH = 2
SLAB = 2 * REACH + 1
PAIR = 2 * BLOCK
ROWS = SLAB * PAIR
OWN = REACH * PAIR
LANES = 256
STEP = 0.3
PEERS = SUBS - 1
OTHERS = 24
VMEM_LIMIT = 67043328 - 700 * 1024


def dot(a, b):
    return jnp.dot(a, b, preferred_element_type=F32)


def dot_ta(a, b):
    return lax.dot_general(a, b, (((0,), (0,)), ((), ())), preferred_element_type=F32)


def dot_tb(a, b):
    return lax.dot_general(a, b, (((1,), (1,)), ((), ())), preferred_element_type=F32)


def two_parts(x):
    high = x.astype(BF16)
    return jnp.concatenate([high, (x - high.astype(F32)).astype(BF16)], axis=0)


def dot2(x, b):
    out = dot(two_parts(x), b)
    return out[: x.shape[0]] + out[x.shape[0] :]


def iota(shape, dim):
    return lax.broadcasted_iota(jnp.int32, shape, dim)


def offsets_by_hops():
    def hops(at):
        x, y, z = at
        return min(x, 4 - x) + 2 * y + min(z, 8 - z)

    every = [(x, y, z) for z in range(8) for x in range(4) for y in range(2)]
    return sorted(every, key=lambda at: (-hops(at), at))


def folded(part):
    return jnp.concatenate([part[0:8, 0:64], part[8:16, 0:64]], axis=1)


def unfolded(part):
    return jnp.concatenate([part[:, 0:64], part[:, 64:128]], axis=0)


def kernel(
    cost, coup, solve, rel_h, near_h, owner_h, cap_h,
    plan_o, price_o, dual_o,
    X, S, C, cs, vfull, rel, near_in, owner_in, cap, meta, cts, send1, recv1, send2, recv2,
    mbuf, offs, L2, lown, p4t, p5, mp, zf, zb, sacc, usum, ara, arb, aka, akb, akc, maps, price_s, price_r,

    load_sem, s1, r1, s2, r2, sm, rm, sp, rp, sa, ra, sb, rb, ska, rka, skb, rkb, sc, rc, se, re, skc, rkc,
):
    sub = lax.axis_index("sub")
    dist = lax.axis_index("district")
    sxy, sz = sub // 8, lax.rem(sub, 8)
    pair, side = sub // 2, lax.rem(sub, 2)

    small = [
        pltpu.make_async_copy(src, dst, load_sem.at[6 + i])
        for i, (src, dst) in enumerate(
            ((rel_h, rel), (near_h, near_in), (owner_h, owner_in), (cap_h, cap))
        )
    ]
    loads = []
    for d in range(2):
        loads.append(pltpu.make_async_copy(cost.at[d], X.at[d], load_sem.at[3 * d]))
        loads.append(pltpu.make_async_copy(solve.at[d], S.at[d], load_sem.at[3 * d + 1]))
        loads.append(pltpu.make_async_copy(coup.at[d], C.at[d], load_sem.at[3 * d + 2]))
    for copy in small + loads:
        copy.start()

    barrier = pltpu.get_barrier_semaphore()
    sx, sy = sub // 16, lax.rem(sxy, 2)
    x_at = [16 * lax.rem(sx + k, 4) for k in range(4)]
    y_at = [8 * lax.rem(sy + k, 2) for k in range(2)]
    z_at = [lax.rem(sz + k, 8) for k in range(8)]
    xy_at = {(x, y): x_at[x] + y_at[y] for x in range(4) for y in range(2)}
    dist_at = [lax.rem(dist + k, DISTS) for k in range(DISTS)]
    order = offsets_by_hops()
    peers = [xy_at[x, y] + z_at[z] for x, y, z in order[:-1]]
    level = [xy_at[x, y] for x, y, z in order if z == 0]
    ring = [z_at[k] for k in (4, 3, 5, 2, 6, 1, 7)]

    def hello(device):
        pl.semaphore_signal(barrier, inc=1, device_id=device, device_id_type=MESH)

    for peer in peers:
        hello({"sub": peer})
    for at in level:
        for k in range(1, DISTS):
            hello({"district": dist_at[k], "sub": at + sz})

    def whole(buf, send_sem, recv_sem):
        return pltpu.make_async_remote_copy(
            src_ref=buf,
            dst_ref=buf,
            send_sem=send_sem,
            recv_sem=recv_sem,
            device_id={"sub": sub},
            device_id_type=MESH,
        )

    for copy in small:
        copy.wait()
    place = iota((4, BLOCK), 1) + sub * BLOCK
    for d in range(2):
        told = [near_in[d] - place, owner_in[d : d + 1], jnp.zeros((11, BLOCK), jnp.int32)]
        told = jnp.concatenate(told, axis=0).astype(F32)
        meta[d] = jnp.concatenate([told, jnp.zeros((16, BLOCK), F32)], axis=1).astype(BF16)
    mbuf[2 * REACH + side] = meta[side]
    here = rel[pair]
    here = jnp.where(side == 0, here[:, 0:BLOCK], here[:, BLOCK:PAIR]) // BLOCK
    own_block = jnp.concatenate([here[0:1], here[1:2]], axis=1)

    first = []
    for d in range(2):
        for copy in loads[3 * d : 3 * d + 3]:
            copy.wait()
        cs_d = dot(X[d], S[d])
        cs[d * BLOCK : (d + 1) * BLOCK] = cs_d
        first.append(dot_tb((-cs_d).astype(BF16), C[d]).astype(BF16))
    first = jnp.concatenate(first, axis=0)
    first = jnp.concatenate([first, jnp.zeros((2 * BLOCK, LANES - INTERFACE), BF16)], axis=1)
    lane = iota((2 * BLOCK, 2 * BLOCK), 1)
    row = iota((2 * BLOCK, 2 * BLOCK), 0)
    to_dest = jnp.where(own_block + BLOCK * (lane // BLOCK) == row, 1.0, 0.0).astype(BF16)
    eye = jnp.where(lane == row, 1.0, 0.0).astype(BF16)
    sorted_rows = dot(to_dest, first).astype(BF16)
    for d in range(2):
        send1[d, 0:REACH] = jnp.zeros((REACH, 2, LANES), BF16)
        send1[d, REACH + PAIRS : PAIRS + 2 * REACH] = jnp.zeros((REACH, 2, LANES), BF16)
        send1[d, REACH : REACH + PAIRS] = sorted_rows[d * BLOCK : (d + 1) * BLOCK].reshape(
            PAIRS, 2, LANES
        )

    pl.semaphore_wait(barrier, PEERS + OTHERS)

    for k in range(2 * SLAB):
        a, e = k // 2, k % 2

        def meta_copy():
            pltpu.make_async_remote_copy(
                src_ref=meta.at[e],
                dst_ref=mbuf.at[4 * REACH - 2 * a + side],
                send_sem=sm,
                recv_sem=rm,
                device_id={"sub": 2 * lax.rem(pair + a - REACH + PAIRS, PAIRS) + e},
                device_id_type=MESH,
            ).start()

        if a == REACH:
            pl.when(side != e)(meta_copy)
        else:
            meta_copy()

    def slot_of(device):
        return lax.rem(device, 2) * PAIRS + device // 2

    slot = slot_of(sub)
    for peer in peers:
        pltpu.make_async_remote_copy(
            src_ref=send1.at[lax.rem(peer, 2), REACH + peer // 2],
            dst_ref=recv1.at[slot, REACH],
            send_sem=se,
            recv_sem=re,
            device_id={"sub": peer},
            device_id_type=MESH,
        ).start()
    for peer in peers:
        for first in (0, REACH + 1):
            pltpu.make_async_remote_copy(
                src_ref=send1.at[lax.rem(peer, 2), pl.ds(peer // 2 + first, REACH)],
                dst_ref=recv1.at[slot, pl.ds(first, REACH)],
                send_sem=s1,
                recv_sem=r1,
                device_id={"sub": peer},
                device_id_type=MESH,
            ).start()
    recv1[slot] = send1[side, pl.ds(pair, SLAB)]

    back_at = 4 * (own_block // 2) + 2 * (lane // BLOCK) + lax.rem(own_block, 2)
    p5[...] = dot_ta(jnp.where(back_at == row, 1.0, 0.0).astype(BF16), eye).astype(BF16)
    for d in range(2):
        cts_d = dot(C[d], S[d]).astype(BF16)
        cts[d] = cts_d
        m_d = dot_tb(cts_d, C[d])
        mp[d] = jnp.zeros((LANES, LANES), BF16)
        mp[d, 0:INTERFACE, 0:INTERFACE] = (-STEP * m_d).astype(BF16)
        ri = iota((LANES - INTERFACE, LANES - 128), 0)
        li = iota((LANES - INTERFACE, LANES - 128), 1)
        shift = jnp.where(li - (INTERFACE - 128) == ri + RES, 1.0, 0.0)
        mp[d, INTERFACE:LANES, 128:LANES] = shift.astype(BF16)
        vfull[d, 0:INTERFACE] = cts_d
    for d in range(2):
        wide_map = mp[d, 0:INTERFACE, 0:INTERFACE]
        size = jnp.max(
            jnp.sum(jnp.abs(wide_map.astype(F32)), axis=0, keepdims=True), axis=1, keepdims=True
        )
        size = (1.0 + 1.02 * size).astype(BF16).astype(F32)
        small_map, tiles = wide_map[0:HORIZON].astype(F32) / size, []
        for j in range(4):
            if j:
                small_map = dot2(small_map, wide_map) / size
            tiles += [small_map[:, 0:HORIZON], jnp.broadcast_to(size, (HORIZON, BLOCK - HORIZON))]
        maps[dist, d] = jnp.concatenate(tiles, axis=1).astype(BF16)

    by_pair = rel[...].reshape(SUBS, PAIR)
    si, sj = iota((SUBS, SUBS), 0), iota((SUBS, SUBS), 1)
    pick = jnp.where((si // 2 == sj // 2) & (lax.rem(si, 2) == side), 1.0, 0.0).astype(BF16)

    def turned(values):
        flat = dot_ta(values.astype(F32).astype(BF16), pick)
        return jnp.concatenate([flat[0:BLOCK], flat[BLOCK:PAIR]], axis=1).astype(jnp.int32)

    block_of, place_in = turned(by_pair // BLOCK), turned(lax.rem(by_pair, BLOCK))
    odd = lax.rem(iota((1, PAIR), 1), 2)

    def place_map(a):
        hit = block_of == 2 * (pair + a - REACH) + odd
        at = jnp.sum(jnp.where(hit, place_in + 1, 0), axis=0, keepdims=True) - 1
        at = jnp.where(at >= 0, at + BLOCK * odd, -1)
        return jnp.where(at == row, 1.0, 0.0).astype(BF16)

    own_map = place_map(REACH)
    p4t[...] = dot_ta(own_map, eye).astype(BF16)

    whole(mbuf.at[pl.ds(0, 2 * SLAB - 1)], sm, rm).wait_recv()
    eye64 = jnp.where(
        iota((BLOCK, 128), 0) == iota((BLOCK, 128), 1), 1.0, 0.0
    ).astype(BF16)
    for m in range(2 * SLAB):
        offs[m * BLOCK : (m + 1) * BLOCK] = dot_tb(eye64, mbuf[m])
    diff = (iota((LANES, LANES), 1) - iota((LANES, LANES), 0)).astype(F32)
    for i in range(3):
        cols = offs[192 * i : 192 * i + 256]
        near = jnp.where(diff == 0.0, 1.0, 0.0)
        for k in range(4):
            near = near - jnp.where(diff == cols[:, k : k + 1], 0.25, 0.0)
        near = near.astype(BF16)
        L2[i, 32:224] = dot(near, near)[32:224].astype(BF16)
        L2[i, 0:32] = jnp.zeros((32, 256), BF16)
        L2[i, 224:256] = jnp.zeros((32, 256), BF16)
        if i == 1:
            lown[...] = near[64:192]

    def to_z(buf, send_sem, recv_sem):
        for z in ring:
            pltpu.make_async_remote_copy(
                src_ref=buf.at[sz],
                dst_ref=buf.at[sz],
                send_sem=send_sem,
                recv_sem=recv_sem,
                device_id={"sub": sxy * 8 + z},
                device_id_type=MESH,
            ).start()

    here_b = dist * 8 + sxy

    def start_b(buf, send_sem, recv_sem):
        for at in level:
            for k in (2, 1, 3, 0):
                if k == 0 and at is level[-1]:
                    continue
                pltpu.make_async_remote_copy(
                    src_ref=buf.at[here_b],
                    dst_ref=buf.at[here_b],
                    send_sem=send_sem,
                    recv_sem=recv_sem,
                    device_id={"district": dist_at[k], "sub": at + sz},
                    device_id_type=MESH,
                ).start()

    def all_of(buf, t, count, send_sem, recv_sem):
        return whole(buf.at[t, pl.ds(0, count)], send_sem.at[t], recv_sem.at[t])

    def reduce_a(t, part):
        ara[t, sz] = folded(part)
        to_z(ara.at[t], sa.at[t], ra.at[t])

    def reduce_b(t):
        all_of(ara, t, 7, sa, ra).wait_recv()
        arb[t, here_b] = jnp.sum(ara[t], axis=0).astype(BF16)
        start_b(arb.at[t], sb.at[t], rb.at[t])

    def reduce_end(t):
        all_of(arb, t, 31, sb, rb).wait_recv()
        return unfolded(jnp.sum(arb[t].astype(F32), axis=0))

    flow_map = mp.at[side]
    owners = []
    for a in range(SLAB):
        owner = [mbuf[2 * a + e][4:5, 0:BLOCK].astype(F32) for e in range(2)]
        owner = jnp.concatenate(owner, axis=1)
        owners.append(jnp.where(iota((RES, PAIR), 0).astype(F32) == owner, 1.0, 0.0))
    own_owners = owners[REACH]
    half_tile = jnp.zeros((2 * RES, BLOCK), F32)

    def back_step(tiles):
        rows2 = jnp.concatenate([two_parts(t) for t in tiles], axis=1)
        out0 = dot(rows2[:, 0:256], L2[0])
        out1 = dot(rows2[:, 192:448], L2[1])
        out2 = dot(rows2[:, 384:640], L2[2])
        out1 = jnp.concatenate([half_tile, out1, half_tile], axis=1)
        sums = [
            out0[:, 0:128],
            out0[:, 128:256] + out1[:, 0:128],
            out1[:, 128:256],
            out1[:, 256:384] + out2[:, 0:128],
            out2[:, 128:256],
        ]
        return [t[0:RES] + t[RES : 2 * RES] for t in sums]

    def seen_flows(weights):
        turned_weights = dot(two_parts(weights), own_map).astype(BF16)
        sums = dot(turned_weights, recv1[:, REACH].reshape(2 * SUBS, LANES))[:, 0:INTERFACE]
        sums = sums[0:BLOCK] + sums[BLOCK : 2 * BLOCK]
        return [sums[RES * j : RES * (j + 1)] for j in range(4)]

    def next_power(total, seen, count, j):
        total = dot2(total, flow_map[0:INTERFACE, 0:INTERFACE])
        return total + seen[j] * float(math.comb(count, j))

    def draws_of(seen, count):
        total = seen[count]
        for j in reversed(range(count)):
            total = next_power(total, seen, count, j)
        return total[:, 0:128]

    weights, tiles = [own_owners], owners
    for _ in range(3):
        tiles = back_step(tiles)
        weights.append(tiles[REACH])
    weights = jnp.concatenate(weights, axis=0)
    whole(recv1.at[pl.ds(0, PEERS), REACH], se, re).wait_recv()
    seen = seen_flows(weights)
    unit = dot_tb(two_parts(weights), own_owners.astype(BF16))
    unit = unit[0:BLOCK] + unit[BLOCK : 2 * BLOCK]
    unit = [unit[RES * j : RES * (j + 1), 0:RES] for j in range(4)]
    early = draws_of(seen, 3)
    reduce_a(0, early)
    aka[sz] = folded(jnp.concatenate(unit, axis=1))
    to_z(aka, ska, rka)
    weights = []
    for _ in range(4):
        tiles = back_step(tiles)
        weights.append(tiles[REACH])
    weights = jnp.concatenate(weights, axis=0)
    seen = seen + seen_flows(weights)
    reduce_a(1, draws_of(seen, 7))

    sacc[...] = jnp.zeros((256, LANES), F32)
    whole(recv1.at[pl.ds(0, PEERS), pl.ds(0, 2 * REACH)], s1, r1).wait_recv()
    for k in (2, 1, 3):
        pltpu.make_async_remote_copy(
            src_ref=maps.at[dist],
            dst_ref=maps.at[dist],
            send_sem=sc,
            recv_sem=rc,
            device_id={"district": dist_at[k]},
            device_id_type=MESH,
        ).start()
    lane_e = iota((PAIR, 128), 1) - (INTERFACE - 128)
    for a in range(SLAB):
        arrived = recv1[:, a].reshape(2 * SUBS, LANES)
        part = dot(place_map(a), arrived)
        top = a * PAIR
        owner = offs[top : top + PAIR, 4:5].astype(jnp.int32)
        mark = jnp.where((lane_e == owner) & (lane_e >= 0) & (lane_e < RES), 1.0, 0.0)
        low, high = part[:, 0:128], part[:, 128:LANES] + mark
        zf[top : top + PAIR, 0:128] = low
        zf[top : top + PAIR, 128:LANES] = high
        zb[top : top + PAIR, 0:128] = low.astype(BF16)
        zb[top : top + PAIR, 128:LANES] = high.astype(BF16)
    sacc[32:224] = zf[224:416]
    usum[...] = jnp.zeros((PAIR, LANES), F32)

    def half(i):
        u = dot(L2[i, 32:224], zb[192 * i : 192 * i + 256])
        if i == 1:
            usum[...] += u[32:160]
        return u.astype(BF16)

    def advance(i, u):
        at = 32 + 192 * i
        z = zf[at : at + 192] + dot(u, flow_map[...])
        zf[at : at + 192] = z
        zb[at : at + 192] = z.astype(BF16)
        if i == 1:
            sacc[32:224] += z

    def step():
        us = [half(i) for i in range(3)]
        for i, u in enumerate(us):
            advance(i, u)

    for k in range(6):
        step()
    reduce_b(0)
    whole(aka.at[pl.ds(0, 7)], ska, rka).wait_recv()
    by_side = [aka[d] + aka[d + 2] + aka[d + 4] + aka[d + 6] for d in range(2)]
    akb[sxy] = jnp.concatenate(by_side, axis=0)
    for at in level[:-1]:
        pltpu.make_async_remote_copy(
            src_ref=akb.at[sxy],
            dst_ref=akb.at[sxy],
            send_sem=skb,
            recv_sem=rkb,
            device_id={"sub": at + sz},
            device_id_type=MESH,
        ).start()

    u = half(1)
    prices = (STEP * usum[...]).astype(BF16)
    marks = zb[OWN : OWN + PAIR, INTERFACE:LANES]
    back = jnp.concatenate([prices[:, 0:INTERFACE], marks], axis=1)
    send2[...] = dot(p4t[...], back).astype(BF16).reshape(SUBS, 2, LANES)

    for peer in peers:
        pltpu.make_async_remote_copy(
            src_ref=send2.at[slot_of(peer)],
            dst_ref=recv2.at[sub],
            send_sem=s2,
            recv_sem=r2,
            device_id={"sub": peer},
            device_id_type=MESH,
        ).start()
    recv2[sub] = send2[slot_of(sub)]

    near_marks = dot(lown[...], zb[192:448, 128:LANES])[:, INTERFACE - 128 :]
    advance(1, u)
    near_sums = dot(lown[...], sacc[...].astype(BF16))[:, 0:INTERFACE]
    prices = jnp.concatenate([near_sums, near_marks], axis=1)
    kept = jnp.where(side == 0, prices[0:BLOCK], prices[BLOCK:PAIR])
    price0, marks0 = kept[:, 0:INTERFACE], kept[:, INTERFACE:LANES]
    price_s[...] = jnp.where(side == 0, prices[BLOCK:PAIR], prices[0:BLOCK])
    price_copy = pltpu.make_async_remote_copy(
        src_ref=price_s,
        dst_ref=price_r,
        send_sem=sp,
        recv_sem=rp,
        device_id={"sub": 2 * pair + 1 - side},
        device_id_type=MESH,
    )
    price_copy.start()

    reduce_b(1)
    whole(akb.at[pl.ds(0, 7)], skb, rkb).wait_recv()
    akc[dist] = jnp.sum(akb[...], axis=0)
    for k in (2, 1, 3):
        pltpu.make_async_remote_copy(
            src_ref=akc.at[dist],
            dst_ref=akc.at[dist],
            send_sem=skc,
            recv_sem=rkc,
            device_id={"district": dist_at[k]},
            device_id_type=MESH,
        ).start()
    capacity = cap[...]
    scale = 1.0 / math.sqrt(DISTS * 2 * SUBS * BLOCK / (2 * RES))
    duals = (reduce_end(0)[:, 0:HORIZON] - capacity) * scale
    wide = jnp.concatenate([duals, jnp.zeros((RES, INTERFACE - HORIZON), F32)], axis=1)

    binom = (1.0, 6.0, 15.0, 20.0)
    in_price = (1.0, -0.9, 0.27, -0.027)
    in_sum = (-4.0, 1.8, -0.36, 0.027)

    def powers_of(m_ref, count):
        powers = [wide]
        for _ in range(count):
            powers.append(dot2(powers[-1], m_ref[0:INTERFACE, 0:INTERFACE]) * (-1.0 / STEP))
        return powers

    def stack(powers, weights):
        parts = [p * (w / b) for p, w, b in zip(powers, weights, binom)]
        return jnp.concatenate(parts, axis=0).astype(BF16)

    powers_by = [powers_of(mp.at[d], 4) for d in range(2)]
    sums = [stack(powers_by[d][1:], in_sum) for d in range(2)]
    here_sums = jnp.where(side == 0, sums[0], sums[1])
    there_sums = jnp.where(side == 0, sums[1], sums[0])
    price_o[side] = STEP * (price0 + dot(marks0.astype(BF16), here_sums))
    price_copy.wait_recv()
    sent = price_r[...]
    price_o[1 - side] = STEP * (
        sent[:, 0:INTERFACE] + dot(sent[:, INTERFACE:LANES].astype(BF16), there_sums)
    )
    for d in range(2):
        vfull[d, INTERFACE:LANES] = dot(stack(powers_by[d][0:4], in_price), cts[d]).astype(BF16)

    whole(recv2.at[pl.ds(0, PEERS)], s2, r2).wait_recv()
    mine = dot(p5[...], recv2[...].reshape(2 * SUBS, LANES)).astype(BF16)
    for d in range(2):
        at = d * BLOCK
        plan_o[d] = -(cs[at : at + BLOCK] + dot(mine[at : at + BLOCK], vfull[d]))

    whole(akc.at[pl.ds(0, 3)], skc, rkc).wait_recv()
    whole(maps.at[pl.ds(0, 3)], sc, rc).wait_recv()
    units, causes = [], []
    for k in range(DISTS):
        unit = akc[k]
        for d in range(2):
            units.append(unfolded(unit[8 * d : 8 * d + 8]))
            size = maps[k, d, 0:1, HORIZON : HORIZON + 1].astype(F32)
            moved = dot2(duals, maps[k, d])
            for j in range(4):
                part = moved[:, BLOCK * j : BLOCK * (j + 1)] * (math.comb(3, j) / STEP)
                for _ in range(j + 1):
                    part = part * size
                causes.append(part)
    units, causes = jnp.concatenate(units, axis=1), two_parts(jnp.concatenate(causes, axis=0))
    count = units.shape[1]
    draws1 = dot2(units, causes[0:count]) + dot(units.astype(BF16), causes[count : 2 * count])
    draws1 = draws1[:, 0:HORIZON]

    draws0 = reduce_end(1)[:, 0:HORIZON]
    dual_o[...] = duals + (draws0 + draws1 - capacity) * scale

    whole(mbuf.at[pl.ds(0, 2 * SLAB - 1)], sm, rm).wait_send()
    whole(recv1.at[pl.ds(0, PEERS), pl.ds(0, 2 * REACH)], s1, r1).wait_send()
    whole(recv2.at[pl.ds(0, PEERS)], s2, r2).wait_send()
    for t in range(2):
        all_of(ara, t, 7, sa, ra).wait_send()
        all_of(arb, t, 31, sb, rb).wait_send()
    whole(aka.at[pl.ds(0, 7)], ska, rka).wait_send()
    whole(akb.at[pl.ds(0, 7)], skb, rkb).wait_send()
    whole(akc.at[pl.ds(0, 3)], skc, rkc).wait_send()
    whole(maps.at[pl.ds(0, 3)], sc, rc).wait_send()
    whole(recv1.at[pl.ds(0, PEERS), REACH], se, re).wait_send()
    price_copy.wait_send()


def write_out(plan, price, dual, plan_o, price_o, dual_o, sems):
    copies = [
        pltpu.make_async_copy(src, dst, sems.at[i])
        for i, (src, dst) in enumerate(((plan, plan_o), (price, price_o), (dual, dual_o)))
    ]
    for copy in copies:
        copy.start()
    for copy in copies:
        copy.wait()


def on_device(cost_terms, neighbours, relayout, ownership, capacity, coupling, solve_factor):
    pairs = relayout.reshape(2, SUBS // 2, 2 * BLOCK).transpose(1, 0, 2)
    vmem = pl.BlockSpec(memory_space=pltpu.VMEM)
    hbm = pl.BlockSpec(memory_space=pltpu.HBM)
    dma = pltpu.SemaphoreType.DMA
    parts = pl.pallas_call(
        kernel,
        out_shape=(
            pltpu.VMEM((2, BLOCK, UNKNOWNS), F32),
            pltpu.VMEM((2, BLOCK, INTERFACE), F32),
            pltpu.VMEM((RES, HORIZON), F32),
        ),
        in_specs=[hbm] * 7,
        out_specs=(vmem,) * 3,
        scratch_shapes=[
            pltpu.VMEM((2, BLOCK, UNKNOWNS), BF16),
            pltpu.VMEM((2, UNKNOWNS, UNKNOWNS), BF16),
            pltpu.VMEM((2, INTERFACE, UNKNOWNS), BF16),
            pltpu.VMEM((2 * BLOCK, UNKNOWNS), F32),
            pltpu.VMEM((2, LANES, UNKNOWNS), BF16),
            pltpu.VMEM((SUBS // 2, 2, 2 * BLOCK), jnp.int32),
            pltpu.VMEM((2, 4, BLOCK), jnp.int32),
            pltpu.VMEM((2, BLOCK), jnp.int32),
            pltpu.VMEM((RES, HORIZON), F32),
            pltpu.VMEM((2, 16, 128), BF16),
            pltpu.VMEM((2, INTERFACE, UNKNOWNS), BF16),
            pltpu.VMEM((2, PAIRS + 2 * REACH, 2, LANES), BF16),
            pltpu.VMEM((SUBS, SLAB, 2, LANES), BF16),
            pltpu.VMEM((SUBS, 2, LANES), BF16),
            pltpu.VMEM((SUBS, 2, LANES), BF16),
            pltpu.VMEM((2 * SLAB, 16, 128), BF16),
            pltpu.VMEM((ROWS, 16), F32),
            pltpu.VMEM((3, 256, 256), BF16),
            pltpu.VMEM((PAIR, 256), BF16),
            pltpu.VMEM((128, 128), BF16),
            pltpu.VMEM((128, 128), BF16),
            pltpu.VMEM((2, LANES, LANES), BF16),
            pltpu.VMEM((ROWS, LANES), F32),
            pltpu.VMEM((ROWS, LANES), BF16),
            pltpu.VMEM((256, LANES), F32),
            pltpu.VMEM((PAIR, LANES), F32),
            pltpu.VMEM((2, 8, 8, 128), F32),
            pltpu.VMEM((2, 32, 8, 128), BF16),
            pltpu.VMEM((8, 8, 128), F32),
            pltpu.VMEM((8, 16, 128), F32),
            pltpu.VMEM((DISTS, 16, 128), F32),
            pltpu.VMEM((DISTS, 2, HORIZON, LANES), BF16),
            pltpu.VMEM((BLOCK, LANES), F32),
            pltpu.VMEM((BLOCK, LANES), F32),
            dma((10,)),
            dma, dma, dma, dma, dma, dma, dma, dma,
            dma((2,)), dma((2,)), dma((2,)), dma((2,)),
            dma, dma, dma, dma, dma, dma, dma, dma, dma, dma,
        ],
        compiler_params=pltpu.CompilerParams(
            collective_id=0, has_side_effects=True, vmem_limit_bytes=VMEM_LIMIT
        ),
    )(
        cost_terms, coupling.transpose(0, 2, 1), solve_factor, pairs,
        neighbours.transpose(0, 2, 1), ownership, capacity,
    )
    return pl.pallas_call(
        write_out,
        out_shape=(
            jax.ShapeDtypeStruct((2, BLOCK, UNKNOWNS), F32),
            jax.ShapeDtypeStruct((2, BLOCK, INTERFACE), F32),
            jax.ShapeDtypeStruct((RES, HORIZON), F32),
        ),
        in_specs=[vmem] * 3,
        out_specs=(hbm,) * 3,
        scratch_shapes=[dma((3,))],
        compiler_params=pltpu.CompilerParams(vmem_limit_bytes=1024 * 1024),
    )(*parts)


def solution(mesh):
    placed = (
        P("district", "sub", None),
        P("district", "sub", None),
        P("district", None),
        P("district", "sub"),
        P(),
        P("district", None, None),
        P("district", None, None),
    )
    return jax.shard_map(
        on_device,
        mesh=mesh,
        in_specs=placed,
        out_specs=(P("district", "sub", None), P("district", "sub", None), P()),
        check_vma=False,
    )
```

```python
import math

import jax
import jax.numpy as jnp
from jax import lax
from jax.experimental import pallas as pl
from jax.experimental.pallas import tpu as pltpu
from jax.sharding import PartitionSpec as P

MESH = pl.DeviceIdType.MESH
F32, BF16 = jnp.float32, jnp.bfloat16
HORIZON, UNKNOWNS, INTERFACE, BLOCK = 48, 768, 192, 64
RES, SUBS, DISTS = 16, 64, 4
PAIRS = SUBS // 2
REACH = 2
SLAB = 2 * REACH + 1
SPAN = PAIRS + 2 * REACH
PAIR = 2 * BLOCK
ROWS = SLAB * PAIR
OWN = REACH * PAIR
LANES = 256
STEP = 0.3
PEERS = SUBS - 1
OTHERS = 24
VMEM_LIMIT = 67043328 - 700 * 1024


def dot(a, b):
    return jnp.dot(a, b, preferred_element_type=F32)


def dot_ta(a, b):
    return lax.dot_general(a, b, (((0,), (0,)), ((), ())), preferred_element_type=F32)


def dot_tb(a, b):
    return lax.dot_general(a, b, (((1,), (1,)), ((), ())), preferred_element_type=F32)


def two_parts(x):
    high = x.astype(BF16)
    return jnp.concatenate([high, (x - high.astype(F32)).astype(BF16)], axis=0)


def dot2(x, b):
    out = dot(two_parts(x), b)
    return out[: x.shape[0]] + out[x.shape[0] :]


def iota(shape, dim):
    return lax.broadcasted_iota(jnp.int32, shape, dim)


def offsets_by_hops():
    def hops(at):
        x, y, z = at
        return min(x, 4 - x) + 2 * y + min(z, 8 - z)

    every = [(x, y, z) for z in range(8) for x in range(4) for y in range(2)]
    return sorted(every, key=lambda at: (-hops(at), at))


def folded(part):
    return jnp.concatenate([part[0:8, 0:64], part[8:16, 0:64]], axis=1)


def unfolded(part):
    return jnp.concatenate([part[:, 0:64], part[:, 64:128]], axis=0)


def kernel(
    cost, coup, solve, rel_h, near_h, owner_h, cap_h,
    plan_o, price_o, dual_o,
    X, S, C, cs, vfull, rel, near_in, owner_in, cap, meta, cts, send1, recv1, sendh, recvh, send2, recv2,
    mbuf, offs, L2, lown, p4t, p5, mp, zf, zb, sacc, usum, ara, arb, aka, akb, akc, maps, price_s, price_r,

    load_sem, s1, r1, s2, r2, sm, rm, sp, rp, sa, ra, sb, rb, ska, rka, skb, rkb, sc, rc, se, re, skc, rkc,
):
    sub = lax.axis_index("sub")
    dist = lax.axis_index("district")
    sxy, sz = sub // 8, lax.rem(sub, 8)
    pair, side = sub // 2, lax.rem(sub, 2)

    small = [
        pltpu.make_async_copy(src, dst, load_sem.at[6 + i])
        for i, (src, dst) in enumerate(
            ((rel_h, rel), (near_h, near_in), (owner_h, owner_in), (cap_h, cap))
        )
    ]
    loads = []
    for d in range(2):
        loads.append(pltpu.make_async_copy(cost.at[d], X.at[d], load_sem.at[3 * d]))
        loads.append(pltpu.make_async_copy(solve.at[d], S.at[d], load_sem.at[3 * d + 1]))
        loads.append(pltpu.make_async_copy(coup.at[d], C.at[d], load_sem.at[3 * d + 2]))
    for copy in small + loads:
        copy.start()

    barrier = pltpu.get_barrier_semaphore()
    sx, sy = sub // 16, lax.rem(sxy, 2)
    x_at = [16 * lax.rem(sx + k, 4) for k in range(4)]
    y_at = [8 * lax.rem(sy + k, 2) for k in range(2)]
    z_at = [lax.rem(sz + k, 8) for k in range(8)]
    xy_at = {(x, y): x_at[x] + y_at[y] for x in range(4) for y in range(2)}
    dist_at = [lax.rem(dist + k, DISTS) for k in range(DISTS)]
    order = offsets_by_hops()
    peers = [xy_at[x, y] + z_at[z] for x, y, z in order[:-1]]
    level = [xy_at[x, y] for x, y, z in order if z == 0]
    ring = [z_at[k] for k in (4, 3, 5, 2, 6, 1, 7)]

    def hello(device):
        pl.semaphore_signal(barrier, inc=1, device_id=device, device_id_type=MESH)

    for peer in peers:
        hello({"sub": peer})
    for at in level:
        for k in range(1, DISTS):
            hello({"district": dist_at[k], "sub": at + sz})

    def whole(buf, send_sem, recv_sem):
        return pltpu.make_async_remote_copy(
            src_ref=buf,
            dst_ref=buf,
            send_sem=send_sem,
            recv_sem=recv_sem,
            device_id={"sub": sub},
            device_id_type=MESH,
        )

    for copy in small:
        copy.wait()
    place = iota((4, BLOCK), 1) + sub * BLOCK
    for d in range(2):
        told = [near_in[d] - place, owner_in[d : d + 1], jnp.zeros((11, BLOCK), jnp.int32)]
        told = jnp.concatenate(told, axis=0).astype(F32)
        meta[d] = jnp.concatenate([told, jnp.zeros((16, BLOCK), F32)], axis=1).astype(BF16)
    mbuf[2 * REACH + side] = meta[side]
    here = rel[pair]
    here = jnp.where(side == 0, here[:, 0:BLOCK], here[:, BLOCK:PAIR]) // BLOCK
    own_block = jnp.concatenate([here[0:1], here[1:2]], axis=1)

    first = []
    for d in range(2):
        for copy in loads[3 * d : 3 * d + 3]:
            copy.wait()
        cs_d = dot(X[d], S[d])
        cs[d * BLOCK : (d + 1) * BLOCK] = cs_d
        first.append(dot_tb((-cs_d).astype(BF16), C[d]).astype(BF16))
    first = jnp.concatenate(first, axis=0)
    first = jnp.concatenate([first, jnp.zeros((2 * BLOCK, LANES - INTERFACE), BF16)], axis=1)
    lane = iota((2 * BLOCK, 2 * BLOCK), 1)
    row = iota((2 * BLOCK, 2 * BLOCK), 0)
    eye = jnp.where(lane == row, 1.0, 0.0).astype(BF16)
    dest = own_block + 2 * SPAN * (lane[0:1] // BLOCK)
    at_row = iota((4 * SPAN, 2 * BLOCK), 0)
    sorted_rows, next_rows = [
        dot(jnp.where(dest + 2 * skip == at_row, 1.0, 0.0).astype(BF16), first).astype(BF16)
        for skip in (REACH, REACH - 1)
    ]
    send1[...] = sorted_rows.reshape(2 * SPAN, 2, LANES)
    rest = [t[:, 128:INTERFACE] for t in (sorted_rows, next_rows)]
    for k, tile in enumerate(
        (sorted_rows[:, 0:128], next_rows[:, 0:128], jnp.concatenate(rest, axis=1))
    ):
        sendh[:, k] = tile.reshape(2 * SPAN, 2, 128)

    pl.semaphore_wait(barrier, PEERS + OTHERS)

    for k in range(2 * SLAB):
        a, e = k // 2, k % 2

        def meta_copy():
            pltpu.make_async_remote_copy(
                src_ref=meta.at[e],
                dst_ref=mbuf.at[4 * REACH - 2 * a + side],
                send_sem=sm,
                recv_sem=rm,
                device_id={"sub": 2 * lax.rem(pair + a - REACH + PAIRS, PAIRS) + e},
                device_id_type=MESH,
            ).start()

        if a == REACH:
            pl.when(side != e)(meta_copy)
        else:
            meta_copy()

    def slot_of(device):
        return lax.rem(device, 2) * PAIRS + device // 2

    slot = slot_of(sub)
    for peer in peers:
        pltpu.make_async_remote_copy(
            src_ref=send1.at[SPAN * lax.rem(peer, 2) + peer // 2 + REACH],
            dst_ref=recv1.at[slot],
            send_sem=se,
            recv_sem=re,
            device_id={"sub": peer},
            device_id_type=MESH,
        ).start()
    for peer in peers:
        for k in range(2):
            pltpu.make_async_remote_copy(
                src_ref=sendh.at[SPAN * lax.rem(peer, 2) + peer // 2 + (REACH + 1) * k],
                dst_ref=recvh.at[slot, k],
                send_sem=s1,
                recv_sem=r1,
                device_id={"sub": peer},
                device_id_type=MESH,
            ).start()
    mine_at = SPAN * side + pair
    recv1[slot] = send1[mine_at + REACH]
    for k in range(2):
        recvh[slot, k] = sendh[mine_at + (REACH + 1) * k]

    back_at = 4 * (own_block // 2) + 2 * (lane // BLOCK) + lax.rem(own_block, 2)
    p5[...] = dot_ta(jnp.where(back_at == row, 1.0, 0.0).astype(BF16), eye).astype(BF16)
    for d in range(2):
        cts_d = dot(C[d], S[d]).astype(BF16)
        cts[d] = cts_d
        m_d = dot_tb(cts_d, C[d])
        mp[d] = jnp.zeros((LANES, LANES), BF16)
        mp[d, 0:INTERFACE, 0:INTERFACE] = (-STEP * m_d).astype(BF16)
        ri = iota((LANES - INTERFACE, LANES - 128), 0)
        li = iota((LANES - INTERFACE, LANES - 128), 1)
        shift = jnp.where(li - (INTERFACE - 128) == ri + RES, 1.0, 0.0)
        mp[d, INTERFACE:LANES, 128:LANES] = shift.astype(BF16)
        vfull[d, 0:INTERFACE] = cts_d
    for d in range(2):
        wide_map = mp[d, 0:INTERFACE, 0:INTERFACE]
        size = jnp.max(
            jnp.sum(jnp.abs(wide_map.astype(F32)), axis=0, keepdims=True), axis=1, keepdims=True
        )
        size = (1.0 + 1.02 * size).astype(BF16).astype(F32)
        small_map, tiles = wide_map[0:HORIZON].astype(F32) / size, []
        for j in range(4):
            if j:
                small_map = dot2(small_map, wide_map) / size
            tiles += [small_map[:, 0:HORIZON], jnp.broadcast_to(size, (HORIZON, BLOCK - HORIZON))]
        maps[dist, d] = jnp.concatenate(tiles, axis=1).astype(BF16)

    by_pair = rel[...].reshape(SUBS, PAIR)
    si, sj = iota((SUBS, SUBS), 0), iota((SUBS, SUBS), 1)
    pick = jnp.where((si // 2 == sj // 2) & (lax.rem(si, 2) == side), 1.0, 0.0).astype(BF16)

    def turned(values):
        flat = dot_ta(values.astype(F32).astype(BF16), pick)
        return jnp.concatenate([flat[0:BLOCK], flat[BLOCK:PAIR]], axis=1).astype(jnp.int32)

    block_of, place_in = turned(by_pair // BLOCK), turned(lax.rem(by_pair, BLOCK))
    odd = lax.rem(iota((1, PAIR), 1), 2)

    def place_map(a):
        hit = block_of == 2 * (pair + a - REACH) + odd
        at = jnp.sum(jnp.where(hit, place_in + 1, 0), axis=0, keepdims=True) - 1
        at = jnp.where(at >= 0, at + BLOCK * odd, -1)
        return jnp.where(at == row, 1.0, 0.0).astype(BF16)

    own_map = place_map(REACH)
    p4t[...] = dot_ta(own_map, eye).astype(BF16)

    whole(mbuf.at[pl.ds(0, 2 * SLAB - 1)], sm, rm).wait_recv()
    eye64 = jnp.where(
        iota((BLOCK, 128), 0) == iota((BLOCK, 128), 1), 1.0, 0.0
    ).astype(BF16)
    for m in range(2 * SLAB):
        offs[m * BLOCK : (m + 1) * BLOCK] = dot_tb(eye64, mbuf[m])
    diff = (iota((LANES, LANES), 1) - iota((LANES, LANES), 0)).astype(F32)
    for i in range(3):
        cols = offs[192 * i : 192 * i + 256]
        near = jnp.where(diff == 0.0, 1.0, 0.0)
        for k in range(4):
            near = near - jnp.where(diff == cols[:, k : k + 1], 0.25, 0.0)
        near = near.astype(BF16)
        L2[i, 32:224] = dot(near, near)[32:224].astype(BF16)
        L2[i, 0:32] = jnp.zeros((32, 256), BF16)
        L2[i, 224:256] = jnp.zeros((32, 256), BF16)
        if i == 1:
            lown[...] = near[64:192]

    def to_z(buf, send_sem, recv_sem):
        for z in ring:
            pltpu.make_async_remote_copy(
                src_ref=buf.at[sz],
                dst_ref=buf.at[sz],
                send_sem=send_sem,
                recv_sem=recv_sem,
                device_id={"sub": sxy * 8 + z},
                device_id_type=MESH,
            ).start()

    here_b = dist * 8 + sxy

    def start_b(buf, send_sem, recv_sem):
        for at in level:
            for k in (2, 1, 3, 0):
                if k == 0 and at is level[-1]:
                    continue
                pltpu.make_async_remote_copy(
                    src_ref=buf.at[here_b],
                    dst_ref=buf.at[here_b],
                    send_sem=send_sem,
                    recv_sem=recv_sem,
                    device_id={"district": dist_at[k], "sub": at + sz},
                    device_id_type=MESH,
                ).start()

    def all_of(buf, t, count, send_sem, recv_sem):
        return whole(buf.at[t, pl.ds(0, count)], send_sem.at[t], recv_sem.at[t])

    def reduce_a(t, part):
        ara[t, sz] = folded(part)
        to_z(ara.at[t], sa.at[t], ra.at[t])

    def reduce_b(t):
        all_of(ara, t, 7, sa, ra).wait_recv()
        arb[t, here_b] = jnp.sum(ara[t], axis=0).astype(BF16)
        start_b(arb.at[t], sb.at[t], rb.at[t])

    def reduce_end(t):
        all_of(arb, t, 31, sb, rb).wait_recv()
        return unfolded(jnp.sum(arb[t].astype(F32), axis=0))

    flow_map = mp.at[side]
    owners = []
    for a in range(SLAB):
        owner = [mbuf[2 * a + e][4:5, 0:BLOCK].astype(F32) for e in range(2)]
        owner = jnp.concatenate(owner, axis=1)
        owners.append(jnp.where(iota((RES, PAIR), 0).astype(F32) == owner, 1.0, 0.0))
    own_owners = owners[REACH]
    half_tile = jnp.zeros((2 * RES, BLOCK), F32)

    def back_step(tiles):
        rows2 = jnp.concatenate([two_parts(t) for t in tiles], axis=1)
        out0 = dot(rows2[:, 0:256], L2[0])
        out1 = dot(rows2[:, 192:448], L2[1])
        out2 = dot(rows2[:, 384:640], L2[2])
        out1 = jnp.concatenate([half_tile, out1, half_tile], axis=1)
        sums = [
            out0[:, 0:128],
            out0[:, 128:256] + out1[:, 0:128],
            out1[:, 128:256],
            out1[:, 256:384] + out2[:, 0:128],
            out2[:, 128:256],
        ]
        return [t[0:RES] + t[RES : 2 * RES] for t in sums]

    def seen_flows(weights):
        turned_weights = dot(two_parts(weights), own_map).astype(BF16)
        sums = dot(turned_weights, recv1[...].reshape(2 * SUBS, LANES))[:, 0:INTERFACE]
        sums = sums[0:BLOCK] + sums[BLOCK : 2 * BLOCK]
        return [sums[RES * j : RES * (j + 1)] for j in range(4)]

    def next_power(total, seen, count, j):
        total = dot2(total, flow_map[0:INTERFACE, 0:INTERFACE])
        return total + seen[j] * float(math.comb(count, j))

    def draws_of(seen, count):
        total = seen[count]
        for j in reversed(range(count)):
            total = next_power(total, seen, count, j)
        return total[:, 0:128]

    weights, tiles = [own_owners], owners
    for _ in range(3):
        tiles = back_step(tiles)
        weights.append(tiles[REACH])
    weights = jnp.concatenate(weights, axis=0)
    unit = dot_tb(two_parts(weights), own_owners.astype(BF16))
    unit = unit[0:BLOCK] + unit[BLOCK : 2 * BLOCK]
    unit = [unit[RES * j : RES * (j + 1), 0:RES] for j in range(4)]
    aka[sz] = folded(jnp.concatenate(unit, axis=1))
    to_z(aka, ska, rka)
    whole(recv1.at[pl.ds(0, PEERS)], se, re).wait_recv()
    seen = seen_flows(weights)
    early = draws_of(seen, 3)
    reduce_a(0, early)
    weights = []
    for _ in range(4):
        tiles = back_step(tiles)
        weights.append(tiles[REACH])
    weights = jnp.concatenate(weights, axis=0)
    seen = seen + seen_flows(weights)
    late = seen[7]
    for j in (6, 5, 4, 3):
        late = next_power(late, seen, 7, j)

    sacc[...] = jnp.zeros((256, LANES), F32)
    whole(recvh.at[pl.ds(0, PEERS)], s1, r1).wait_recv()
    for k in (2, 1, 3):
        pltpu.make_async_remote_copy(
            src_ref=maps.at[dist],
            dst_ref=maps.at[dist],
            send_sem=sc,
            recv_sem=rc,
            device_id={"district": dist_at[k]},
            device_id_type=MESH,
        ).start()
    lane_e = iota((PAIR, 128), 1) - (INTERFACE - 128)
    for a in range(SLAB):
        top = a * PAIR
        if a == REACH:
            part = dot(own_map, recv1[...].reshape(2 * SUBS, LANES))
            low, high = part[:, 0:128], part[:, 128:LANES]
        else:
            k, which = (0, a) if a < REACH else (1, a - REACH - 1)
            low = dot(place_map(a), recvh[:, k, which].reshape(2 * SUBS, 128))
            high = dot(place_map(a), recvh[:, k, 2].reshape(2 * SUBS, 128))
            if which:
                high = pltpu.roll(high, BLOCK, 1)
            high = jnp.where(lane_e < 0, high, 0.0)
        owner = offs[top : top + PAIR, 4:5].astype(jnp.int32)
        mark = jnp.where((lane_e == owner) & (lane_e >= 0) & (lane_e < RES), 1.0, 0.0)
        high = high + mark
        zf[top : top + PAIR, 0:128] = low
        zf[top : top + PAIR, 128:LANES] = high
        zb[top : top + PAIR, 0:128] = low.astype(BF16)
        zb[top : top + PAIR, 128:LANES] = high.astype(BF16)
    sacc[32:224] = zf[224:416]
    usum[...] = jnp.zeros((PAIR, LANES), F32)

    def half(i):
        u = dot(L2[i, 32:224], zb[192 * i : 192 * i + 256])
        if i == 1:
            usum[...] += u[32:160]
        return u.astype(BF16)

    def advance(i, u):
        at = 32 + 192 * i
        z = zf[at : at + 192] + dot(u, flow_map[...])
        zf[at : at + 192] = z
        zb[at : at + 192] = z.astype(BF16)
        if i == 1:
            sacc[32:224] += z

    def step():
        us = [half(i) for i in range(3)]
        for i, u in enumerate(us):
            advance(i, u)

    for j in (2, 1, 0):
        if j:
            step()
        late = next_power(late, seen, 7, j)
    reduce_a(1, late[:, 0:128])
    for k in range(4):
        step()
    whole(aka.at[pl.ds(0, 7)], ska, rka).wait_recv()
    by_side = [aka[d] + aka[d + 2] + aka[d + 4] + aka[d + 6] for d in range(2)]
    akb[sxy] = jnp.concatenate(by_side, axis=0)
    for at in level[:-1]:
        pltpu.make_async_remote_copy(
            src_ref=akb.at[sxy],
            dst_ref=akb.at[sxy],
            send_sem=skb,
            recv_sem=rkb,
            device_id={"sub": at + sz},
            device_id_type=MESH,
        ).start()
    reduce_b(0)

    u = half(1)
    prices = (STEP * usum[...]).astype(BF16)
    marks = zb[OWN : OWN + PAIR, INTERFACE:LANES]
    back = jnp.concatenate([prices[:, 0:INTERFACE], marks], axis=1)
    send2[...] = dot(p4t[...], back).astype(BF16).reshape(SUBS, 2, LANES)

    for peer in peers:
        pltpu.make_async_remote_copy(
            src_ref=send2.at[slot_of(peer)],
            dst_ref=recv2.at[sub],
            send_sem=s2,
            recv_sem=r2,
            device_id={"sub": peer},
            device_id_type=MESH,
        ).start()
    recv2[sub] = send2[slot_of(sub)]

    near_marks = dot(lown[...], zb[192:448, 128:LANES])[:, INTERFACE - 128 :]
    advance(1, u)
    near_sums = dot(lown[...], sacc[...].astype(BF16))[:, 0:INTERFACE]
    prices = jnp.concatenate([near_sums, near_marks], axis=1)
    kept = jnp.where(side == 0, prices[0:BLOCK], prices[BLOCK:PAIR])
    price0, marks0 = kept[:, 0:INTERFACE], kept[:, INTERFACE:LANES]
    price_s[...] = jnp.where(side == 0, prices[BLOCK:PAIR], prices[0:BLOCK])
    price_copy = pltpu.make_async_remote_copy(
        src_ref=price_s,
        dst_ref=price_r,
        send_sem=sp,
        recv_sem=rp,
        device_id={"sub": 2 * pair + 1 - side},
        device_id_type=MESH,
    )
    price_copy.start()

    reduce_b(1)
    whole(akb.at[pl.ds(0, 7)], skb, rkb).wait_recv()
    akc[dist] = jnp.sum(akb[...], axis=0)
    for k in (2, 1, 3):
        pltpu.make_async_remote_copy(
            src_ref=akc.at[dist],
            dst_ref=akc.at[dist],
            send_sem=skc,
            recv_sem=rkc,
            device_id={"district": dist_at[k]},
            device_id_type=MESH,
        ).start()
    capacity = cap[...]
    scale = 1.0 / math.sqrt(DISTS * 2 * SUBS * BLOCK / (2 * RES))
    duals = (reduce_end(0)[:, 0:HORIZON] - capacity) * scale
    wide = jnp.concatenate([duals, jnp.zeros((RES, INTERFACE - HORIZON), F32)], axis=1)

    binom = (1.0, 6.0, 15.0, 20.0)
    in_price = (1.0, -0.9, 0.27, -0.027)
    in_sum = (-4.0, 1.8, -0.36, 0.027)

    def powers_of(m_ref, count):
        powers = [wide]
        for _ in range(count):
            powers.append(dot2(powers[-1], m_ref[0:INTERFACE, 0:INTERFACE]) * (-1.0 / STEP))
        return powers

    def stack(powers, weights):
        parts = [p * (w / b) for p, w, b in zip(powers, weights, binom)]
        return jnp.concatenate(parts, axis=0).astype(BF16)

    powers_by = [powers_of(mp.at[d], 4) for d in range(2)]
    for d in range(2):
        vfull[d, INTERFACE:LANES] = dot(stack(powers_by[d][0:4], in_price), cts[d]).astype(BF16)

    whole(recv2.at[pl.ds(0, PEERS)], s2, r2).wait_recv()
    mine = dot(p5[...], recv2[...].reshape(2 * SUBS, LANES)).astype(BF16)
    for d in range(2):
        at = d * BLOCK
        plan_o[d] = -(cs[at : at + BLOCK] + dot(mine[at : at + BLOCK], vfull[d]))

    price_copy.wait_recv()
    whole(maps.at[pl.ds(0, 3)], sc, rc).wait_recv()
    sums = [stack(powers_by[d][1:], in_sum) for d in range(2)]
    here_sums = jnp.where(side == 0, sums[0], sums[1])
    there_sums = jnp.where(side == 0, sums[1], sums[0])
    price_o[side] = STEP * (price0 + dot(marks0.astype(BF16), here_sums))
    sent = price_r[...]
    price_o[1 - side] = STEP * (
        sent[:, 0:INTERFACE] + dot(sent[:, INTERFACE:LANES].astype(BF16), there_sums)
    )
    causes = []
    for k in range(DISTS):
        for d in range(2):
            size = maps[k, d, 0:1, HORIZON : HORIZON + 1].astype(F32)
            moved = dot2(duals, maps[k, d])
            for j in range(4):
                part = moved[:, BLOCK * j : BLOCK * (j + 1)] * (math.comb(3, j) / STEP)
                for _ in range(j + 1):
                    part = part * size
                causes.append(part)
    causes = two_parts(jnp.concatenate(causes, axis=0))
    whole(akc.at[pl.ds(0, 3)], skc, rkc).wait_recv()
    units = [unfolded(akc[k][8 * d : 8 * d + 8]) for k in range(DISTS) for d in range(2)]
    units = jnp.concatenate(units, axis=1)
    count = units.shape[1]
    draws1 = dot2(units, causes[0:count]) + dot(units.astype(BF16), causes[count : 2 * count])
    draws1 = draws1[:, 0:HORIZON]
    draws0 = reduce_end(1)[:, 0:HORIZON]
    dual_o[...] = duals + (draws0 + draws1 - capacity) * scale

    whole(mbuf.at[pl.ds(0, 2 * SLAB - 1)], sm, rm).wait_send()
    whole(recvh.at[pl.ds(0, PEERS)], s1, r1).wait_send()
    whole(recv2.at[pl.ds(0, PEERS)], s2, r2).wait_send()
    for t in range(2):
        all_of(ara, t, 7, sa, ra).wait_send()
        all_of(arb, t, 31, sb, rb).wait_send()
    whole(aka.at[pl.ds(0, 7)], ska, rka).wait_send()
    whole(akb.at[pl.ds(0, 7)], skb, rkb).wait_send()
    whole(akc.at[pl.ds(0, 3)], skc, rkc).wait_send()
    whole(maps.at[pl.ds(0, 3)], sc, rc).wait_send()
    whole(recv1.at[pl.ds(0, PEERS)], se, re).wait_send()
    price_copy.wait_send()


def write_out(plan, price, dual, plan_o, price_o, dual_o, sems):
    copies = [
        pltpu.make_async_copy(src, dst, sems.at[i])
        for i, (src, dst) in enumerate(((plan, plan_o), (price, price_o), (dual, dual_o)))
    ]
    for copy in copies:
        copy.start()
    for copy in copies:
        copy.wait()


def on_device(cost_terms, neighbours, relayout, ownership, capacity, coupling, solve_factor):
    pairs = relayout.reshape(2, SUBS // 2, 2 * BLOCK).transpose(1, 0, 2)
    vmem = pl.BlockSpec(memory_space=pltpu.VMEM)
    hbm = pl.BlockSpec(memory_space=pltpu.HBM)
    dma = pltpu.SemaphoreType.DMA
    parts = pl.pallas_call(
        kernel,
        out_shape=(
            pltpu.VMEM((2, BLOCK, UNKNOWNS), F32),
            pltpu.VMEM((2, BLOCK, INTERFACE), F32),
            pltpu.VMEM((RES, HORIZON), F32),
        ),
        in_specs=[hbm] * 7,
        out_specs=(vmem,) * 3,
        scratch_shapes=[
            pltpu.VMEM((2, BLOCK, UNKNOWNS), BF16),
            pltpu.VMEM((2, UNKNOWNS, UNKNOWNS), BF16),
            pltpu.VMEM((2, INTERFACE, UNKNOWNS), BF16),
            pltpu.VMEM((2 * BLOCK, UNKNOWNS), F32),
            pltpu.VMEM((2, LANES, UNKNOWNS), BF16),
            pltpu.VMEM((SUBS // 2, 2, 2 * BLOCK), jnp.int32),
            pltpu.VMEM((2, 4, BLOCK), jnp.int32),
            pltpu.VMEM((2, BLOCK), jnp.int32),
            pltpu.VMEM((RES, HORIZON), F32),
            pltpu.VMEM((2, 16, 128), BF16),
            pltpu.VMEM((2, INTERFACE, UNKNOWNS), BF16),
            pltpu.VMEM((2 * SPAN, 2, LANES), BF16),
            pltpu.VMEM((SUBS, 2, LANES), BF16),
            pltpu.VMEM((2 * SPAN, 3, 2, 128), BF16),
            pltpu.VMEM((SUBS, 2, 3, 2, 128), BF16),
            pltpu.VMEM((SUBS, 2, LANES), BF16),
            pltpu.VMEM((SUBS, 2, LANES), BF16),
            pltpu.VMEM((2 * SLAB, 16, 128), BF16),
            pltpu.VMEM((ROWS, 16), F32),
            pltpu.VMEM((3, 256, 256), BF16),
            pltpu.VMEM((PAIR, 256), BF16),
            pltpu.VMEM((128, 128), BF16),
            pltpu.VMEM((128, 128), BF16),
            pltpu.VMEM((2, LANES, LANES), BF16),
            pltpu.VMEM((ROWS, LANES), F32),
            pltpu.VMEM((ROWS, LANES), BF16),
            pltpu.VMEM((256, LANES), F32),
            pltpu.VMEM((PAIR, LANES), F32),
            pltpu.VMEM((2, 8, 8, 128), F32),
            pltpu.VMEM((2, 32, 8, 128), BF16),
            pltpu.VMEM((8, 8, 128), F32),
            pltpu.VMEM((8, 16, 128), F32),
            pltpu.VMEM((DISTS, 16, 128), F32),
            pltpu.VMEM((DISTS, 2, HORIZON, LANES), BF16),
            pltpu.VMEM((BLOCK, LANES), F32),
            pltpu.VMEM((BLOCK, LANES), F32),
            dma((10,)),
            dma, dma, dma, dma, dma, dma, dma, dma,
            dma((2,)), dma((2,)), dma((2,)), dma((2,)),
            dma, dma, dma, dma, dma, dma, dma, dma, dma, dma,
        ],
        compiler_params=pltpu.CompilerParams(
            collective_id=0, has_side_effects=True, vmem_limit_bytes=VMEM_LIMIT
        ),
    )(
        cost_terms, coupling.transpose(0, 2, 1), solve_factor, pairs,
        neighbours.transpose(0, 2, 1), ownership, capacity,
    )
    return pl.pallas_call(
        write_out,
        out_shape=(
            jax.ShapeDtypeStruct((2, BLOCK, UNKNOWNS), F32),
            jax.ShapeDtypeStruct((2, BLOCK, INTERFACE), F32),
            jax.ShapeDtypeStruct((RES, HORIZON), F32),
        ),
        in_specs=[vmem] * 3,
        out_specs=(hbm,) * 3,
        scratch_shapes=[dma((3,))],
        compiler_params=pltpu.CompilerParams(vmem_limit_bytes=1024 * 1024),
    )(*parts)


def solution(mesh):
    placed = (
        P("district", "sub", None),
        P("district", "sub", None),
        P("district", None),
        P("district", "sub"),
        P(),
        P("district", None, None),
        P("district", None, None),
    )
    return jax.shard_map(
        on_device,
        mesh=mesh,
        in_specs=placed,
        out_specs=(P("district", "sub", None), P("district", "sub", None), P()),
        check_vma=False,
    )
```

```python
import math

import jax
import jax.numpy as jnp
from jax import lax
from jax.experimental import pallas as pl
from jax.experimental.pallas import tpu as pltpu
from jax.sharding import PartitionSpec as P

MESH = pl.DeviceIdType.MESH
F32, BF16 = jnp.float32, jnp.bfloat16
HORIZON, UNKNOWNS, INTERFACE, BLOCK = 48, 768, 192, 64
RES, SUBS, DISTS = 16, 64, 4
PAIRS = SUBS // 2
REACH = 2
SLAB = 2 * REACH + 1
SPAN = PAIRS + 2 * REACH
PAIR = 2 * BLOCK
ROWS = SLAB * PAIR
OWN = REACH * PAIR
LANES = 256
STEP = 0.3
PEERS = SUBS - 1
OTHERS = 24
VMEM_LIMIT = 67043328 - 700 * 1024


def dot(a, b):
    return jnp.dot(a, b, preferred_element_type=F32)


def dot_ta(a, b):
    return lax.dot_general(a, b, (((0,), (0,)), ((), ())), preferred_element_type=F32)


def dot_tb(a, b):
    return lax.dot_general(a, b, (((1,), (1,)), ((), ())), preferred_element_type=F32)


def two_parts(x):
    high = x.astype(BF16)
    return jnp.concatenate([high, (x - high.astype(F32)).astype(BF16)], axis=0)


def dot2(x, b):
    out = dot(two_parts(x), b)
    return out[: x.shape[0]] + out[x.shape[0] :]


def iota(shape, dim):
    return lax.broadcasted_iota(jnp.int32, shape, dim)


def offsets_by_hops():
    def hops(at):
        x, y, z = at
        return min(x, 4 - x) + 2 * y + min(z, 8 - z)

    every = [(x, y, z) for z in range(8) for x in range(4) for y in range(2)]
    return sorted(every, key=lambda at: (-hops(at), at))


def folded(part):
    return jnp.concatenate([part[0:8, 0:64], part[8:16, 0:64]], axis=1)


def unfolded(part):
    return jnp.concatenate([part[:, 0:64], part[:, 64:128]], axis=0)


def kernel(
    cost, coup, solve, rel_h, near_h, owner_h, cap_h,
    plan_o, price_o, dual_o,
    X, S, C, cs, vfull, rel, near_in, owner_in, cap, meta, cts, send1, recv1, sendh, recvh, send2, recv2,
    mbuf, offs, L2, lown, p4t, p5, mp, zf, zb, sacc, usum, ara, arb, aka, akb, akc, maps, tops, price_s, price_r,

    load_sem, s1, r1, s2, r2, sm, rm, sp, rp, sa, ra, sb, rb, ska, rka, skb, rkb, sc, rc, se, re, skc, rkc,
):
    sub = lax.axis_index("sub")
    dist = lax.axis_index("district")
    sxy, sz = sub // 8, lax.rem(sub, 8)
    pair, side = sub // 2, lax.rem(sub, 2)

    small = [
        pltpu.make_async_copy(src, dst, load_sem.at[6 + i])
        for i, (src, dst) in enumerate(
            ((rel_h, rel), (near_h, near_in), (owner_h, owner_in), (cap_h, cap))
        )
    ]
    loads = []
    for d in range(2):
        loads.append(pltpu.make_async_copy(cost.at[d], X.at[d], load_sem.at[3 * d]))
        loads.append(pltpu.make_async_copy(solve.at[d], S.at[d], load_sem.at[3 * d + 1]))
        loads.append(pltpu.make_async_copy(coup.at[d], C.at[d], load_sem.at[3 * d + 2]))
    for copy in small + loads:
        copy.start()

    barrier = pltpu.get_barrier_semaphore()
    sx, sy = sub // 16, lax.rem(sxy, 2)
    x_at = [16 * lax.rem(sx + k, 4) for k in range(4)]
    y_at = [8 * lax.rem(sy + k, 2) for k in range(2)]
    z_at = [lax.rem(sz + k, 8) for k in range(8)]
    xy_at = {(x, y): x_at[x] + y_at[y] for x in range(4) for y in range(2)}
    dist_at = [lax.rem(dist + k, DISTS) for k in range(DISTS)]
    order = offsets_by_hops()
    peers = [xy_at[x, y] + z_at[z] for x, y, z in order[:-1]]
    level = [xy_at[x, y] for x, y, z in order if z == 0]
    ring = [z_at[k] for k in (4, 3, 5, 2, 6, 1, 7)]

    def hello(device):
        pl.semaphore_signal(barrier, inc=1, device_id=device, device_id_type=MESH)

    for peer in peers:
        hello({"sub": peer})
    for at in level:
        for k in range(1, DISTS):
            hello({"district": dist_at[k], "sub": at + sz})

    def whole(buf, send_sem, recv_sem):
        return pltpu.make_async_remote_copy(
            src_ref=buf,
            dst_ref=buf,
            send_sem=send_sem,
            recv_sem=recv_sem,
            device_id={"sub": sub},
            device_id_type=MESH,
        )

    for copy in small:
        copy.wait()
    place = iota((4, BLOCK), 1) + sub * BLOCK
    for d in range(2):
        told = [near_in[d] - place, owner_in[d : d + 1], jnp.zeros((11, BLOCK), jnp.int32)]
        told = jnp.concatenate(told, axis=0).astype(F32)
        meta[d] = jnp.concatenate([told, jnp.zeros((16, BLOCK), F32)], axis=1).astype(BF16)
    mbuf[2 * REACH + side] = meta[side]
    here = rel[pair]
    here = jnp.where(side == 0, here[:, 0:BLOCK], here[:, BLOCK:PAIR]) // BLOCK
    own_block = jnp.concatenate([here[0:1], here[1:2]], axis=1)

    first = []
    for d in range(2):
        for copy in loads[3 * d : 3 * d + 3]:
            copy.wait()
        cs_d = dot(X[d], S[d])
        cs[d * BLOCK : (d + 1) * BLOCK] = cs_d
        first.append(dot_tb((-cs_d).astype(BF16), C[d]).astype(BF16))
    first = jnp.concatenate(first, axis=0)
    first = jnp.concatenate([first, jnp.zeros((2 * BLOCK, LANES - INTERFACE), BF16)], axis=1)
    lane = iota((2 * BLOCK, 2 * BLOCK), 1)
    row = iota((2 * BLOCK, 2 * BLOCK), 0)
    eye = jnp.where(lane == row, 1.0, 0.0).astype(BF16)
    dest = own_block + 2 * SPAN * (lane[0:1] // BLOCK)
    at_row = iota((4 * SPAN, 2 * BLOCK), 0)
    sorted_rows, next_rows = [
        dot(jnp.where(dest + 2 * skip == at_row, 1.0, 0.0).astype(BF16), first).astype(BF16)
        for skip in (REACH, REACH - 1)
    ]
    send1[...] = sorted_rows.reshape(2 * SPAN, 2, LANES)
    rest = [t[:, 128:INTERFACE] for t in (sorted_rows, next_rows)]
    for k, tile in enumerate(
        (sorted_rows[:, 0:128], next_rows[:, 0:128], jnp.concatenate(rest, axis=1))
    ):
        sendh[:, k] = tile.reshape(2 * SPAN, 2, 128)

    pl.semaphore_wait(barrier, PEERS + OTHERS)

    for k in range(2 * SLAB):
        a, e = k // 2, k % 2

        def meta_copy():
            pltpu.make_async_remote_copy(
                src_ref=meta.at[e],
                dst_ref=mbuf.at[4 * REACH - 2 * a + side],
                send_sem=sm,
                recv_sem=rm,
                device_id={"sub": 2 * lax.rem(pair + a - REACH + PAIRS, PAIRS) + e},
                device_id_type=MESH,
            ).start()

        if a == REACH:
            pl.when(side != e)(meta_copy)
        else:
            meta_copy()

    def slot_of(device):
        return lax.rem(device, 2) * PAIRS + device // 2

    slot = slot_of(sub)
    for peer in peers:
        pltpu.make_async_remote_copy(
            src_ref=send1.at[SPAN * lax.rem(peer, 2) + peer // 2 + REACH],
            dst_ref=recv1.at[slot],
            send_sem=se,
            recv_sem=re,
            device_id={"sub": peer},
            device_id_type=MESH,
        ).start()
    for peer in peers:
        for k in range(2):
            pltpu.make_async_remote_copy(
                src_ref=sendh.at[SPAN * lax.rem(peer, 2) + peer // 2 + (REACH + 1) * k],
                dst_ref=recvh.at[slot, k],
                send_sem=s1,
                recv_sem=r1,
                device_id={"sub": peer},
                device_id_type=MESH,
            ).start()
    mine_at = SPAN * side + pair
    recv1[slot] = send1[mine_at + REACH]
    for k in range(2):
        recvh[slot, k] = sendh[mine_at + (REACH + 1) * k]

    back_at = 4 * (own_block // 2) + 2 * (lane // BLOCK) + lax.rem(own_block, 2)
    p5[...] = dot_ta(jnp.where(back_at == row, 1.0, 0.0).astype(BF16), eye).astype(BF16)
    for d in range(2):
        cts_d = dot(C[d], S[d]).astype(BF16)
        cts[d] = cts_d
        m_d = dot_tb(cts_d, C[d])
        mp[d] = jnp.zeros((LANES, LANES), BF16)
        mp[d, 0:INTERFACE, 0:INTERFACE] = (-STEP * m_d).astype(BF16)
        ri = iota((LANES - INTERFACE, LANES - 128), 0)
        li = iota((LANES - INTERFACE, LANES - 128), 1)
        shift = jnp.where(li - (INTERFACE - 128) == ri + RES, 1.0, 0.0)
        mp[d, INTERFACE:LANES, 128:LANES] = shift.astype(BF16)
        vfull[d, 0:INTERFACE] = cts_d
    for d in range(2):
        wide_map = mp[d, 0:INTERFACE, 0:INTERFACE]
        size = jnp.max(
            jnp.sum(jnp.abs(wide_map.astype(F32)), axis=0, keepdims=True), axis=1, keepdims=True
        )
        size = (1.0 + 1.02 * size).astype(BF16).astype(F32)
        small_map, tiles = wide_map[0:HORIZON].astype(F32) / size, []
        for j in range(4):
            if j:
                small_map = dot2(small_map, wide_map) / size
            padded = jnp.concatenate(
                [small_map, jnp.zeros((HORIZON, LANES - INTERFACE), F32)], axis=1
            )
            tops[d, :, LANES * j : LANES * (j + 1)] = two_parts(padded)
            tiles += [small_map[:, 0:HORIZON], jnp.broadcast_to(size, (HORIZON, BLOCK - HORIZON))]
        maps[dist, d] = jnp.concatenate(tiles, axis=1).astype(BF16)

    by_pair = rel[...].reshape(SUBS, PAIR)
    si, sj = iota((SUBS, SUBS), 0), iota((SUBS, SUBS), 1)
    pick = jnp.where((si // 2 == sj // 2) & (lax.rem(si, 2) == side), 1.0, 0.0).astype(BF16)

    def turned(values):
        flat = dot_ta(values.astype(F32).astype(BF16), pick)
        return jnp.concatenate([flat[0:BLOCK], flat[BLOCK:PAIR]], axis=1).astype(jnp.int32)

    block_of, place_in = turned(by_pair // BLOCK), turned(lax.rem(by_pair, BLOCK))
    odd = lax.rem(iota((1, PAIR), 1), 2)

    def place_map(a):
        hit = block_of == 2 * (pair + a - REACH) + odd
        at = jnp.sum(jnp.where(hit, place_in + 1, 0), axis=0, keepdims=True) - 1
        at = jnp.where(at >= 0, at + BLOCK * odd, -1)
        return jnp.where(at == row, 1.0, 0.0).astype(BF16)

    own_map = place_map(REACH)
    p4t[...] = dot_ta(own_map, eye).astype(BF16)

    whole(mbuf.at[pl.ds(0, 2 * SLAB - 1)], sm, rm).wait_recv()
    eye64 = jnp.where(
        iota((BLOCK, 128), 0) == iota((BLOCK, 128), 1), 1.0, 0.0
    ).astype(BF16)
    for m in range(2 * SLAB):
        offs[m * BLOCK : (m + 1) * BLOCK] = dot_tb(eye64, mbuf[m])
    diff = (iota((LANES, LANES), 1) - iota((LANES, LANES), 0)).astype(F32)
    for i in range(3):
        cols = offs[192 * i : 192 * i + 256]
        near = jnp.where(diff == 0.0, 1.0, 0.0)
        for k in range(4):
            near = near - jnp.where(diff == cols[:, k : k + 1], 0.25, 0.0)
        near = near.astype(BF16)
        L2[i, 32:224] = dot(near, near)[32:224].astype(BF16)
        L2[i, 0:32] = jnp.zeros((32, 256), BF16)
        L2[i, 224:256] = jnp.zeros((32, 256), BF16)
        if i == 1:
            lown[...] = near[64:192]

    def to_z(buf, send_sem, recv_sem):
        for z in ring:
            pltpu.make_async_remote_copy(
                src_ref=buf.at[sz],
                dst_ref=buf.at[sz],
                send_sem=send_sem,
                recv_sem=recv_sem,
                device_id={"sub": sxy * 8 + z},
                device_id_type=MESH,
            ).start()

    here_b = dist * 8 + sxy

    def start_b(buf, send_sem, recv_sem):
        for at in level:
            for k in (2, 1, 3, 0):
                if k == 0 and at is level[-1]:
                    continue
                pltpu.make_async_remote_copy(
                    src_ref=buf.at[here_b],
                    dst_ref=buf.at[here_b],
                    send_sem=send_sem,
                    recv_sem=recv_sem,
                    device_id={"district": dist_at[k], "sub": at + sz},
                    device_id_type=MESH,
                ).start()

    def all_of(buf, t, count, send_sem, recv_sem):
        return whole(buf.at[t, pl.ds(0, count)], send_sem.at[t], recv_sem.at[t])

    def reduce_a(t, part):
        ara[t, sz] = folded(part)
        to_z(ara.at[t], sa.at[t], ra.at[t])

    def reduce_b(t):
        all_of(ara, t, 7, sa, ra).wait_recv()
        arb[t, here_b] = jnp.sum(ara[t], axis=0).astype(BF16)
        start_b(arb.at[t], sb.at[t], rb.at[t])

    def reduce_end(t):
        all_of(arb, t, 31, sb, rb).wait_recv()
        return unfolded(jnp.sum(arb[t].astype(F32), axis=0))

    flow_map = mp.at[side]
    owners = []
    for a in range(SLAB):
        owner = [mbuf[2 * a + e][4:5, 0:BLOCK].astype(F32) for e in range(2)]
        owner = jnp.concatenate(owner, axis=1)
        owners.append(jnp.where(iota((RES, PAIR), 0).astype(F32) == owner, 1.0, 0.0))
    own_owners = owners[REACH]
    half_tile = jnp.zeros((2 * RES, BLOCK), F32)

    def back_step(tiles):
        rows2 = jnp.concatenate([two_parts(t) for t in tiles], axis=1)
        out0 = dot(rows2[:, 0:256], L2[0])
        out1 = dot(rows2[:, 192:448], L2[1])
        out2 = dot(rows2[:, 384:640], L2[2])
        out1 = jnp.concatenate([half_tile, out1, half_tile], axis=1)
        sums = [
            out0[:, 0:128],
            out0[:, 128:256] + out1[:, 0:128],
            out1[:, 128:256],
            out1[:, 256:384] + out2[:, 0:128],
            out2[:, 128:256],
        ]
        return [t[0:RES] + t[RES : 2 * RES] for t in sums]

    def seen_flows(weights):
        turned_weights = dot(two_parts(weights), own_map).astype(BF16)
        sums = dot(turned_weights, recv1[...].reshape(2 * SUBS, LANES))[:, 0:INTERFACE]
        sums = sums[0:BLOCK] + sums[BLOCK : 2 * BLOCK]
        return [sums[RES * j : RES * (j + 1)] for j in range(4)]

    def next_power(total, seen, count, j):
        total = dot2(total, flow_map[0:INTERFACE, 0:INTERFACE])
        return total + seen[j] * float(math.comb(count, j))

    def draws_of(seen, count):
        total = seen[count]
        for j in reversed(range(count)):
            total = next_power(total, seen, count, j)
        return total[:, 0:128]

    weights, tiles = [own_owners], owners
    for _ in range(3):
        tiles = back_step(tiles)
        weights.append(tiles[REACH])
    weights = jnp.concatenate(weights, axis=0)
    unit = dot_tb(two_parts(weights), own_owners.astype(BF16))
    unit = unit[0:BLOCK] + unit[BLOCK : 2 * BLOCK]
    unit = [unit[RES * j : RES * (j + 1), 0:RES] for j in range(4)]
    aka[sz] = folded(jnp.concatenate(unit, axis=1))
    to_z(aka, ska, rka)
    whole(recv1.at[pl.ds(0, PEERS)], se, re).wait_recv()
    seen = seen_flows(weights)
    early = draws_of(seen, 3)
    reduce_a(0, early)
    weights = []
    for _ in range(4):
        tiles = back_step(tiles)
        weights.append(tiles[REACH])
    weights = jnp.concatenate(weights, axis=0)
    seen = seen + seen_flows(weights)
    late = seen[7]
    for j in (6, 5, 4, 3):
        late = next_power(late, seen, 7, j)

    sacc[...] = jnp.zeros((256, LANES), F32)
    whole(recvh.at[pl.ds(0, PEERS)], s1, r1).wait_recv()
    for k in (2, 1, 3):
        pltpu.make_async_remote_copy(
            src_ref=maps.at[dist],
            dst_ref=maps.at[dist],
            send_sem=sc,
            recv_sem=rc,
            device_id={"district": dist_at[k]},
            device_id_type=MESH,
        ).start()
    lane_e = iota((PAIR, 128), 1) - (INTERFACE - 128)
    for a in range(SLAB):
        top = a * PAIR
        if a == REACH:
            part = dot(own_map, recv1[...].reshape(2 * SUBS, LANES))
            low, high = part[:, 0:128], part[:, 128:LANES]
        else:
            k, which = (0, a) if a < REACH else (1, a - REACH - 1)
            low = dot(place_map(a), recvh[:, k, which].reshape(2 * SUBS, 128))
            high = dot(place_map(a), recvh[:, k, 2].reshape(2 * SUBS, 128))
            if which:
                high = pltpu.roll(high, BLOCK, 1)
            high = jnp.where(lane_e < 0, high, 0.0)
        owner = offs[top : top + PAIR, 4:5].astype(jnp.int32)
        mark = jnp.where((lane_e == owner) & (lane_e >= 0) & (lane_e < RES), 1.0, 0.0)
        high = high + mark
        zf[top : top + PAIR, 0:128] = low
        zf[top : top + PAIR, 128:LANES] = high
        zb[top : top + PAIR, 0:128] = low.astype(BF16)
        zb[top : top + PAIR, 128:LANES] = high.astype(BF16)
    sacc[32:224] = zf[224:416]
    usum[...] = jnp.zeros((PAIR, LANES), F32)

    def half(i):
        u = dot(L2[i, 32:224], zb[192 * i : 192 * i + 256])
        if i == 1:
            usum[...] += u[32:160]
        return u.astype(BF16)

    def advance(i, u):
        at = 32 + 192 * i
        z = zf[at : at + 192] + dot(u, flow_map[...])
        zf[at : at + 192] = z
        zb[at : at + 192] = z.astype(BF16)
        if i == 1:
            sacc[32:224] += z

    def step():
        us = [half(i) for i in range(3)]
        for i, u in enumerate(us):
            advance(i, u)

    for j in (2, 1, 0):
        if j:
            step()
        late = next_power(late, seen, 7, j)
    reduce_a(1, late[:, 0:128])
    for k in range(4):
        step()
    whole(aka.at[pl.ds(0, 7)], ska, rka).wait_recv()
    by_side = [aka[d] + aka[d + 2] + aka[d + 4] + aka[d + 6] for d in range(2)]
    akb[sxy] = jnp.concatenate(by_side, axis=0)
    for at in level[:-1]:
        pltpu.make_async_remote_copy(
            src_ref=akb.at[sxy],
            dst_ref=akb.at[sxy],
            send_sem=skb,
            recv_sem=rkb,
            device_id={"sub": at + sz},
            device_id_type=MESH,
        ).start()
    reduce_b(0)

    u = half(1)
    prices = (STEP * usum[...]).astype(BF16)
    marks = zb[OWN : OWN + PAIR, INTERFACE:LANES]
    back = jnp.concatenate([prices[:, 0:INTERFACE], marks], axis=1)
    send2[...] = dot(p4t[...], back).astype(BF16).reshape(SUBS, 2, LANES)

    for peer in peers:
        pltpu.make_async_remote_copy(
            src_ref=send2.at[slot_of(peer)],
            dst_ref=recv2.at[sub],
            send_sem=s2,
            recv_sem=r2,
            device_id={"sub": peer},
            device_id_type=MESH,
        ).start()
    recv2[sub] = send2[slot_of(sub)]

    near_marks = dot(lown[...], zb[192:448, 128:LANES])[:, INTERFACE - 128 :]
    advance(1, u)
    near_sums = dot(lown[...], sacc[...].astype(BF16))[:, 0:INTERFACE]
    prices = jnp.concatenate([near_sums, near_marks], axis=1)
    kept = jnp.where(side == 0, prices[0:BLOCK], prices[BLOCK:PAIR])
    price0, marks0 = kept[:, 0:INTERFACE], kept[:, INTERFACE:LANES]
    price_s[...] = jnp.where(side == 0, prices[BLOCK:PAIR], prices[0:BLOCK])
    price_copy = pltpu.make_async_remote_copy(
        src_ref=price_s,
        dst_ref=price_r,
        send_sem=sp,
        recv_sem=rp,
        device_id={"sub": 2 * pair + 1 - side},
        device_id_type=MESH,
    )
    price_copy.start()

    reduce_b(1)
    whole(akb.at[pl.ds(0, 7)], skb, rkb).wait_recv()
    akc[dist] = jnp.sum(akb[...], axis=0)
    for k in (2, 1, 3):
        pltpu.make_async_remote_copy(
            src_ref=akc.at[dist],
            dst_ref=akc.at[dist],
            send_sem=skc,
            recv_sem=rkc,
            device_id={"district": dist_at[k]},
            device_id_type=MESH,
        ).start()
    capacity = cap[...]
    scale = 1.0 / math.sqrt(DISTS * 2 * SUBS * BLOCK / (2 * RES))
    duals = (reduce_end(0)[:, 0:HORIZON] - capacity) * scale
    wide = jnp.concatenate([duals, jnp.zeros((RES, INTERFACE - HORIZON), F32)], axis=1)

    binom = (1.0, 6.0, 15.0, 20.0)
    in_price = (1.0, -0.9, 0.27, -0.027)
    in_sum = (-4.0, 1.8, -0.36, 0.027)

    def powers_of(d):
        moved = dot2(duals, tops[d, 0:HORIZON]) + dot(
            duals.astype(BF16), tops[d, HORIZON : 2 * HORIZON]
        )
        size = maps[dist, d, 0:1, HORIZON : HORIZON + 1].astype(F32)
        powers = [wide]
        for j in range(4):
            part = moved[:, LANES * j : LANES * j + INTERFACE]
            for _ in range(j + 1):
                part = part * size * (-1.0 / STEP)
            powers.append(part)
        return powers

    def stack(powers, weights):
        parts = [p * (w / b) for p, w, b in zip(powers, weights, binom)]
        return jnp.concatenate(parts, axis=0).astype(BF16)

    powers_by = [powers_of(d) for d in range(2)]
    for d in range(2):
        vfull[d, INTERFACE:LANES] = dot(stack(powers_by[d][0:4], in_price), cts[d]).astype(BF16)

    price_copy.wait_recv()
    whole(maps.at[pl.ds(0, 3)], sc, rc).wait_recv()
    sums = [stack(powers_by[d][1:], in_sum) for d in range(2)]
    here_sums = jnp.where(side == 0, sums[0], sums[1])
    there_sums = jnp.where(side == 0, sums[1], sums[0])
    price_o[side] = STEP * (price0 + dot(marks0.astype(BF16), here_sums))
    sent = price_r[...]
    price_o[1 - side] = STEP * (
        sent[:, 0:INTERFACE] + dot(sent[:, INTERFACE:LANES].astype(BF16), there_sums)
    )
    causes = []
    for k in range(DISTS):
        for d in range(2):
            size = maps[k, d, 0:1, HORIZON : HORIZON + 1].astype(F32)
            moved = dot2(duals, maps[k, d])
            for j in range(4):
                part = moved[:, BLOCK * j : BLOCK * (j + 1)] * (math.comb(3, j) / STEP)
                for _ in range(j + 1):
                    part = part * size
                causes.append(part)
    causes = two_parts(jnp.concatenate(causes, axis=0))
    whole(recv2.at[pl.ds(0, PEERS)], s2, r2).wait_recv()
    mine = dot(p5[...], recv2[...].reshape(2 * SUBS, LANES)).astype(BF16)
    for d in range(2):
        at = d * BLOCK
        plan_o[d] = -(cs[at : at + BLOCK] + dot(mine[at : at + BLOCK], vfull[d]))

    whole(akc.at[pl.ds(0, 3)], skc, rkc).wait_recv()
    units = [unfolded(akc[k][8 * d : 8 * d + 8]) for k in range(DISTS) for d in range(2)]
    units = jnp.concatenate(units, axis=1)
    count = units.shape[1]
    draws1 = dot2(units, causes[0:count]) + dot(units.astype(BF16), causes[count : 2 * count])
    draws1 = draws1[:, 0:HORIZON]
    draws0 = reduce_end(1)[:, 0:HORIZON]
    dual_o[...] = duals + (draws0 + draws1 - capacity) * scale

    whole(mbuf.at[pl.ds(0, 2 * SLAB - 1)], sm, rm).wait_send()
    whole(recvh.at[pl.ds(0, PEERS)], s1, r1).wait_send()
    whole(recv2.at[pl.ds(0, PEERS)], s2, r2).wait_send()
    for t in range(2):
        all_of(ara, t, 7, sa, ra).wait_send()
        all_of(arb, t, 31, sb, rb).wait_send()
    whole(aka.at[pl.ds(0, 7)], ska, rka).wait_send()
    whole(akb.at[pl.ds(0, 7)], skb, rkb).wait_send()
    whole(akc.at[pl.ds(0, 3)], skc, rkc).wait_send()
    whole(maps.at[pl.ds(0, 3)], sc, rc).wait_send()
    whole(recv1.at[pl.ds(0, PEERS)], se, re).wait_send()
    price_copy.wait_send()


def write_out(plan, price, dual, plan_o, price_o, dual_o, sems):
    copies = [
        pltpu.make_async_copy(src, dst, sems.at[i])
        for i, (src, dst) in enumerate(((plan, plan_o), (price, price_o), (dual, dual_o)))
    ]
    for copy in copies:
        copy.start()
    for copy in copies:
        copy.wait()


def on_device(cost_terms, neighbours, relayout, ownership, capacity, coupling, solve_factor):
    pairs = relayout.reshape(2, SUBS // 2, 2 * BLOCK).transpose(1, 0, 2)
    vmem = pl.BlockSpec(memory_space=pltpu.VMEM)
    hbm = pl.BlockSpec(memory_space=pltpu.HBM)
    dma = pltpu.SemaphoreType.DMA
    parts = pl.pallas_call(
        kernel,
        out_shape=(
            pltpu.VMEM((2, BLOCK, UNKNOWNS), F32),
            pltpu.VMEM((2, BLOCK, INTERFACE), F32),
            pltpu.VMEM((RES, HORIZON), F32),
        ),
        in_specs=[hbm] * 7,
        out_specs=(vmem,) * 3,
        scratch_shapes=[
            pltpu.VMEM((2, BLOCK, UNKNOWNS), BF16),
            pltpu.VMEM((2, UNKNOWNS, UNKNOWNS), BF16),
            pltpu.VMEM((2, INTERFACE, UNKNOWNS), BF16),
            pltpu.VMEM((2 * BLOCK, UNKNOWNS), F32),
            pltpu.VMEM((2, LANES, UNKNOWNS), BF16),
            pltpu.VMEM((SUBS // 2, 2, 2 * BLOCK), jnp.int32),
            pltpu.VMEM((2, 4, BLOCK), jnp.int32),
            pltpu.VMEM((2, BLOCK), jnp.int32),
            pltpu.VMEM((RES, HORIZON), F32),
            pltpu.VMEM((2, 16, 128), BF16),
            pltpu.VMEM((2, INTERFACE, UNKNOWNS), BF16),
            pltpu.VMEM((2 * SPAN, 2, LANES), BF16),
            pltpu.VMEM((SUBS, 2, LANES), BF16),
            pltpu.VMEM((2 * SPAN, 3, 2, 128), BF16),
            pltpu.VMEM((SUBS, 2, 3, 2, 128), BF16),
            pltpu.VMEM((SUBS, 2, LANES), BF16),
            pltpu.VMEM((SUBS, 2, LANES), BF16),
            pltpu.VMEM((2 * SLAB, 16, 128), BF16),
            pltpu.VMEM((ROWS, 16), F32),
            pltpu.VMEM((3, 256, 256), BF16),
            pltpu.VMEM((PAIR, 256), BF16),
            pltpu.VMEM((128, 128), BF16),
            pltpu.VMEM((128, 128), BF16),
            pltpu.VMEM((2, LANES, LANES), BF16),
            pltpu.VMEM((ROWS, LANES), F32),
            pltpu.VMEM((ROWS, LANES), BF16),
            pltpu.VMEM((256, LANES), F32),
            pltpu.VMEM((PAIR, LANES), F32),
            pltpu.VMEM((2, 8, 8, 128), F32),
            pltpu.VMEM((2, 32, 8, 128), BF16),
            pltpu.VMEM((8, 8, 128), F32),
            pltpu.VMEM((8, 16, 128), F32),
            pltpu.VMEM((DISTS, 16, 128), F32),
            pltpu.VMEM((DISTS, 2, HORIZON, LANES), BF16),
            pltpu.VMEM((2, 2 * HORIZON, 4 * LANES), BF16),
            pltpu.VMEM((BLOCK, LANES), F32),
            pltpu.VMEM((BLOCK, LANES), F32),
            dma((10,)),
            dma, dma, dma, dma, dma, dma, dma, dma,
            dma((2,)), dma((2,)), dma((2,)), dma((2,)),
            dma, dma, dma, dma, dma, dma, dma, dma, dma, dma,
        ],
        compiler_params=pltpu.CompilerParams(
            collective_id=0, has_side_effects=True, vmem_limit_bytes=VMEM_LIMIT
        ),
    )(
        cost_terms, coupling.transpose(0, 2, 1), solve_factor, pairs,
        neighbours.transpose(0, 2, 1), ownership, capacity,
    )
    return pl.pallas_call(
        write_out,
        out_shape=(
            jax.ShapeDtypeStruct((2, BLOCK, UNKNOWNS), F32),
            jax.ShapeDtypeStruct((2, BLOCK, INTERFACE), F32),
            jax.ShapeDtypeStruct((RES, HORIZON), F32),
        ),
        in_specs=[vmem] * 3,
        out_specs=(hbm,) * 3,
        scratch_shapes=[dma((3,))],
        compiler_params=pltpu.CompilerParams(vmem_limit_bytes=1024 * 1024),
    )(*parts)


def solution(mesh):
    placed = (
        P("district", "sub", None),
        P("district", "sub", None),
        P("district", None),
        P("district", "sub"),
        P(),
        P("district", None, None),
        P("district", None, None),
    )
    return jax.shard_map(
        on_device,
        mesh=mesh,
        in_specs=placed,
        out_specs=(P("district", "sub", None), P("district", "sub", None), P()),
        check_vma=False,
    )
```
